128 devices in a mesh: ez: 4 (over z), ey: 4 (over y), ex: 8 (over x, core).
Axes of the slice: x: 4, y: 4, z: 4, core: 2. Of those that a mesh axis runs over, the one named last changes fastest.
Arguments:
- x_tokens: bfloat16 [16384, 2048], P(('ez', 'ey', 'ex'))
- expert_ids: int32 [16384, 8], P(('ez', 'ey', 'ex'))
- gate_vals: float32 [16384, 8], P(('ez', 'ey', 'ex'))
- w_gate: bfloat16 [128, 2048, 768], P(('ex', 'ey', 'ez'))
- w_up: bfloat16 [128, 2048, 768], P(('ex', 'ey', 'ez'))
- w_down: bfloat16 [128, 768, 2048], P(('ex', 'ey', 'ez'))
Outputs:
- output: bfloat16 [16384, 2048], P(('ez', 'ey', 'ex'))
All inputs are finite; a program needn't handle non-finite values.
Results may differ from the reference program's by a relative error of at most 0.00512202.
Values are sent between devices in bfloat16 or wider.
A program may use at most 1 GiB of HBM per device.

```python
import jax
import jax.numpy as jnp
from jax import lax

HIDDEN = 2048
FFN_DIM = 768
EXPERTS = 128
TOP_K = 8
TOK_DEV = 128
DEVICES = 128
GROUPS = 8

TOKENS_ALL = DEVICES * TOK_DEV
CAP_EXPERT = 2 * DEVICES * TOK_DEV * TOP_K // EXPERTS


def draw_routing(route_key):
    perm_key, group_key = jax.random.split(route_key)
    group_size = EXPERTS // GROUPS
    pair_count = group_size // 2
    pick_groups = TOP_K // 2
    perm_score = jax.random.randint(perm_key, (DEVICES, GROUPS, group_size), 0, 1 << 20)
    inner_perm = jnp.argsort(perm_score * group_size + jnp.arange(group_size), axis=-1)
    inner_perm = inner_perm.at[:, :, 2].set(inner_perm[:, :, 0])
    group_score = jax.random.randint(group_key, (DEVICES, GROUPS), 0, 1 << 20)
    group_perm = jnp.argsort(group_score * GROUPS + jnp.arange(GROUPS), axis=-1)
    visit_idx = jnp.arange(TOK_DEV)[:, None] * pick_groups + jnp.arange(pick_groups)[None, :]
    dev_idx = jnp.arange(DEVICES)[:, None, None]
    group_id = group_perm[dev_idx, visit_idx[None] % GROUPS]
    pair_pos = 2 * ((visit_idx // GROUPS) % pair_count)[None]
    first_pick = inner_perm[dev_idx, group_id, pair_pos]
    second_pick = inner_perm[dev_idx, group_id, pair_pos + 1]
    local_pick = jnp.stack([first_pick, second_pick], axis=-1)
    expert_ids = group_id[:, :, :, None] * group_size + local_pick
    return expert_ids.reshape(TOKENS_ALL, TOP_K).astype(jnp.int32)


def setup_inputs(seed: int = 0) -> dict:
    base_key = jax.random.key(seed)
    key_x, key_gate, key_one, key_three, key_two, key_route = jax.random.split(base_key, 6)
    x_tokens = jax.random.normal(key_x, (TOKENS_ALL, HIDDEN), jnp.float32)
    gate_raw = jax.random.uniform(key_gate, (TOKENS_ALL, TOP_K), jnp.float32, 0.5, 1.5)
    gate_vals = 2.5 * gate_raw / jnp.sum(gate_raw, axis=1, keepdims=True)
    w_gate = jax.random.normal(key_one, (EXPERTS, HIDDEN, FFN_DIM), jnp.float32) * HIDDEN ** -0.5
    w_up = jax.random.normal(key_three, (EXPERTS, HIDDEN, FFN_DIM), jnp.float32) * HIDDEN ** -0.5
    w_down = jax.random.normal(key_two, (EXPERTS, FFN_DIM, HIDDEN), jnp.float32) * FFN_DIM ** -0.5
    return {
        'x_tokens': x_tokens.astype(jnp.bfloat16),
        'expert_ids': draw_routing(key_route),
        'gate_vals': gate_vals,
        'w_gate': w_gate.astype(jnp.bfloat16),
        'w_up': w_up.astype(jnp.bfloat16),
        'w_down': w_down.astype(jnp.bfloat16),
    }


def reference(x_tokens, expert_ids, gate_vals, w_gate, w_up, w_down):
    flat_ids = expert_ids.reshape(-1)
    flat_gates = gate_vals.reshape(-1)
    pair_tok = jnp.arange(TOKENS_ALL * TOP_K) // TOP_K
    slot_pos = jnp.arange(CAP_EXPERT)

    def expert_step(acc_sum, scan_in):
        expert, w_one, w_three, w_two = scan_in
        chosen = flat_ids == expert
        n_chosen = jnp.sum(chosen.astype(jnp.int32))
        pair_sel = jnp.nonzero(chosen, size=CAP_EXPERT, fill_value=0)[0]
        tok_sel = pair_tok[pair_sel]
        weight = jnp.where(slot_pos < n_chosen, flat_gates[pair_sel], 0.0)
        tok_rows = x_tokens[tok_sel]
        h_gate = jnp.dot(tok_rows, w_one, preferred_element_type=jnp.float32)
        h_up = jnp.dot(tok_rows, w_three, preferred_element_type=jnp.float32)
        act_bf = (jax.nn.silu(h_gate) * h_up).astype(jnp.bfloat16)
        exp_out = jnp.dot(act_bf, w_two, preferred_element_type=jnp.float32).astype(jnp.bfloat16)
        acc_sum = acc_sum.at[tok_sel].add(weight[:, None] * exp_out.astype(jnp.float32))
        return acc_sum, None

    acc_init = jnp.zeros((TOKENS_ALL, HIDDEN), jnp.float32)
    moe_sum = lax.scan(expert_step, acc_init, (jnp.arange(EXPERTS), w_gate, w_up, w_down))[0]
    return (x_tokens.astype(jnp.float32) + moe_sum).astype(jnp.bfloat16)
```

```python
import functools

import jax
import jax.numpy as jnp
from jax import lax
from jax.experimental import pallas as pl
from jax.experimental.pallas import tpu as pltpu
from jax.sharding import PartitionSpec as P

TOKEN_AXES = ('ez', 'ey', 'ex')
EXPERT_AXES = ('ex', 'ey', 'ez')
MESH = pl.DeviceIdType.MESH
F32 = jnp.float32
BF16 = jnp.bfloat16

Z, Y, X = 0, 1, 2
D1 = (Y, Z, X)
D2 = (Z, X, Y)
D3 = (X, Y, Z)
A_IS_D1 = (True, False, True)
RING = 4
CORES = 2
CAP = 16
TOK = 128
LEAD = (CORES, RING, RING, RING)


def split_width(hid):
    tiles = hid // 128
    first = -(-tiles // 3)
    rest = tiles - first
    return (first * 128, (rest - rest // 2) * 128, (rest // 2) * 128)


def moe_kernel(widths, fdim, f_tile, x_ref, meta_ref, w1_hbm, w3_hbm, w2_hbm, y_ref, *scr):
    it = iter(scr)
    take3 = lambda: [next(it) for _ in range(3)]
    gat, til, rec = take3(), take3(), take3()
    meta, sel, comb = take3(), take3(), take3()
    pas3, pas4, pas5 = take3(), take3(), take3()
    part, prec, pas6 = take3(), take3(), take3()
    w1, w3, w2, act = next(it), next(it), next(it), next(it)
    send_sem, recv_sem, w_sem, credit = next(it), next(it), next(it), next(it)

    offs = (0, widths[0], widths[0] + widths[1])
    ez, ey, ex = lax.axis_index('ez'), lax.axis_index('ey'), lax.axis_index('ex')
    core = lax.rem(ex, CORES)
    pos = (ez, ey, ex // CORES)
    mod = lambda v: lax.rem(v + RING, RING)
    other = 1 - core

    def peer(dim, off, c):
        q = [mod(pos[d] + off) if d == dim else pos[d] for d in range(3)]
        return (q[0], q[1], q[2] * CORES + c)

    counter = [0]

    def rcopy(src, dst, dev):
        i = counter[0]
        counter[0] += 1
        return pltpu.make_async_remote_copy(src, dst, send_sem.at[i], recv_sem.at[i], device_id=dev, device_id_type=MESH)

    bar = pltpu.get_barrier_semaphore()
    npeer = 0
    for dim in range(3):
        for off in (1, -1):
            for c in (core, other):
                pl.semaphore_signal(bar, inc=1, device_id=peer(dim, off, c), device_id_type=MESH)
                npeer += 1
    pl.semaphore_signal(bar, inc=1, device_id=peer(0, 0, other), device_id_type=MESH)
    w_copies = [pltpu.make_async_copy(s, d, w_sem.at[i]) for i, (s, d) in enumerate(((w1_hbm, w1), (w3_hbm, w3), (w2_hbm, w2)))]
    pl.semaphore_wait(bar, npeer + 1)

    DIRS = (1, -1)
    p1 = [pos[D1[k]] for k in range(3)]
    p2 = [pos[D2[k]] for k in range(3)]
    p3 = [pos[D3[k]] for k in range(3)]

    def chunk(k, r):
        return gat[k].at[:, :, p2[k], mod(p1[k] + r)]

    g1 = [[None, None] for _ in range(3)]
    m1 = [[None, None] for _ in range(3)]
    for k in range(3):
        xk = x_ref.at[:, :, :, pl.ds(offs[k], widths[k])]
        for i, d in enumerate(DIRS):
            m1[k][i] = rcopy(meta_ref, meta[k].at[p2[k], p1[k]], peer(D1[k], d, core))
            m1[k][i].start()
            g1[k][i] = rcopy(xk, chunk(k, 0), peer(D1[k], d, core))
            g1[k][i].start()
    g2 = [[[None] * 4, [None] * 4] for _ in range(3)]
    for k in range(3):
        xk = x_ref.at[:, :, :, pl.ds(offs[k], widths[k])]
        for i, d in enumerate(DIRS):
            g2[k][i][0] = rcopy(xk, chunk(k, 0), peer(D2[k], d, core))
            g2[k][i][0].start()
    for c in w_copies:
        c.start()
    for k in range(3):
        gat[k][:, :, p2[k], p1[k]] = x_ref[:, :, :, offs[k]:offs[k] + widths[k]]
        meta[k][p2[k], p1[k]] = meta_ref[...]
    f1 = [[None, None] for _ in range(3)]
    mf1 = [None] * 3
    for k in range(3):
        for i, d in enumerate(DIRS):
            m1[k][i].wait_recv()
            if i == 0:
                src = meta[k].at[p2[k], mod(p1[k] - 1)]
                mf1[k] = rcopy(src, src, peer(D1[k], 1, core))
                mf1[k].start()
            g1[k][i].wait_recv()
            half = chunk(k, -d).at[i]
            f1[k][i] = rcopy(half, half, peer(D1[k], d, core))
            f1[k][i].start()
    m2 = [[None, None] for _ in range(3)]
    for k in range(3):
        for i, d in enumerate(DIRS):
            for r in (1, 3):
                g2[k][i][r] = rcopy(chunk(k, r), chunk(k, r), peer(D2[k], d, core))
                g2[k][i][r].start()
    for k in range(3):
        mf1[k].wait_recv()
        for i, d in enumerate(DIRS):
            row = meta[k].at[p2[k]]
            m2[k][i] = rcopy(row, row, peer(D2[k], d, core))
            m2[k][i].start()

    def forward2(k, i, r):
        d = DIRS[i]
        g2[k][i][r].wait_recv()
        src = gat[k].at[:, :, mod(p2[k] - d), mod(p1[k] + r)]
        c = rcopy(src, src, peer(D2[k], d, core))
        c.start()
        return c

    f2 = [[None] * 4 for _ in range(3)]
    for k in range(3):
        f2[k][0] = forward2(k, 0, 0)
    for k in range(3):
        for i in range(2):
            f1[k][i].wait_recv()
        for i, d in enumerate(DIRS):
            g2[k][i][2] = rcopy(chunk(k, 2), chunk(k, 2), peer(D2[k], d, core))
            g2[k][i][2].start()
    mf2 = [None] * 3
    for k in range(3):
        for i in range(2):
            m2[k][i].wait_recv()
        src = meta[k].at[mod(p2[k] - 1)]
        mf2[k] = rcopy(src, src, peer(D2[k], 1, core))
        mf2[k].start()
    for k in range(3):
        f2[k][1] = forward2(k, 0, 1)
        f2[k][3] = forward2(k, 1, 3)

    tri = (lax.broadcasted_iota(jnp.int32, (TOK, TOK), 0) < lax.broadcasted_iota(jnp.int32, (TOK, TOK), 1)).astype(BF16)
    i8 = lax.broadcasted_iota(jnp.int32, (8, 1), 0)
    stride3 = (2 * RING * RING, RING, 1)
    strides = (1, RING, 2 * RING * RING)
    slot = lax.broadcasted_iota(jnp.int32, (8, CAP, TOK), 1).astype(F32)

    def experts8(k):
        base = pos[D1[k]] * strides[D1[k]] + pos[D2[k]] * strides[D2[k]]
        return (base + (i8 & 3) * stride3[k] + (i8 >> 2) * (RING * RING)).astype(F32)

    def picked(ids, evec):
        m = (ids[0:1, :] == evec).astype(F32)
        for j in range(1, 8):
            m = m + (ids[j:j + 1, :] == evec).astype(F32)
        return m

    def rank_of(m):
        rank = jnp.dot(m.astype(BF16), tri, preferred_element_type=F32)
        return jnp.where(m > 0.5, rank, -1.0)

    for k in range(3):
        mf2[k].wait_recv()
        evec = experts8(k)

        def ranks(i, carry, k=k, evec=evec):
            rows = [picked(meta[k][i, j, 0:8], evec) for j in range(4)]
            rm = rank_of(jnp.concatenate(rows, axis=0))
            for j in range(4):
                hot = (rm[j * 8:(j + 1) * 8][:, None, :] == slot).astype(F32)
                sel[k][i, j] = hot.reshape(TOK, TOK).astype(BF16)
            return carry

        lax.fori_loop(0, 4, ranks, 0)

    for k in range(3):
        f2[k][2] = forward2(k, 1, 2)

    def sub(ref, k, c, d, half=None):
        a = slice(None) if half is None else pl.ds(2 * half, 2)
        return (ref.at[c, d, a], ref.at[c, a, d], ref.at[c, a, :, d])[k]

    def opened(k):
        for r in (0, 1, 2, 3):
            for i in range(2):
                if (i, r) not in ((0, 0), (0, 1), (1, 3), (1, 2)):
                    g2[k][i][r].wait_recv()
            f2[k][r].wait_recv()
        for c in m1[k] + g1[k] + f1[k] + [mf1[k]] + m2[k] + [mf2[k]] + g2[k][0] + g2[k][1] + f2[k]:
            c.wait_send()

    def exchange_start(k, cr, src, src_block, dst, dst_block, pas, self_copy):
        c = core if cr == 0 else other
        first, direct = [], []
        for i, d in enumerate(DIRS):
            cp = rcopy(src_block(src, c, mod(p3[k] + 2), i), pas.at[i, cr], peer(D3[k], d, core))
            cp.start()
            first.append(cp)
        for i, d in enumerate(DIRS):
            cp = rcopy(src_block(src, c, mod(p3[k] + d), None), dst_block(dst, core, p3[k], None), peer(D3[k], d, c))
            cp.start()
            direct.append(cp)
        if cr == 0:
            self_copy()
        else:
            cp = rcopy(src_block(src, c, p3[k], None), dst_block(dst, core, p3[k], None), peer(D3[k], 0, other))
            cp.start()
            direct.append(cp)
        return first, direct

    def exchange_forward(k, cr, first, direct, dst, dst_block, pas):
        c = core if cr == 0 else other
        for i, d in enumerate(DIRS):
            first[i].wait_recv()
            cp = rcopy(pas.at[i, cr], dst_block(dst, core, mod(p3[k] - d), i), peer(D3[k], d, c))
            cp.start()
            direct.append(cp)

    def til_block(ref, c, d, half):
        return ref.at[c, d] if half is None else ref.at[c, d, pl.ds(2 * half, 2)]

    x3 = [[None, None] for _ in range(3)]
    for k in range(3):
        opened(k)
        w = widths[k]

        def select(i, carry, k=k, w=w):
            for j in range(4):
                rows = gat[k][:, :, i, j].reshape(TOK, w)
                out = jnp.dot(sel[k][i, j], rows, preferred_element_type=F32).astype(BF16).reshape(CORES, RING, CAP, w)
                if A_IS_D1[k]:
                    til[k][:, :, j, i] = out
                else:
                    til[k][:, :, i, j] = out
            return carry

        lax.fori_loop(0, 4, select, 0)
        for cr in range(2):
            def keep(k=k):
                v = til[k][core, p3[k]]
                if k == 0:
                    rec[k][core, p3[k]] = v
                elif k == 1:
                    rec[k][core, :, p3[k]] = v
                else:
                    rec[k][core, :, :, p3[k]] = v
            rblock = lambda ref, c, d, half, k=k: sub(ref, k, c, d, half)
            x3[k][cr] = exchange_start(k, cr, til[k], til_block, rec[k], rblock, pas3[k], keep)
    for k in range(3):
        rblock = lambda ref, c, d, half, k=k: sub(ref, k, c, d, half)
        for cr in range(2):
            exchange_forward(k, cr, *x3[k][cr], rec[k], rblock, pas3[k])
    for k in range(3):
        for cr in range(2):
            first, direct = x3[k][cr]
            for cp in direct:
                cp.wait_recv()
            for cp in first + direct:
                cp.wait_send()
    for c in w_copies:
        c.wait()

    x4 = [[None, None] for _ in range(3)]
    for cr in range(2):
        c = core if cr == 0 else other

        def rows_step(i, carry, c=c):
            rows = 2 * RING * RING * CAP
            xs = [rec[k][c, pl.ds(2 * i, 2)].reshape(rows, widths[k]) for k in range(3)]

            for f in range(fdim // f_tile):
                cols = slice(f * f_tile, (f + 1) * f_tile)
                hg = sum(jnp.dot(xs[k], w1[offs[k]:offs[k] + widths[k], cols], preferred_element_type=F32) for k in range(3))
                hu = sum(jnp.dot(xs[k], w3[offs[k]:offs[k] + widths[k], cols], preferred_element_type=F32) for k in range(3))
                act[:, cols] = (hg * jax.nn.sigmoid(hg) * hu).astype(BF16)
            a = act[...]
            for k in range(3):
                o = jnp.dot(a, w2[:, offs[k]:offs[k] + widths[k]], preferred_element_type=F32).astype(BF16)
                til[k][c, pl.ds(2 * i, 2)] = o.reshape(2, RING, RING, CAP, widths[k])
            return carry

        lax.fori_loop(0, 2, rows_step, 0)
        for k in range(3):
            def keep(k=k):
                if k == 0:
                    v = til[k][core, p3[k]]
                elif k == 1:
                    v = til[k][core, :, p3[k]]
                else:
                    v = til[k][core, :, :, p3[k]]
                gat[k][core, p3[k]] = v
            sblock = lambda ref, cc, d, half, k=k: sub(ref, k, cc, d, half)
            x4[k][cr] = exchange_start(k, cr, til[k], sblock, gat[k], til_block, pas4[k], keep)
    for k in range(3):
        for i, d in enumerate(DIRS):
            pl.semaphore_signal(credit.at[k, i], inc=1, device_id=peer(D1[k], d, core), device_id_type=MESH)
    for cr in range(2):
        for k in range(3):
            exchange_forward(k, cr, *x4[k][cr], gat[k], til_block, pas4[k])

    for k in range(3):
        def weights(i, carry, k=k):
            mrow = meta[k][i, p1[k]]
            ids, gates = mrow[0:8], mrow[8:16]
            own = pos[D2[k]] * strides[D2[k]]
            ms, gs = [], []
            for b in range(4):
                idx = i8 + b * 8
                d3e, d1e, ce = idx & 3, (idx >> 2) & 3, idx >> 4
                evec = (own + d3e * stride3[k] + d1e * strides[D1[k]] + ce * (RING * RING)).astype(F32)
                m = jnp.zeros((8, TOK), F32)
                g = jnp.zeros((8, TOK), F32)
                for j in range(8):
                    hit = ids[j:j + 1, :] == evec
                    m = m + hit.astype(F32)
                    g = g + jnp.where(hit, gates[j:j + 1, :], 0.0)
                ms.append(m)
                gs.append(g)
            rm = rank_of(jnp.concatenate(ms, axis=0))
            for b in range(4):
                hot = jnp.where(rm[b * 8:(b + 1) * 8][:, None, :] == slot, gs[b][:, None, :], 0.0).reshape(TOK, TOK).T
                hi = hot.astype(BF16)
                r1 = hot - hi.astype(F32)
                mid = r1.astype(BF16)
                lo = (r1 - mid.astype(F32)).astype(BF16)
                comb[k][i, b, 0] = hi
                comb[k][i, b, 1] = mid
                comb[k][i, b, 2] = lo
            return carry

        lax.fori_loop(0, 4, weights, 0)

    def from_src(ref, k, d, half=None):
        cs = slice(None) if half is None else half
        return ref.at[cs, :, d] if A_IS_D1[k] else ref.at[cs, :, :, d]

    x5 = [None] * 3
    for k in range(3):
        for cr in range(2):
            first, direct = x4[k][cr]
            for cp in direct:
                cp.wait_recv()
        for i in range(2):
            pl.semaphore_wait(credit.at[k, i], 1)
        first, direct = [], []
        for i, d in enumerate(DIRS):
            cp = rcopy(from_src(gat[k], k, mod(p1[k] + 2), i), pas5[k].at[i], peer(D1[k], d, core))
            cp.start()
            first.append(cp)
        for i, d in enumerate(DIRS):
            cp = rcopy(from_src(gat[k], k, mod(p1[k] + d)), rec[k].at[:, p1[k]], peer(D1[k], d, core))
            cp.start()
            direct.append(cp)
        if A_IS_D1[k]:
            rec[k][:, p1[k]] = gat[k][:, :, p1[k]]
        else:
            rec[k][:, p1[k]] = gat[k][:, :, :, p1[k]]
        x5[k] = (first, direct)
    for k in range(3):
        first, direct = x5[k]
        for i, d in enumerate(DIRS):
            first[i].wait_recv()
            cp = rcopy(pas5[k].at[i], rec[k].at[i, mod(p1[k] - d)], peer(D1[k], d, core))
            cp.start()
            direct.append(cp)

    x6 = [None] * 3
    for k in range(3):
        first, direct = x5[k]
        for cp in direct:
            cp.wait_recv()
        w = widths[k]

        def combine(i, carry, k=k, w=w):
            acc = jnp.zeros((TOK, w), F32)
            for b in range(4):
                o = rec[k][b // 2, pl.ds(2 * (b % 2), 2), :, i].reshape(TOK, w)
                for q in range(3):
                    acc = acc + jnp.dot(comb[k][i, b, q], o, preferred_element_type=F32)
            part[k][i] = acc
            return carry

        lax.fori_loop(0, 4, combine, 0)
        first, direct = [], []
        for i, d in enumerate(DIRS):
            cp = rcopy(part[k].at[mod(p2[k] + 2), pl.ds(i * (TOK // 2), TOK // 2)], pas6[k].at[i], peer(D2[k], d, core))
            cp.start()
            first.append(cp)
        for i, d in enumerate(DIRS):
            cp = rcopy(part[k].at[mod(p2[k] + d)], prec[k].at[i], peer(D2[k], d, core))
            cp.start()
            direct.append(cp)
        x6[k] = (first, direct)
    for k in range(3):
        first, direct = x6[k]
        for i, d in enumerate(DIRS):
            first[i].wait_recv()
            cp = rcopy(pas6[k].at[i], prec[k].at[2, pl.ds(i * (TOK // 2), TOK // 2)], peer(D2[k], d, core))
            cp.start()
            direct.append(cp)
    for k in range(3):
        first, direct = x6[k]
        for cp in direct:
            cp.wait_recv()
        total = part[k][p2[k]] + prec[k][0] + prec[k][1] + prec[k][2]
        xk = x_ref[:, :, :, offs[k]:offs[k] + widths[k]].reshape(TOK, widths[k]).astype(F32)
        y_ref[:, offs[k]:offs[k] + widths[k]] = (xk + total).astype(BF16)
    for k in range(3):
        for cp in x4[k][0][0] + x4[k][0][1] + x4[k][1][0] + x4[k][1][1] + x5[k][0] + x5[k][1] + x6[k][0] + x6[k][1]:
            cp.wait_send()


N_COPIES = 3 * (7 + 15 + 14 + 14 + 6 + 6)


def solution(mesh):
    def local_layer(x_loc, ids_loc, gates_loc, w_g, w_u, w_d):
        tok, hid = x_loc.shape
        fdim = w_g.shape[2]
        widths = split_width(hid)
        f_tile = 256 if fdim % 256 == 0 else fdim
        meta = jnp.concatenate([ids_loc.T.astype(F32), gates_loc.T], axis=0)
        x4 = x_loc.reshape(CORES, RING, CAP, hid)
        scratch = []
        each = lambda f: scratch.extend(f(w) for w in widths)
        for _ in range(3):
            each(lambda w: pltpu.VMEM(LEAD + (CAP, w), BF16))
        each(lambda w: pltpu.VMEM((RING, RING, 16, TOK), F32))
        each(lambda w: pltpu.VMEM((RING, RING, TOK, TOK), BF16))
        each(lambda w: pltpu.VMEM((RING, 4, 3, TOK, TOK), BF16))
        each(lambda w: pltpu.VMEM((2, CORES, 2, RING, CAP, w), BF16))
        each(lambda w: pltpu.VMEM((2, CORES, 2, RING, CAP, w), BF16))
        each(lambda w: pltpu.VMEM((2, RING, RING, CAP, w), BF16))
        each(lambda w: pltpu.VMEM((RING, TOK, w), F32))
        each(lambda w: pltpu.VMEM((3, TOK, w), F32))
        each(lambda w: pltpu.VMEM((2, TOK // 2, w), F32))
        scratch += [
            pltpu.VMEM((hid, fdim), BF16),
            pltpu.VMEM((hid, fdim), BF16),
            pltpu.VMEM((fdim, hid), BF16),
            pltpu.VMEM((2 * RING * RING * CAP, fdim), BF16),
            pltpu.SemaphoreType.DMA((N_COPIES,)),
            pltpu.SemaphoreType.DMA((N_COPIES,)),
            pltpu.SemaphoreType.DMA((3,)),
            pltpu.SemaphoreType.REGULAR((3, 2)),
        ]
        vm = pl.BlockSpec(memory_space=pltpu.VMEM)
        hbm = pl.BlockSpec(memory_space=pl.ANY)
        return pl.pallas_call(
            functools.partial(moe_kernel, widths, fdim, f_tile),
            out_shape=jax.ShapeDtypeStruct((tok, hid), BF16),
            in_specs=[vm, vm, hbm, hbm, hbm],
            out_specs=vm,
            scratch_shapes=scratch,
            compiler_params=pltpu.CompilerParams(collective_id=0, has_side_effects=True, vmem_limit_bytes=67043328),
            name='moe',
        )(x4, meta, w_g[0], w_u[0], w_d[0])

    tok_spec = P(TOKEN_AXES, None)
    w_spec = P(EXPERT_AXES, None, None)
    return jax.shard_map(local_layer, mesh=mesh, in_specs=(tok_spec, tok_spec, tok_spec, w_spec, w_spec, w_spec), out_specs=tok_spec, check_vma=False)
```

```python
import functools

import jax
import jax.numpy as jnp
from jax import lax
from jax.experimental import pallas as pl
from jax.experimental.pallas import tpu as pltpu
from jax.sharding import PartitionSpec as P

TOKEN_AXES = ('ez', 'ey', 'ex')
EXPERT_AXES = ('ex', 'ey', 'ez')
MESH = pl.DeviceIdType.MESH
F32 = jnp.float32
BF16 = jnp.bfloat16

Z, Y, X = 0, 1, 2
D1 = (Y, Z, X)
D2 = (Z, X, Y)
D3 = (X, Y, Z)
A_IS_D1 = (True, False, True)
RING = 4
CORES = 2
CAP = 16
TOK = 128
LEAD = (CORES, RING, RING, RING)


NQ = 6
W1, W2 = (0, 1, 2), (3, 4, 5)


def split_width(hid):
    tiles = hid // 128
    return tuple((tiles * (i + 1) // NQ - tiles * i // NQ) * 128 for i in ORDER)


ORDER = (1, 2, 4, 5, 0, 3)


def moe_kernel(widths, fdim, f_tile, x_ref, meta_ref, w1_hbm, w3_hbm, w2_hbm, y_ref, *scr):
    it = iter(scr)
    take = lambda n: [next(it) for _ in range(n)]
    gat, til, rec = take(NQ), take(NQ), take(NQ)
    meta, sel, comb = take(3), take(3), take(3)
    pas3, pas4, pas5 = take(NQ), take(NQ), take(NQ)
    part, prec, pas6 = take(NQ), take(NQ), take(NQ)
    w1, w3, w2, act = take(4)
    send_sem, recv_sem, w_sem, credit = take(4)

    offs = [sum(widths[:q]) for q in range(NQ)]
    ez, ey, ex = lax.axis_index('ez'), lax.axis_index('ey'), lax.axis_index('ex')
    core = lax.rem(ex, CORES)
    pos = (ez, ey, ex // CORES)
    mod = lambda v: lax.rem(v + RING, RING)
    other = 1 - core

    def peer(dim, off, c):
        q = [mod(pos[d] + off) if d == dim else pos[d] for d in range(3)]
        return (q[0], q[1], q[2] * CORES + c)

    counter = [0]

    def send(src, dst, dev):
        i = counter[0]
        counter[0] += 1
        cp = pltpu.make_async_remote_copy(src, dst, send_sem.at[i], recv_sem.at[i], device_id=dev, device_id_type=MESH)
        cp.start()
        return cp

    bar = pltpu.get_barrier_semaphore()
    npeer = 0
    for dim in range(3):
        for off in (1, -1):
            for c in (core, other):
                pl.semaphore_signal(bar, inc=1, device_id=peer(dim, off, c), device_id_type=MESH)
                npeer += 1
    pl.semaphore_signal(bar, inc=1, device_id=peer(0, 0, other), device_id_type=MESH)
    w_copies = [pltpu.make_async_copy(s, d, w_sem.at[i]) for i, (s, d) in enumerate(((w1_hbm, w1), (w3_hbm, w3), (w2_hbm, w2)))]
    pl.semaphore_wait(bar, npeer + 1)

    DIRS = (1, -1)
    d1 = [D1[q % 3] for q in range(NQ)]
    d2 = [D2[q % 3] for q in range(NQ)]
    d3 = [D3[q % 3] for q in range(NQ)]
    a1 = [A_IS_D1[q % 3] for q in range(NQ)]
    p1 = [pos[d] for d in d1]
    p2 = [pos[d] for d in d2]
    p3 = [pos[d] for d in d3]
    xcol = [x_ref.at[:, :, :, pl.ds(offs[q], widths[q])] for q in range(NQ)]
    unwaited = []

    def chunk(q, r):
        return gat[q].at[:, :, p2[q], mod(p1[q] + r)]

    m1 = [[None, None] for _ in range(3)]
    mf1 = [None] * 3
    m2 = [[None, None] for _ in range(3)]
    mf2 = [None] * 3
    g1 = [[None, None] for _ in range(NQ)]
    f1 = [[None, None] for _ in range(NQ)]
    g2 = [[[None] * 4, [None] * 4] for _ in range(NQ)]
    f2 = [[None] * 4 for _ in range(NQ)]

    def first_sends(wave):
        for q in wave:
            for i, d in enumerate(DIRS):
                if q < 3:
                    m1[q][i] = send(meta_ref, meta[q].at[p2[q], p1[q]], peer(d1[q], d, core))
                g1[q][i] = send(xcol[q], chunk(q, 0), peer(d1[q], d, core))
        for q in wave:
            for i, d in enumerate(DIRS):
                g2[q][i][0] = send(xcol[q], chunk(q, 0), peer(d2[q], d, core))

    def first_forwards(wave):
        for q in wave:
            for i, d in enumerate(DIRS):
                if q < 3:
                    m1[q][i].wait_recv()
                    if i == 0:
                        src = meta[q].at[p2[q], mod(p1[q] - 1)]
                        mf1[q] = send(src, src, peer(d1[q], 1, core))
                g1[q][i].wait_recv()
                half = chunk(q, -d).at[i]
                f1[q][i] = send(half, half, peer(d1[q], d, core))
        for q in wave:
            for i, d in enumerate(DIRS):
                for r in (1, 3):
                    g2[q][i][r] = send(chunk(q, r), chunk(q, r), peer(d2[q], d, core))

    def forward2(q, i, r):
        g2[q][i][r].wait_recv()
        src = gat[q].at[:, :, mod(p2[q] - DIRS[i]), mod(p1[q] + r)]
        f2[q][r] = send(src, src, peer(d2[q], DIRS[i], core))

    first_sends(W1)
    first_sends(W2)
    for c in w_copies:
        c.start()
    for q in range(NQ):
        gat[q][:, :, p2[q], p1[q]] = x_ref[:, :, :, offs[q]:offs[q] + widths[q]]
    for k in range(3):
        meta[k][p2[k], p1[k]] = meta_ref[...]
    first_forwards(W1)
    for k in range(3):
        mf1[k].wait_recv()
        for i, d in enumerate(DIRS):
            row = meta[k].at[p2[k]]
            m2[k][i] = send(row, row, peer(d2[k], d, core))
    first_forwards(W2)
    for q in W1 + W2:
        forward2(q, 0, 0)
        for i, d in enumerate(DIRS):
            f1[q][i].wait_recv()
        for i, d in enumerate(DIRS):
            g2[q][i][2] = send(chunk(q, 2), chunk(q, 2), peer(d2[q], d, core))
    for k in range(3):
        for i in range(2):
            m2[k][i].wait_recv()
        src = meta[k].at[mod(p2[k] - 1)]
        mf2[k] = send(src, src, peer(d2[k], 1, core))

    tri = (lax.broadcasted_iota(jnp.int32, (TOK, TOK), 0) < lax.broadcasted_iota(jnp.int32, (TOK, TOK), 1)).astype(BF16)
    i8 = lax.broadcasted_iota(jnp.int32, (8, 1), 0)
    stride3 = (2 * RING * RING, RING, 1)
    strides = (1, RING, 2 * RING * RING)
    slot = lax.broadcasted_iota(jnp.int32, (8, CAP, TOK), 1).astype(F32)

    def experts8(k):
        base = pos[D1[k]] * strides[D1[k]] + pos[D2[k]] * strides[D2[k]]
        return (base + (i8 & 3) * stride3[k] + (i8 >> 2) * (RING * RING)).astype(F32)

    def picked(ids, evec):
        m = (ids[0:1, :] == evec).astype(F32)
        for j in range(1, 8):
            m = m + (ids[j:j + 1, :] == evec).astype(F32)
        return m

    def rank_of(m):
        rank = jnp.dot(m.astype(BF16), tri, preferred_element_type=F32)
        return jnp.where(m > 0.5, rank, -1.0)

    def onehot(k, i):
        evec = experts8(k)
        rm = rank_of(jnp.concatenate([picked(meta[k][i, j, 0:8], evec) for j in range(4)], axis=0))
        for j in range(4):
            hot = (rm[j * 8:(j + 1) * 8][:, None, :] == slot).astype(F32)
            sel[k][i, j] = hot.reshape(TOK, TOK).astype(BF16)

    def select(q, i):
        k, w = q % 3, widths[q]
        for j in range(4):
            rows = gat[q][:, :, i, j].reshape(TOK, w)
            out = jnp.dot(sel[k][i, j], rows, preferred_element_type=F32).astype(BF16).reshape(CORES, RING, CAP, w)
            if a1[q]:
                til[q][:, :, j, i] = out
            else:
                til[q][:, :, i, j] = out

    def loop(n, f):
        def body(i, carry):
            f(i)
            return carry
        lax.fori_loop(0, n, body, 0)

    for k in range(3):
        onehot(k, p2[k])
    for q in W1 + W2:
        select(q, p2[q])
    for q in W1:
        forward2(q, 0, 1)
        forward2(q, 1, 3)
    for k in range(3):
        mf2[k].wait_recv()
        loop(3, lambda i, k=k: onehot(k, mod(p2[k] + 1 + i)))
    for q in W2:
        forward2(q, 0, 1)
        forward2(q, 1, 3)
    for q in W1 + W2:
        forward2(q, 1, 2)

    def gathered(q, near):
        if near:
            for i, r in ((0, 2), (0, 3), (1, 0), (1, 1)):
                g2[q][i][r].wait_recv()
            loop(2, lambda i, q=q: select(q, mod(p2[q] - 1 + 2 * i)))
        else:
            for r in range(4):
                f2[q][r].wait_recv()
            select(q, mod(p2[q] + 2))
            done = g1[q] + f1[q] + g2[q][0] + g2[q][1] + f2[q]
            if q < 3:
                done = done + m1[q] + [mf1[q]] + m2[q] + [mf2[q]]
            for c in done:
                c.wait_send()

    def sub(ref, q, c, d, half=None):
        a = slice(None) if half is None else pl.ds(2 * half, 2)
        return (ref.at[c, d, a], ref.at[c, a, d], ref.at[c, a, :, d])[q % 3]

    def til_block(ref, q, c, d, half=None):
        return ref.at[c, d] if half is None else ref.at[c, d, pl.ds(2 * half, 2)]

    class Leg:
        def __init__(self, q, cr, src, src_block, dst, dst_block, pas):
            self.a = (q, cr, src, src_block, dst, dst_block, pas)
            self.c = core if cr == 0 else other
            self.first, self.direct = [], []

        def far(self):
            q, cr, src, src_block, dst, dst_block, pas = self.a
            for i, d in enumerate(DIRS):
                self.first.append(send(src_block(src, q, self.c, mod(p3[q] + 2), i), pas.at[i, cr], peer(d3[q], d, core)))

        def near(self):
            q, cr, src, src_block, dst, dst_block, pas = self.a
            for i, d in enumerate(DIRS):
                self.direct.append(send(src_block(src, q, self.c, mod(p3[q] + d)), dst_block(dst, q, core, p3[q]), peer(d3[q], d, self.c)))
            if cr == 1:
                self.direct.append(send(src_block(src, q, self.c, p3[q]), dst_block(dst, q, core, p3[q]), peer(d3[q], 0, other)))

        def forward(self):
            q, cr, src, src_block, dst, dst_block, pas = self.a
            for i, d in enumerate(DIRS):
                self.first[i].wait_recv()
                self.direct.append(send(pas.at[i, cr], dst_block(dst, q, core, mod(p3[q] - d), i), peer(d3[q], d, self.c)))

        def arrive(self):
            for cp in self.direct:
                cp.wait_recv()

        def sent(self):
            for cp in self.first + self.direct:
                cp.wait_send()

    def keep3(q):
        v = til[q][core, p3[q]]
        if q % 3 == 0:
            rec[q][core, p3[q]] = v
        elif q % 3 == 1:
            rec[q][core, :, p3[q]] = v
        else:
            rec[q][core, :, :, p3[q]] = v

    def keep4(q):
        if q % 3 == 0:
            v = til[q][core, p3[q]]
        elif q % 3 == 1:
            v = til[q][core, :, p3[q]]
        else:
            v = til[q][core, :, :, p3[q]]
        gat[q][core, p3[q]] = v

    x3 = [[Leg(q, cr, til[q], til_block, rec[q], sub, pas3[q]) for cr in range(2)] for q in range(NQ)]
    for q in W1:
        gathered(q, True)
    for q in W1:
        gathered(q, False)
        for cr in range(2):
            x3[q][cr].far()
        for cr in range(2):
            x3[q][cr].near()
    for q in W2:
        gathered(q, True)
    for q in W2:
        gathered(q, False)
        for cr in range(2):
            x3[q][cr].far()
    for q in W1:
        for cr in range(2):
            x3[q][cr].forward()
    for q in W2:
        for cr in range(2):
            x3[q][cr].near()
    for q in W1 + W2:
        keep3(q)
    for q in W2:
        for cr in range(2):
            x3[q][cr].forward()
    for c in w_copies:
        c.wait()
    for q in range(NQ):
        for cr in range(2):
            x3[q][cr].arrive()
    for q in range(NQ):
        for cr in range(2):
            x3[q][cr].sent()

    x4 = [[Leg(q, cr, til[q], sub, gat[q], til_block, pas4[q]) for cr in range(2)] for q in range(NQ)]
    rows = 2 * RING * RING * CAP
    for cr in range(2):
        c = core if cr == 0 else other

        def hidden(i, c=c):
            xs = [rec[q][c, pl.ds(2 * i, 2)].reshape(rows, widths[q]) for q in range(NQ)]
            for f in range(fdim // f_tile):
                cols = slice(f * f_tile, (f + 1) * f_tile)
                hg = sum(jnp.dot(xs[q], w1[offs[q]:offs[q] + widths[q], cols], preferred_element_type=F32) for q in range(NQ))
                hu = sum(jnp.dot(xs[q], w3[offs[q]:offs[q] + widths[q], cols], preferred_element_type=F32) for q in range(NQ))
                act[i, :, cols] = (hg * jax.nn.sigmoid(hg) * hu).astype(BF16)

        def down(wave, c=c):
            def step(i):
                for q in wave:
                    o = jnp.dot(act[i], w2[:, offs[q]:offs[q] + widths[q]], preferred_element_type=F32).astype(BF16)
                    til[q][c, pl.ds(2 * i, 2)] = o.reshape(2, RING, RING, CAP, widths[q])
            loop(2, step)

        loop(2, hidden)
        down(W1)
        if cr == 1:
            for q in W1 + W2:
                x4[q][0].forward()
        for q in W1:
            x4[q][cr].far()
        for q in W1:
            x4[q][cr].near()
        down(W2)
        for q in W2:
            x4[q][cr].far()
        if cr == 1:
            for q in W1:
                x4[q][1].forward()
        for q in W2:
            x4[q][cr].near()
        if cr == 0:
            for q in W1 + W2:
                keep4(q)
    for k in range(3):
        for i, d in enumerate(DIRS):
            pl.semaphore_signal(credit.at[k, i], inc=1, device_id=peer(D1[k], d, core), device_id_type=MESH)

    def weights(k, i):
        mrow = meta[k][i, p1[k]]
        ids, gates = mrow[0:8], mrow[8:16]
        own = pos[D2[k]] * strides[D2[k]]
        ms, gs = [], []
        for b in range(4):
            idx = i8 + b * 8
            d3e, d1e, ce = idx & 3, (idx >> 2) & 3, idx >> 4
            evec = (own + d3e * stride3[k] + d1e * strides[D1[k]] + ce * (RING * RING)).astype(F32)
            m = jnp.zeros((8, TOK), F32)
            g = jnp.zeros((8, TOK), F32)
            for j in range(8):
                hit = ids[j:j + 1, :] == evec
                m = m + hit.astype(F32)
                g = g + jnp.where(hit, gates[j:j + 1, :], 0.0)
            ms.append(m)
            gs.append(g)
        rm = rank_of(jnp.concatenate(ms, axis=0))
        for b in range(4):
            hot = jnp.where(rm[b * 8:(b + 1) * 8][:, None, :] == slot, gs[b][:, None, :], 0.0).reshape(TOK, TOK).T
            hi = hot.astype(BF16)
            r1 = hot - hi.astype(F32)
            mid = r1.astype(BF16)
            lo = (r1 - mid.astype(F32)).astype(BF16)
            comb[k][i, b, 0] = hi
            comb[k][i, b, 1] = mid
            comb[k][i, b, 2] = lo

    for q in W2:
        x4[q][1].forward()
    for k in range(3):
        loop(4, lambda i, k=k: weights(k, i))

    def from_src(ref, q, d, half=None):
        cs = slice(None) if half is None else half
        return ref.at[cs, :, d] if a1[q] else ref.at[cs, :, :, d]

    x5 = [([], []) for _ in range(NQ)]

    def arrive4(q):
        for cr in range(2):
            x4[q][cr].arrive()
        if q < 3:
            for i in range(2):
                pl.semaphore_wait(credit.at[q, i], 1)

    def far5(q):
        for i, d in enumerate(DIRS):
            x5[q][0].append(send(from_src(gat[q], q, mod(p1[q] + 2), i), pas5[q].at[i], peer(d1[q], d, core)))

    def near5(q):
        for i, d in enumerate(DIRS):
            x5[q][1].append(send(from_src(gat[q], q, mod(p1[q] + d)), rec[q].at[:, p1[q]], peer(d1[q], d, core)))

    def keep5(q):
        if a1[q]:
            rec[q][:, p1[q]] = gat[q][:, :, p1[q]]
        else:
            rec[q][:, p1[q]] = gat[q][:, :, :, p1[q]]

    def forward5(q):
        for i, d in enumerate(DIRS):
            x5[q][0][i].wait_recv()
            x5[q][1].append(send(pas5[q].at[i], rec[q].at[i, mod(p1[q] - d)], peer(d1[q], d, core)))

    for q in W1:
        arrive4(q)
        far5(q)
        near5(q)
    for q in W1:
        keep5(q)
    for q in W2:
        arrive4(q)
        far5(q)
    for q in W1:
        forward5(q)
    for q in W2:
        near5(q)
    for q in W2:
        keep5(q)
    for q in W2:
        forward5(q)

    x6 = [([], []) for _ in range(NQ)]
    half_tok = TOK // 2

    def combine(q):
        for cp in x5[q][1]:
            cp.wait_recv()
        k, w = q % 3, widths[q]

        def step(i):
            acc = jnp.zeros((TOK, w), F32)
            for b in range(4):
                o = rec[q][b // 2, pl.ds(2 * (b % 2), 2), :, i].reshape(TOK, w)
                for t in range(3):
                    acc = acc + jnp.dot(comb[k][i, b, t], o, preferred_element_type=F32)
            part[q][i] = acc

        loop(4, step)

    def far6(q):
        for i, d in enumerate(DIRS):
            x6[q][0].append(send(part[q].at[mod(p2[q] + 2), pl.ds(i * half_tok, half_tok)], pas6[q].at[i], peer(d2[q], d, core)))

    def near6(q):
        for i, d in enumerate(DIRS):
            x6[q][1].append(send(part[q].at[mod(p2[q] + d)], prec[q].at[i], peer(d2[q], d, core)))

    def forward6(q):
        for i, d in enumerate(DIRS):
            x6[q][0][i].wait_recv()
            x6[q][1].append(send(pas6[q].at[i], prec[q].at[2, pl.ds(i * half_tok, half_tok)], peer(d2[q], d, core)))

    def final(q):
        for cp in x6[q][1]:
            cp.wait_recv()
        total = part[q][p2[q]] + prec[q][0] + prec[q][1] + prec[q][2]
        xk = x_ref[:, :, :, offs[q]:offs[q] + widths[q]].reshape(TOK, widths[q]).astype(F32)
        y_ref[:, offs[q]:offs[q] + widths[q]] = (xk + total).astype(BF16)

    for q in W1:
        combine(q)
        far6(q)
        near6(q)
    for q in W2:
        combine(q)
        far6(q)
    for q in W1:
        forward6(q)
    for q in W2:
        near6(q)
    for q in W2:
        forward6(q)
    for q in W1 + W2:
        final(q)
    for q in range(NQ):
        for cr in range(2):
            x4[q][cr].sent()
        for cp in x5[q][0] + x5[q][1] + x6[q][0] + x6[q][1]:
            cp.wait_send()


N_COPIES = 3 * 7 + NQ * (16 + 14 + 14 + 6 + 6)


def solution(mesh):
    def local_layer(x_loc, ids_loc, gates_loc, w_g, w_u, w_d):
        tok, hid = x_loc.shape
        fdim = w_g.shape[2]
        widths = split_width(hid)
        f_tile = 256 if fdim % 256 == 0 else fdim
        meta = jnp.concatenate([ids_loc.T.astype(F32), gates_loc.T], axis=0)
        x4 = x_loc.reshape(CORES, RING, CAP, hid)
        scratch = []
        each = lambda f: scratch.extend(f(w) for w in widths)
        for _ in range(3):
            each(lambda w: pltpu.VMEM(LEAD + (CAP, w), BF16))
        scratch += [pltpu.VMEM((RING, RING, 16, TOK), F32)] * 3
        scratch += [pltpu.VMEM((RING, RING, TOK, TOK), BF16)] * 3
        scratch += [pltpu.VMEM((RING, 4, 3, TOK, TOK), BF16)] * 3
        each(lambda w: pltpu.VMEM((2, CORES, 2, RING, CAP, w), BF16))
        each(lambda w: pltpu.VMEM((2, CORES, 2, RING, CAP, w), BF16))
        each(lambda w: pltpu.VMEM((2, RING, RING, CAP, w), BF16))
        each(lambda w: pltpu.VMEM((RING, TOK, w), F32))
        each(lambda w: pltpu.VMEM((3, TOK, w), F32))
        each(lambda w: pltpu.VMEM((2, TOK // 2, w), F32))
        scratch += [
            pltpu.VMEM((hid, fdim), BF16),
            pltpu.VMEM((hid, fdim), BF16),
            pltpu.VMEM((fdim, hid), BF16),
            pltpu.VMEM((2, 2 * RING * RING * CAP, fdim), BF16),
            pltpu.SemaphoreType.DMA((N_COPIES,)),
            pltpu.SemaphoreType.DMA((N_COPIES,)),
            pltpu.SemaphoreType.DMA((3,)),
            pltpu.SemaphoreType.REGULAR((3, 2)),
        ]
        vm = pl.BlockSpec(memory_space=pltpu.VMEM)
        hbm = pl.BlockSpec(memory_space=pl.ANY)
        return pl.pallas_call(
            functools.partial(moe_kernel, widths, fdim, f_tile),
            out_shape=jax.ShapeDtypeStruct((tok, hid), BF16),
            in_specs=[vm, vm, hbm, hbm, hbm],
            out_specs=vm,
            scratch_shapes=scratch,
            compiler_params=pltpu.CompilerParams(collective_id=0, has_side_effects=True, vmem_limit_bytes=67043328),
            name='moe',
        )(x4, meta, w_g[0], w_u[0], w_d[0])

    tok_spec = P(TOKEN_AXES, None)
    w_spec = P(EXPERT_AXES, None, None)
    return jax.shard_map(local_layer, mesh=mesh, in_specs=(tok_spec, tok_spec, tok_spec, w_spec, w_spec, w_spec), out_specs=tok_spec, check_vma=False)
```

```python
import functools

import jax
import jax.numpy as jnp
from jax import lax
from jax.experimental import pallas as pl
from jax.experimental.pallas import tpu as pltpu
from jax.sharding import PartitionSpec as P

TOKEN_AXES = ('ez', 'ey', 'ex')
EXPERT_AXES = ('ex', 'ey', 'ez')
MESH = pl.DeviceIdType.MESH
F32 = jnp.float32
BF16 = jnp.bfloat16

Z, Y, X = 0, 1, 2
D1 = (Y, Z, X)
D2 = (Z, X, Y)
D3 = (X, Y, Z)
A_IS_D1 = (True, False, True)
RING = 4
CORES = 2
CAP = 16
TOK = 128
LEAD = (CORES, RING, RING, RING)


NQ = 6
W1, W2 = (0, 1, 2), (3, 4, 5)


def split_width(hid):
    tiles = hid // 128
    return tuple((tiles * (i + 1) // NQ - tiles * i // NQ) * 128 for i in ORDER)


ORDER = (1, 2, 4, 5, 0, 3)


def moe_kernel(widths, fdim, f_tile, x_ref, meta_ref, w1_hbm, w3_hbm, w2_hbm, y_ref, *scr):
    it = iter(scr)
    take = lambda n: [next(it) for _ in range(n)]
    gat, til, rec = take(NQ), take(NQ), take(NQ)
    meta, sel, comb = take(3), take(3), take(3)
    pas3, pas4, pas5 = take(NQ), take(NQ), take(NQ)
    part, prec, pas6 = take(NQ), take(NQ), take(NQ)
    w1, w3, w2, act = take(4)
    send_sem, recv_sem, w_sem, credit = take(4)

    offs = [sum(widths[:q]) for q in range(NQ)]
    ez, ey, ex = lax.axis_index('ez'), lax.axis_index('ey'), lax.axis_index('ex')
    core = lax.rem(ex, CORES)
    pos = (ez, ey, ex // CORES)
    mod = lambda v: lax.rem(v + RING, RING)
    other = 1 - core

    def peer(dim, off, c):
        q = [mod(pos[d] + off) if d == dim else pos[d] for d in range(3)]
        return (q[0], q[1], q[2] * CORES + c)

    counter = [0]

    def send(src, dst, dev):
        i = counter[0]
        counter[0] += 1
        cp = pltpu.make_async_remote_copy(src, dst, send_sem.at[i], recv_sem.at[i], device_id=dev, device_id_type=MESH)
        cp.start()
        return cp

    bar = pltpu.get_barrier_semaphore()
    npeer = 0
    for dim in range(3):
        for off in (1, -1):
            for c in (core, other):
                pl.semaphore_signal(bar, inc=1, device_id=peer(dim, off, c), device_id_type=MESH)
                npeer += 1
    pl.semaphore_signal(bar, inc=1, device_id=peer(0, 0, other), device_id_type=MESH)
    w_copies = [pltpu.make_async_copy(s, d, w_sem.at[i]) for i, (s, d) in enumerate(((w1_hbm, w1), (w3_hbm, w3), (w2_hbm, w2)))]
    pl.semaphore_wait(bar, npeer + 1)

    DIRS = (1, -1)
    d1 = [D1[q % 3] for q in range(NQ)]
    d2 = [D2[q % 3] for q in range(NQ)]
    d3 = [D3[q % 3] for q in range(NQ)]
    a1 = [A_IS_D1[q % 3] for q in range(NQ)]
    p1 = [pos[d] for d in d1]
    p2 = [pos[d] for d in d2]
    p3 = [pos[d] for d in d3]
    xcol = [x_ref.at[:, :, :, pl.ds(offs[q], widths[q])] for q in range(NQ)]
    unwaited = []

    def chunk(q, r):
        return gat[q].at[:, :, p2[q], mod(p1[q] + r)]

    m1 = [[None, None] for _ in range(3)]
    mf1 = [None] * 3
    m2 = [[None, None] for _ in range(3)]
    mf2 = [None] * 3
    g1 = [[None, None] for _ in range(NQ)]
    f1 = [[None, None] for _ in range(NQ)]
    g2 = [[[None] * 4, [None] * 4] for _ in range(NQ)]
    f2 = [[None] * 4 for _ in range(NQ)]

    def first_sends(wave):
        for q in wave:
            for i, d in enumerate(DIRS):
                if q < 3:
                    m1[q][i] = send(meta_ref, meta[q].at[p2[q], p1[q]], peer(d1[q], d, core))
                g1[q][i] = send(xcol[q], chunk(q, 0), peer(d1[q], d, core))
        for q in wave:
            for i, d in enumerate(DIRS):
                g2[q][i][0] = send(xcol[q], chunk(q, 0), peer(d2[q], d, core))

    def first_forwards(wave):
        for q in wave:
            for i, d in enumerate(DIRS):
                if q < 3:
                    m1[q][i].wait_recv()
                    if i == 0:
                        src = meta[q].at[p2[q], mod(p1[q] - 1)]
                        mf1[q] = send(src, src, peer(d1[q], 1, core))
                g1[q][i].wait_recv()
                half = chunk(q, -d).at[i]
                f1[q][i] = send(half, half, peer(d1[q], d, core))
        for q in wave:
            for i, d in enumerate(DIRS):
                for r in (1, 3):
                    g2[q][i][r] = send(chunk(q, r), chunk(q, r), peer(d2[q], d, core))

    def forward2(q, i, r):
        g2[q][i][r].wait_recv()
        src = gat[q].at[:, :, mod(p2[q] - DIRS[i]), mod(p1[q] + r)]
        f2[q][r] = send(src, src, peer(d2[q], DIRS[i], core))

    first_sends(W1)
    first_sends(W2)
    for c in w_copies:
        c.start()
    for q in range(NQ):
        gat[q][:, :, p2[q], p1[q]] = x_ref[:, :, :, offs[q]:offs[q] + widths[q]]
    for k in range(3):
        meta[k][p2[k], p1[k]] = meta_ref[...]
    first_forwards(W1)
    for k in range(3):
        mf1[k].wait_recv()
        for i, d in enumerate(DIRS):
            row = meta[k].at[p2[k]]
            m2[k][i] = send(row, row, peer(d2[k], d, core))
    first_forwards(W2)
    for q in W1 + W2:
        forward2(q, 0, 0)
        for i, d in enumerate(DIRS):
            f1[q][i].wait_recv()
        for i, d in enumerate(DIRS):
            g2[q][i][2] = send(chunk(q, 2), chunk(q, 2), peer(d2[q], d, core))
    for k in range(3):
        for i in range(2):
            m2[k][i].wait_recv()
        src = meta[k].at[mod(p2[k] - 1)]
        mf2[k] = send(src, src, peer(d2[k], 1, core))

    tri = (lax.broadcasted_iota(jnp.int32, (TOK, TOK), 0) < lax.broadcasted_iota(jnp.int32, (TOK, TOK), 1)).astype(BF16)
    i8 = lax.broadcasted_iota(jnp.int32, (8, 1), 0)
    stride3 = (2 * RING * RING, RING, 1)
    strides = (1, RING, 2 * RING * RING)
    slot = lax.broadcasted_iota(jnp.int32, (8, CAP, TOK), 1).astype(F32)

    def experts8(k):
        base = pos[D1[k]] * strides[D1[k]] + pos[D2[k]] * strides[D2[k]]
        return (base + (i8 & 3) * stride3[k] + (i8 >> 2) * (RING * RING)).astype(F32)

    def picked(ids, evec):
        m = (ids[0:1, :] == evec).astype(F32)
        for j in range(1, 8):
            m = m + (ids[j:j + 1, :] == evec).astype(F32)
        return m

    def rank_of(m):
        rank = jnp.dot(m.astype(BF16), tri, preferred_element_type=F32)
        return jnp.where(m > 0.5, rank, -1.0)

    def onehot(k, i):
        evec = experts8(k)
        rm = rank_of(jnp.concatenate([picked(meta[k][i, j, 0:8], evec) for j in range(4)], axis=0))
        for j in range(4):
            hot = (rm[j * 8:(j + 1) * 8][:, None, :] == slot).astype(F32)
            sel[k][i, j] = hot.reshape(TOK, TOK).astype(BF16)

    def select(q, i):
        k, w = q % 3, widths[q]
        for j in range(4):
            rows = gat[q][:, :, i, j].reshape(TOK, w)
            out = jnp.dot(sel[k][i, j], rows, preferred_element_type=F32).astype(BF16).reshape(CORES, RING, CAP, w)
            if a1[q]:
                til[q][:, :, j, i] = out
            else:
                til[q][:, :, i, j] = out

    def loop(n, f):
        def body(i, carry):
            f(i)
            return carry
        lax.fori_loop(0, n, body, 0)

    for k in range(3):
        onehot(k, p2[k])
    for q in W1 + W2:
        select(q, p2[q])
    for q in W1:
        forward2(q, 0, 1)
        forward2(q, 1, 3)
    for k in range(3):
        mf2[k].wait_recv()
        loop(3, lambda i, k=k: onehot(k, mod(p2[k] + 1 + i)))
    for q in W2:
        forward2(q, 0, 1)
        forward2(q, 1, 3)
    for q in W1 + W2:
        forward2(q, 1, 2)

    def gathered(q, near):
        if near:
            for i, r in ((0, 2), (0, 3), (1, 0), (1, 1)):
                g2[q][i][r].wait_recv()
            loop(2, lambda i, q=q: select(q, mod(p2[q] - 1 + 2 * i)))
        else:
            for r in range(4):
                f2[q][r].wait_recv()
            select(q, mod(p2[q] + 2))
            done = g1[q] + f1[q] + g2[q][0] + g2[q][1] + f2[q]
            if q < 3:
                done = done + m1[q] + [mf1[q]] + m2[q] + [mf2[q]]
            for c in done:
                c.wait_send()

    def sub(ref, q, c, d, half=None):
        a = slice(None) if half is None else pl.ds(2 * half, 2)
        return (ref.at[c, d, a], ref.at[c, a, d], ref.at[c, a, :, d])[q % 3]

    def til_block(ref, q, c, d, half=None):
        return ref.at[c, d] if half is None else ref.at[c, d, pl.ds(2 * half, 2)]

    class Leg:
        def __init__(self, q, cr, src, src_block, dst, dst_block, pas):
            self.a = (q, cr, src, src_block, dst, dst_block, pas)
            self.c = core if cr == 0 else other
            self.first, self.direct = [], []

        def far(self):
            q, cr, src, src_block, dst, dst_block, pas = self.a
            for i, d in enumerate(DIRS):
                self.first.append(send(src_block(src, q, self.c, mod(p3[q] + 2), i), pas.at[i, cr], peer(d3[q], d, core)))

        def near(self):
            q, cr, src, src_block, dst, dst_block, pas = self.a
            for i, d in enumerate(DIRS):
                self.direct.append(send(src_block(src, q, self.c, mod(p3[q] + d)), dst_block(dst, q, core, p3[q]), peer(d3[q], d, self.c)))
            if cr == 1:
                self.direct.append(send(src_block(src, q, self.c, p3[q]), dst_block(dst, q, core, p3[q]), peer(d3[q], 0, other)))

        def forward(self):
            q, cr, src, src_block, dst, dst_block, pas = self.a
            for i, d in enumerate(DIRS):
                self.first[i].wait_recv()
                self.direct.append(send(pas.at[i, cr], dst_block(dst, q, core, mod(p3[q] - d), i), peer(d3[q], d, self.c)))

        def arrive(self):
            for cp in self.direct:
                cp.wait_recv()

        def sent(self):
            for cp in self.first + self.direct:
                cp.wait_send()

    def keep3(q):
        v = til[q][core, p3[q]]
        if q % 3 == 0:
            rec[q][core, p3[q]] = v
        elif q % 3 == 1:
            rec[q][core, :, p3[q]] = v
        else:
            rec[q][core, :, :, p3[q]] = v

    def keep4(q):
        if q % 3 == 0:
            v = til[q][core, p3[q]]
        elif q % 3 == 1:
            v = til[q][core, :, p3[q]]
        else:
            v = til[q][core, :, :, p3[q]]
        gat[q][core, p3[q]] = v

    x3 = [[Leg(q, cr, til[q], til_block, rec[q], sub, pas3[q]) for cr in range(2)] for q in range(NQ)]
    for q in W1:
        gathered(q, True)
    for q in W1:
        gathered(q, False)
        x3[q][0].far()
        x3[q][0].near()
    for q in W2:
        gathered(q, True)
    for q in W2:
        gathered(q, False)
        x3[q][0].far()
    for q in W1:
        x3[q][1].far()
    for q in W1:
        x3[q][0].forward()
    for q in W2:
        x3[q][0].near()
        x3[q][1].far()
    for q in W2:
        x3[q][0].forward()
    for q in W1 + W2:
        x3[q][1].near()
    for q in W1 + W2:
        keep3(q)
    for q in W1 + W2:
        x3[q][1].forward()
    for c in w_copies:
        c.wait()

    x4 = [[Leg(q, cr, til[q], sub, gat[q], til_block, pas4[q]) for cr in range(2)] for q in range(NQ)]
    rows = 2 * RING * RING * CAP
    for cr in range(2):
        c = core if cr == 0 else other
        for q in range(NQ):
            x3[q][cr].arrive()
        for q in range(NQ):
            x3[q][cr].sent()

        def hidden(i, c=c):
            xs = [rec[q][c, pl.ds(2 * i, 2)].reshape(rows, widths[q]) for q in range(NQ)]
            for f in range(fdim // f_tile):
                cols = slice(f * f_tile, (f + 1) * f_tile)
                hg = sum(jnp.dot(xs[q], w1[offs[q]:offs[q] + widths[q], cols], preferred_element_type=F32) for q in range(NQ))
                hu = sum(jnp.dot(xs[q], w3[offs[q]:offs[q] + widths[q], cols], preferred_element_type=F32) for q in range(NQ))
                act[i, :, cols] = (hg * jax.nn.sigmoid(hg) * hu).astype(BF16)

        def down(wave, c=c):
            def step(i):
                for q in wave:
                    o = jnp.dot(act[i], w2[:, offs[q]:offs[q] + widths[q]], preferred_element_type=F32).astype(BF16)
                    til[q][c, pl.ds(2 * i, 2)] = o.reshape(2, RING, RING, CAP, widths[q])
            loop(2, step)

        loop(2, hidden)
        down(W1)
        if cr == 1:
            for q in W1 + W2:
                x4[q][0].forward()
        for q in W1:
            x4[q][cr].far()
        for q in W1:
            x4[q][cr].near()
        down(W2)
        for q in W2:
            x4[q][cr].far()
        if cr == 1:
            for q in W1:
                x4[q][1].forward()
        for q in W2:
            x4[q][cr].near()
        if cr == 0:
            for q in W1 + W2:
                keep4(q)
    for k in range(3):
        for i, d in enumerate(DIRS):
            pl.semaphore_signal(credit.at[k, i], inc=1, device_id=peer(D1[k], d, core), device_id_type=MESH)

    def weights(k, i):
        mrow = meta[k][i, p1[k]]
        ids, gates = mrow[0:8], mrow[8:16]
        own = pos[D2[k]] * strides[D2[k]]
        ms, gs = [], []
        for b in range(4):
            idx = i8 + b * 8
            d3e, d1e, ce = idx & 3, (idx >> 2) & 3, idx >> 4
            evec = (own + d3e * stride3[k] + d1e * strides[D1[k]] + ce * (RING * RING)).astype(F32)
            m = jnp.zeros((8, TOK), F32)
            g = jnp.zeros((8, TOK), F32)
            for j in range(8):
                hit = ids[j:j + 1, :] == evec
                m = m + hit.astype(F32)
                g = g + jnp.where(hit, gates[j:j + 1, :], 0.0)
            ms.append(m)
            gs.append(g)
        rm = rank_of(jnp.concatenate(ms, axis=0))
        for b in range(4):
            hot = jnp.where(rm[b * 8:(b + 1) * 8][:, None, :] == slot, gs[b][:, None, :], 0.0).reshape(TOK, TOK).T
            hi = hot.astype(BF16)
            r1 = hot - hi.astype(F32)
            mid = r1.astype(BF16)
            lo = (r1 - mid.astype(F32)).astype(BF16)
            comb[k][i, b, 0] = hi
            comb[k][i, b, 1] = mid
            comb[k][i, b, 2] = lo

    for q in W2:
        x4[q][1].forward()
    for k in range(3):
        loop(4, lambda i, k=k: weights(k, i))

    def from_src(ref, q, d, half=None):
        cs = slice(None) if half is None else half
        return ref.at[cs, :, d] if a1[q] else ref.at[cs, :, :, d]

    x5 = [([], []) for _ in range(NQ)]

    def arrive4(q):
        for cr in range(2):
            x4[q][cr].arrive()
        if q < 3:
            for i in range(2):
                pl.semaphore_wait(credit.at[q, i], 1)

    def far5(q):
        for i, d in enumerate(DIRS):
            x5[q][0].append(send(from_src(gat[q], q, mod(p1[q] + 2), i), pas5[q].at[i], peer(d1[q], d, core)))

    def near5(q):
        for i, d in enumerate(DIRS):
            x5[q][1].append(send(from_src(gat[q], q, mod(p1[q] + d)), rec[q].at[:, p1[q]], peer(d1[q], d, core)))

    def keep5(q):
        if a1[q]:
            rec[q][:, p1[q]] = gat[q][:, :, p1[q]]
        else:
            rec[q][:, p1[q]] = gat[q][:, :, :, p1[q]]

    def forward5(q):
        for i, d in enumerate(DIRS):
            x5[q][0][i].wait_recv()
            x5[q][1].append(send(pas5[q].at[i], rec[q].at[i, mod(p1[q] - d)], peer(d1[q], d, core)))

    for q in W1:
        arrive4(q)
        far5(q)
        near5(q)
    for q in W1:
        keep5(q)
    for q in W2:
        arrive4(q)
        far5(q)
    for q in W1:
        forward5(q)
    for q in W2:
        near5(q)
    for q in W2:
        keep5(q)
    for q in W2:
        forward5(q)

    x6 = [([], []) for _ in range(NQ)]
    half_tok = TOK // 2

    def combine(q):
        for cp in x5[q][1]:
            cp.wait_recv()
        k, w = q % 3, widths[q]

        def step(i):
            acc = jnp.zeros((TOK, w), F32)
            for b in range(4):
                o = rec[q][b // 2, pl.ds(2 * (b % 2), 2), :, i].reshape(TOK, w)
                for t in range(3):
                    acc = acc + jnp.dot(comb[k][i, b, t], o, preferred_element_type=F32)
            part[q][i] = acc

        loop(4, step)

    def far6(q):
        for i, d in enumerate(DIRS):
            x6[q][0].append(send(part[q].at[mod(p2[q] + 2), pl.ds(i * half_tok, half_tok)], pas6[q].at[i], peer(d2[q], d, core)))

    def rows6(q, i, half):
        return part[q].at[mod(p2[q] + DIRS[i]), pl.ds(half * half_tok, half_tok)], prec[q].at[i, pl.ds(half * half_tok, half_tok)]

    def near6(q):
        for i, d in enumerate(DIRS):
            x6[q][1].append(send(*rows6(q, i, 1 - i), peer(d2[q], d, core)))

    def forward6(q):
        for i, d in enumerate(DIRS):
            x6[q][0][i].wait_recv()
            mine, there = rows6(q, i, i)
            mine[...] = mine[...] + pas6[q][i]
            x6[q][1].append(send(mine, there, peer(d2[q], d, core)))

    def final(q):
        for cp in x6[q][1]:
            cp.wait_recv()
        total = part[q][p2[q]] + prec[q][0] + prec[q][1]
        xk = x_ref[:, :, :, offs[q]:offs[q] + widths[q]].reshape(TOK, widths[q]).astype(F32)
        y_ref[:, offs[q]:offs[q] + widths[q]] = (xk + total).astype(BF16)

    for q in W1:
        combine(q)
        far6(q)
        near6(q)
    for q in W2:
        combine(q)
        far6(q)
    for q in W1:
        forward6(q)
    for q in W2:
        near6(q)
    for q in W2:
        forward6(q)
    for q in W1 + W2:
        final(q)
    for q in range(NQ):
        for cr in range(2):
            x4[q][cr].sent()
        for cp in x5[q][0] + x5[q][1] + x6[q][0] + x6[q][1]:
            cp.wait_send()


N_COPIES = 3 * 6 + NQ * (16 + 13 + 13 + 6 + 6)


def solution(mesh):
    def local_layer(x_loc, ids_loc, gates_loc, w_g, w_u, w_d):
        tok, hid = x_loc.shape
        fdim = w_g.shape[2]
        widths = split_width(hid)
        f_tile = 256 if fdim % 256 == 0 else fdim
        meta = jnp.concatenate([ids_loc.T.astype(F32), gates_loc.T], axis=0)
        x4 = x_loc.reshape(CORES, RING, CAP, hid)
        scratch = []
        each = lambda f: scratch.extend(f(w) for w in widths)
        for _ in range(3):
            each(lambda w: pltpu.VMEM(LEAD + (CAP, w), BF16))
        scratch += [pltpu.VMEM((RING, RING, 16, TOK), F32)] * 3
        scratch += [pltpu.VMEM((RING, RING, TOK, TOK), BF16)] * 3
        scratch += [pltpu.VMEM((RING, 4, 3, TOK, TOK), BF16)] * 3
        each(lambda w: pltpu.VMEM((2, CORES, 2, RING, CAP, w), BF16))
        each(lambda w: pltpu.VMEM((2, CORES, 2, RING, CAP, w), BF16))
        each(lambda w: pltpu.VMEM((2, RING, RING, CAP, w), BF16))
        each(lambda w: pltpu.VMEM((RING, TOK, w), F32))
        each(lambda w: pltpu.VMEM((2, TOK, w), F32))
        each(lambda w: pltpu.VMEM((2, TOK // 2, w), F32))
        scratch += [
            pltpu.VMEM((hid, fdim), BF16),
            pltpu.VMEM((hid, fdim), BF16),
            pltpu.VMEM((fdim, hid), BF16),
            pltpu.VMEM((2, 2 * RING * RING * CAP, fdim), BF16),
            pltpu.SemaphoreType.DMA((N_COPIES,)),
            pltpu.SemaphoreType.DMA((N_COPIES,)),
            pltpu.SemaphoreType.DMA((3,)),
            pltpu.SemaphoreType.REGULAR((3, 2)),
        ]
        vm = pl.BlockSpec(memory_space=pltpu.VMEM)
        hbm = pl.BlockSpec(memory_space=pl.ANY)
        return pl.pallas_call(
            functools.partial(moe_kernel, widths, fdim, f_tile),
            out_shape=jax.ShapeDtypeStruct((tok, hid), BF16),
            in_specs=[vm, vm, hbm, hbm, hbm],
            out_specs=vm,
            scratch_shapes=scratch,
            compiler_params=pltpu.CompilerParams(collective_id=0, has_side_effects=True, vmem_limit_bytes=67043328),
            name='moe',
        )(x4, meta, w_g[0], w_u[0], w_d[0])

    tok_spec = P(TOKEN_AXES, None)
    w_spec = P(EXPERT_AXES, None, None)
    return jax.shard_map(local_layer, mesh=mesh, in_specs=(tok_spec, tok_spec, tok_spec, w_spec, w_spec, w_spec), out_specs=tok_spec, check_vma=False)
```

```python
import functools

import jax
import jax.numpy as jnp
from jax import lax
from jax.experimental import pallas as pl
from jax.experimental.pallas import tpu as pltpu
from jax.sharding import PartitionSpec as P

TOKEN_AXES = ('ez', 'ey', 'ex')
EXPERT_AXES = ('ex', 'ey', 'ez')
MESH = pl.DeviceIdType.MESH
F32 = jnp.float32
BF16 = jnp.bfloat16

Z, Y, X = 0, 1, 2
D1 = (Y, Z, X)
D2 = (Z, X, Y)
D3 = (X, Y, Z)
A_IS_D1 = (True, False, True)
RING = 4
CORES = 2
CAP = 16
TOK = 128
LEAD = (CORES, RING, RING, RING)


NQ = 6
W1, W2 = (0, 1, 2), (3, 4, 5)


def split_width(hid):
    tiles = hid // 128
    return tuple((tiles * (i + 1) // NQ - tiles * i // NQ) * 128 for i in ORDER)


ORDER = (1, 2, 4, 5, 0, 3)


def moe_kernel(widths, fdim, f_tile, x_ref, meta_ref, w1_hbm, w3_hbm, w2_hbm, y_ref, *scr):
    it = iter(scr)
    take = lambda n: [next(it) for _ in range(n)]
    gat, til, rec = take(NQ), take(NQ), take(NQ)
    meta, sel, comb = take(3), take(3), take(3)
    pas3, pas4, pas5 = take(NQ), take(NQ), take(NQ)
    part, prec, pas6 = take(NQ), take(NQ), take(NQ)
    w1, w3, w2, act = take(4)
    send_sem, recv_sem, w_sem, credit = take(4)

    offs = [sum(widths[:q]) for q in range(NQ)]
    ez, ey, ex = lax.axis_index('ez'), lax.axis_index('ey'), lax.axis_index('ex')
    core = lax.rem(ex, CORES)
    pos = (ez, ey, ex // CORES)
    mod = lambda v: lax.rem(v + RING, RING)
    other = 1 - core

    strides = (1, RING, 2 * RING * RING)

    def turned(v, r):
        return [v[d] * (1 - r) + v[(d + 1) % 3] * r for d in range(3)]

    def peer(dim, off, c, lane=None):
        r = core if lane is None else lane
        q = [mod(pos[j] + off * ((1 - r) * int(j == dim) + r * int(j == (dim + 1) % 3))) for j in range(3)]
        return (q[0], q[1], q[2] * CORES + c)

    counter = [0]

    def send(src, dst, dev):
        i = counter[0]
        counter[0] += 1
        cp = pltpu.make_async_remote_copy(src, dst, send_sem.at[i], recv_sem.at[i], device_id=dev, device_id_type=MESH)
        cp.start()
        return cp

    bar = pltpu.get_barrier_semaphore()
    npeer = 0
    for dim in range(3):
        for off in (1, -1):
            for c in (core, other):
                pl.semaphore_signal(bar, inc=1, device_id=peer(dim, off, c, 0), device_id_type=MESH)
                npeer += 1
    pl.semaphore_signal(bar, inc=1, device_id=peer(0, 0, other), device_id_type=MESH)
    w_copies = [pltpu.make_async_copy(s, d, w_sem.at[i]) for i, (s, d) in enumerate(((w1_hbm, w1), (w3_hbm, w3), (w2_hbm, w2)))]
    pl.semaphore_wait(bar, npeer + 1)

    DIRS = (1, -1)
    d1 = [D1[q % 3] for q in range(NQ)]
    d2 = [D2[q % 3] for q in range(NQ)]
    d3 = [D3[q % 3] for q in range(NQ)]
    a1 = [A_IS_D1[q % 3] for q in range(NQ)]
    lpos, lstr = turned(pos, core), turned(strides, core)
    opos = turned(pos, other)
    p1 = [lpos[d] for d in d1]
    p2 = [lpos[d] for d in d2]
    p3 = [lpos[d] for d in d3]
    p3_other = [opos[d] for d in d3]
    xcol = [x_ref.at[:, :, :, pl.ds(offs[q], widths[q])] for q in range(NQ)]
    unwaited = []

    def chunk(q, r):
        return gat[q].at[:, :, p2[q], mod(p1[q] + r)]

    m1 = [[None, None] for _ in range(3)]
    mf1 = [None] * 3
    m2 = [[None, None] for _ in range(3)]
    mf2 = [None] * 3
    g1 = [[None, None] for _ in range(NQ)]
    f1 = [[None, None] for _ in range(NQ)]
    g2 = [[[None] * 4, [None] * 4] for _ in range(NQ)]
    f2 = [[None] * 4 for _ in range(NQ)]

    def first_sends(wave):
        for q in wave:
            for i, d in enumerate(DIRS):
                if q < 3:
                    m1[q][i] = send(meta_ref, meta[q].at[p2[q], p1[q]], peer(d1[q], d, core))
                g1[q][i] = send(xcol[q], chunk(q, 0), peer(d1[q], d, core))
        for q in wave:
            for i, d in enumerate(DIRS):
                g2[q][i][0] = send(xcol[q], chunk(q, 0), peer(d2[q], d, core))

    def first_forwards(wave):
        for q in wave:
            for i, d in enumerate(DIRS):
                if q < 3:
                    m1[q][i].wait_recv()
                    if i == 0:
                        src = meta[q].at[p2[q], mod(p1[q] - 1)]
                        mf1[q] = send(src, src, peer(d1[q], 1, core))
                g1[q][i].wait_recv()
                half = chunk(q, -d).at[i]
                f1[q][i] = send(half, half, peer(d1[q], d, core))
        for q in wave:
            for i, d in enumerate(DIRS):
                for r in (1, 3):
                    g2[q][i][r] = send(chunk(q, r), chunk(q, r), peer(d2[q], d, core))

    def forward2(q, i, r):
        g2[q][i][r].wait_recv()
        src = gat[q].at[:, :, mod(p2[q] - DIRS[i]), mod(p1[q] + r)]
        f2[q][r] = send(src, src, peer(d2[q], DIRS[i], core))

    first_sends(W1)
    first_sends(W2)
    for c in w_copies:
        c.start()
    for q in range(NQ):
        gat[q][:, :, p2[q], p1[q]] = x_ref[:, :, :, offs[q]:offs[q] + widths[q]]
    for k in range(3):
        meta[k][p2[k], p1[k]] = meta_ref[...]
    first_forwards(W1)
    for k in range(3):
        mf1[k].wait_recv()
        for i, d in enumerate(DIRS):
            row = meta[k].at[p2[k]]
            m2[k][i] = send(row, row, peer(d2[k], d, core))
    first_forwards(W2)
    for q in W1 + W2:
        forward2(q, 0, 0)
        for i, d in enumerate(DIRS):
            f1[q][i].wait_recv()
        for i, d in enumerate(DIRS):
            g2[q][i][2] = send(chunk(q, 2), chunk(q, 2), peer(d2[q], d, core))
    for k in range(3):
        for i in range(2):
            m2[k][i].wait_recv()
        src = meta[k].at[mod(p2[k] - 1)]
        mf2[k] = send(src, src, peer(d2[k], 1, core))

    tri = (lax.broadcasted_iota(jnp.int32, (TOK, TOK), 0) < lax.broadcasted_iota(jnp.int32, (TOK, TOK), 1)).astype(BF16)
    i8 = lax.broadcasted_iota(jnp.int32, (8, 1), 0)
    slot = lax.broadcasted_iota(jnp.int32, (8, CAP, TOK), 1).astype(F32)

    def experts8(k):
        base = lpos[D1[k]] * lstr[D1[k]] + lpos[D2[k]] * lstr[D2[k]]
        return (base + (i8 & 3) * lstr[D3[k]] + (i8 >> 2) * (RING * RING)).astype(F32)

    def picked(ids, evec):
        m = (ids[0:1, :] == evec).astype(F32)
        for j in range(1, 8):
            m = m + (ids[j:j + 1, :] == evec).astype(F32)
        return m

    def rank_of(m):
        rank = jnp.dot(m.astype(BF16), tri, preferred_element_type=F32)
        return jnp.where(m > 0.5, rank, -1.0)

    def onehot(k, i):
        evec = experts8(k)
        rm = rank_of(jnp.concatenate([picked(meta[k][i, j, 0:8], evec) for j in range(4)], axis=0))
        for j in range(4):
            hot = (rm[j * 8:(j + 1) * 8][:, None, :] == slot).astype(F32)
            sel[k][i, j] = hot.reshape(TOK, TOK).astype(BF16)

    def select(q, i):
        k, w = q % 3, widths[q]
        for j in range(4):
            rows = gat[q][:, :, i, j].reshape(TOK, w)
            out = jnp.dot(sel[k][i, j], rows, preferred_element_type=F32).astype(BF16).reshape(CORES, RING, CAP, w)
            if a1[q]:
                til[q][:, :, j, i] = out
            else:
                til[q][:, :, i, j] = out

    def loop(n, f):
        def body(i, carry):
            f(i)
            return carry
        lax.fori_loop(0, n, body, 0)

    for k in range(3):
        onehot(k, p2[k])
    for q in W1 + W2:
        select(q, p2[q])
    for q in W1:
        forward2(q, 0, 1)
        forward2(q, 1, 3)
    for k in range(3):
        mf2[k].wait_recv()
        loop(3, lambda i, k=k: onehot(k, mod(p2[k] + 1 + i)))
    for q in W2:
        forward2(q, 0, 1)
        forward2(q, 1, 3)
    for q in W1 + W2:
        forward2(q, 1, 2)

    def gathered(q, near):
        if near:
            for i, r in ((0, 2), (0, 3), (1, 0), (1, 1)):
                g2[q][i][r].wait_recv()
            loop(2, lambda i, q=q: select(q, mod(p2[q] - 1 + 2 * i)))
        else:
            for r in range(4):
                f2[q][r].wait_recv()
            select(q, mod(p2[q] + 2))
            done = g1[q] + f1[q] + g2[q][0] + g2[q][1] + f2[q]
            if q < 3:
                done = done + m1[q] + [mf1[q]] + m2[q] + [mf2[q]]
            for c in done:
                c.wait_send()

    def sub(ref, q, c, d, half=None):
        a = slice(None) if half is None else pl.ds(2 * half, 2)
        return (ref.at[c, d, a], ref.at[c, a, d], ref.at[c, a, :, d])[q % 3]

    def til_block(ref, q, c, d, half=None):
        return ref.at[c, d] if half is None else ref.at[c, d, pl.ds(2 * half, 2)]

    class Leg:
        def __init__(self, q, cr, lane, src, src_block, dst, dst_block, pas):
            self.q, self.cr, self.lane, self.src, self.dst = q, cr, lane, src, dst
            self.src_block, self.dst_block, self.pas = src_block, dst_block, pas
            self.c = core if cr == 0 else other
            self.p = p3[q] if lane is core else p3_other[q]
            self.first, self.direct = [], []

        def out(self, d, half=None):
            return self.src_block(self.src, self.q, self.c, d, half)

        def into(self, d, half=None):
            return self.dst_block(self.dst, self.q, core, d, half)

        def far(self):
            for i, d in enumerate(DIRS):
                self.first.append(send(self.out(mod(self.p + 2), i), self.pas.at[i, self.cr], peer(d3[self.q], d, core, self.lane)))

        def near(self):
            for i, d in enumerate(DIRS):
                self.direct.append(send(self.out(mod(self.p + d)), self.into(self.p), peer(d3[self.q], d, self.c, self.lane)))
            if self.cr == 1:
                self.direct.append(send(self.out(self.p), self.into(self.p), peer(d3[self.q], 0, other, self.lane)))

        def forward(self):
            for i, d in enumerate(DIRS):
                self.first[i].wait_recv()
                self.direct.append(send(self.pas.at[i, self.cr], self.into(mod(self.p - d), i), peer(d3[self.q], d, self.c, self.lane)))

        def arrive(self):
            for cp in self.direct:
                cp.wait_recv()

        def sent(self):
            for cp in self.first + self.direct:
                cp.wait_send()

    def keep3(q):
        v = til[q][core, p3[q]]
        if q % 3 == 0:
            rec[q][core, p3[q]] = v
        elif q % 3 == 1:
            rec[q][core, :, p3[q]] = v
        else:
            rec[q][core, :, :, p3[q]] = v

    def keep4(q):
        if q % 3 == 0:
            v = til[q][core, p3[q]]
        elif q % 3 == 1:
            v = til[q][core, :, p3[q]]
        else:
            v = til[q][core, :, :, p3[q]]
        gat[q][core, p3[q]] = v

    x3 = [[Leg(q, cr, core, til[q], til_block, rec[q], sub, pas3[q]) for cr in range(2)] for q in range(NQ)]
    for q in W1:
        gathered(q, True)
    for q in W1:
        gathered(q, False)
        x3[q][0].far()
        x3[q][0].near()
    for q in W2:
        gathered(q, True)
    for q in W2:
        gathered(q, False)
        x3[q][0].far()
    for q in W1:
        x3[q][1].far()
    for q in W1:
        x3[q][0].forward()
    for q in W2:
        x3[q][0].near()
        x3[q][1].far()
    for q in W2:
        x3[q][0].forward()
    for q in W1 + W2:
        x3[q][1].near()
    for q in W1 + W2:
        keep3(q)
    for q in W1 + W2:
        x3[q][1].forward()
    for c in w_copies:
        c.wait()

    x4 = [[Leg(q, cr, core if cr == 0 else other, til[q], sub, gat[q], til_block, pas4[q]) for cr in range(2)] for q in range(NQ)]
    rows = 2 * RING * RING * CAP
    for cr in range(2):
        c = core if cr == 0 else other
        for q in range(NQ):
            x3[q][cr].arrive()
        for q in range(NQ):
            x3[q][cr].sent()

        def hidden(i, c=c):
            xs = [rec[q][c, pl.ds(2 * i, 2)].reshape(rows, widths[q]) for q in range(NQ)]
            for f in range(fdim // f_tile):
                cols = slice(f * f_tile, (f + 1) * f_tile)
                hg = sum(jnp.dot(xs[q], w1[offs[q]:offs[q] + widths[q], cols], preferred_element_type=F32) for q in range(NQ))
                hu = sum(jnp.dot(xs[q], w3[offs[q]:offs[q] + widths[q], cols], preferred_element_type=F32) for q in range(NQ))
                act[i, :, cols] = (hg * jax.nn.sigmoid(hg) * hu).astype(BF16)

        def down(wave, c=c):
            def step(i):
                for q in wave:
                    o = jnp.dot(act[i], w2[:, offs[q]:offs[q] + widths[q]], preferred_element_type=F32).astype(BF16)
                    til[q][c, pl.ds(2 * i, 2)] = o.reshape(2, RING, RING, CAP, widths[q])
            loop(2, step)

        loop(2, hidden)
        down(W1)
        if cr == 1:
            for q in W1 + W2:
                x4[q][0].forward()
        for q in W1:
            x4[q][cr].far()
        for q in W1:
            x4[q][cr].near()
        down(W2)
        for q in W2:
            x4[q][cr].far()
        if cr == 1:
            for q in W1:
                x4[q][1].forward()
        for q in W2:
            x4[q][cr].near()
        if cr == 0:
            for q in W1 + W2:
                keep4(q)
    for k in range(3):
        for i, d in enumerate(DIRS):
            pl.semaphore_signal(credit.at[k, i], inc=1, device_id=peer(D1[k], d, core), device_id_type=MESH)

    def weights(k, i):
        mrow = meta[k][i, p1[k]]
        ids, gates = mrow[0:8], mrow[8:16]
        own = lpos[D2[k]] * lstr[D2[k]]
        ms, gs = [], []
        for b in range(4):
            idx = i8 + b * 8
            d3e, d1e, ce = idx & 3, (idx >> 2) & 3, idx >> 4
            evec = (own + d3e * lstr[D3[k]] + d1e * lstr[D1[k]] + ce * (RING * RING)).astype(F32)
            m = jnp.zeros((8, TOK), F32)
            g = jnp.zeros((8, TOK), F32)
            for j in range(8):
                hit = ids[j:j + 1, :] == evec
                m = m + hit.astype(F32)
                g = g + jnp.where(hit, gates[j:j + 1, :], 0.0)
            ms.append(m)
            gs.append(g)
        rm = rank_of(jnp.concatenate(ms, axis=0))
        for b in range(4):
            hot = jnp.where(rm[b * 8:(b + 1) * 8][:, None, :] == slot, gs[b][:, None, :], 0.0).reshape(TOK, TOK).T
            hi = hot.astype(BF16)
            r1 = hot - hi.astype(F32)
            mid = r1.astype(BF16)
            lo = (r1 - mid.astype(F32)).astype(BF16)
            comb[k][i, b, 0] = hi
            comb[k][i, b, 1] = mid
            comb[k][i, b, 2] = lo

    for q in W2:
        x4[q][1].forward()
    for k in range(3):
        loop(4, lambda i, k=k: weights(k, i))

    def from_src(ref, q, d, half=None):
        cs = slice(None) if half is None else half
        return ref.at[cs, :, d] if a1[q] else ref.at[cs, :, :, d]

    x5 = [([], []) for _ in range(NQ)]

    def arrive4(q):
        for cr in range(2):
            x4[q][cr].arrive()
        if q < 3:
            for i in range(2):
                pl.semaphore_wait(credit.at[q, i], 1)

    def far5(q):
        for i, d in enumerate(DIRS):
            x5[q][0].append(send(from_src(gat[q], q, mod(p1[q] + 2), i), pas5[q].at[i], peer(d1[q], d, core)))

    def near5(q):
        for i, d in enumerate(DIRS):
            x5[q][1].append(send(from_src(gat[q], q, mod(p1[q] + d)), rec[q].at[:, p1[q]], peer(d1[q], d, core)))

    def keep5(q):
        if a1[q]:
            rec[q][:, p1[q]] = gat[q][:, :, p1[q]]
        else:
            rec[q][:, p1[q]] = gat[q][:, :, :, p1[q]]

    def forward5(q):
        for i, d in enumerate(DIRS):
            x5[q][0][i].wait_recv()
            x5[q][1].append(send(pas5[q].at[i], rec[q].at[i, mod(p1[q] - d)], peer(d1[q], d, core)))

    for q in W1:
        arrive4(q)
        far5(q)
        near5(q)
    for q in W1:
        keep5(q)
    for q in W2:
        arrive4(q)
        far5(q)
    for q in W1:
        forward5(q)
    for q in W2:
        near5(q)
    for q in W2:
        keep5(q)
    for q in W2:
        forward5(q)

    x6 = [([], []) for _ in range(NQ)]
    half_tok = TOK // 2

    def combine(q):
        for cp in x5[q][1]:
            cp.wait_recv()
        k, w = q % 3, widths[q]

        def step(i):
            acc = jnp.zeros((TOK, w), F32)
            for b in range(4):
                o = rec[q][b // 2, pl.ds(2 * (b % 2), 2), :, i].reshape(TOK, w)
                for t in range(3):
                    acc = acc + jnp.dot(comb[k][i, b, t], o, preferred_element_type=F32)
            part[q][i] = acc

        loop(4, step)

    def far6(q):
        for i, d in enumerate(DIRS):
            x6[q][0].append(send(part[q].at[mod(p2[q] + 2), pl.ds(i * half_tok, half_tok)], pas6[q].at[i], peer(d2[q], d, core)))

    def rows6(q, i, half):
        return part[q].at[mod(p2[q] + DIRS[i]), pl.ds(half * half_tok, half_tok)], prec[q].at[i, pl.ds(half * half_tok, half_tok)]

    def near6(q):
        for i, d in enumerate(DIRS):
            x6[q][1].append(send(*rows6(q, i, 1 - i), peer(d2[q], d, core)))

    def forward6(q):
        for i, d in enumerate(DIRS):
            x6[q][0][i].wait_recv()
            mine, there = rows6(q, i, i)
            mine[...] = mine[...] + pas6[q][i]
            x6[q][1].append(send(mine, there, peer(d2[q], d, core)))

    def final(q):
        for cp in x6[q][1]:
            cp.wait_recv()
        total = part[q][p2[q]] + prec[q][0] + prec[q][1]
        xk = x_ref[:, :, :, offs[q]:offs[q] + widths[q]].reshape(TOK, widths[q]).astype(F32)
        y_ref[:, offs[q]:offs[q] + widths[q]] = (xk + total).astype(BF16)

    for q in W1:
        combine(q)
        far6(q)
        near6(q)
    for q in W2:
        combine(q)
        far6(q)
    for q in W1:
        forward6(q)
    for q in W2:
        near6(q)
    for q in W2:
        forward6(q)
    for q in W1 + W2:
        final(q)
    for q in range(NQ):
        for cr in range(2):
            x4[q][cr].sent()
        for cp in x5[q][0] + x5[q][1] + x6[q][0] + x6[q][1]:
            cp.wait_send()


N_COPIES = 3 * 6 + NQ * (16 + 13 + 13 + 6 + 6)


def solution(mesh):
    def local_layer(x_loc, ids_loc, gates_loc, w_g, w_u, w_d):
        tok, hid = x_loc.shape
        fdim = w_g.shape[2]
        widths = split_width(hid)
        f_tile = 256 if fdim % 256 == 0 else fdim
        meta = jnp.concatenate([ids_loc.T.astype(F32), gates_loc.T], axis=0)
        x4 = x_loc.reshape(CORES, RING, CAP, hid)
        scratch = []
        each = lambda f: scratch.extend(f(w) for w in widths)
        for _ in range(3):
            each(lambda w: pltpu.VMEM(LEAD + (CAP, w), BF16))
        scratch += [pltpu.VMEM((RING, RING, 16, TOK), F32)] * 3
        scratch += [pltpu.VMEM((RING, RING, TOK, TOK), BF16)] * 3
        scratch += [pltpu.VMEM((RING, 4, 3, TOK, TOK), BF16)] * 3
        each(lambda w: pltpu.VMEM((2, CORES, 2, RING, CAP, w), BF16))
        each(lambda w: pltpu.VMEM((2, CORES, 2, RING, CAP, w), BF16))
        each(lambda w: pltpu.VMEM((2, RING, RING, CAP, w), BF16))
        each(lambda w: pltpu.VMEM((RING, TOK, w), F32))
        each(lambda w: pltpu.VMEM((2, TOK, w), F32))
        each(lambda w: pltpu.VMEM((2, TOK // 2, w), F32))
        scratch += [
            pltpu.VMEM((hid, fdim), BF16),
            pltpu.VMEM((hid, fdim), BF16),
            pltpu.VMEM((fdim, hid), BF16),
            pltpu.VMEM((2, 2 * RING * RING * CAP, fdim), BF16),
            pltpu.SemaphoreType.DMA((N_COPIES,)),
            pltpu.SemaphoreType.DMA((N_COPIES,)),
            pltpu.SemaphoreType.DMA((3,)),
            pltpu.SemaphoreType.REGULAR((3, 2)),
        ]
        vm = pl.BlockSpec(memory_space=pltpu.VMEM)
        hbm = pl.BlockSpec(memory_space=pl.ANY)
        return pl.pallas_call(
            functools.partial(moe_kernel, widths, fdim, f_tile),
            out_shape=jax.ShapeDtypeStruct((tok, hid), BF16),
            in_specs=[vm, vm, hbm, hbm, hbm],
            out_specs=vm,
            scratch_shapes=scratch,
            compiler_params=pltpu.CompilerParams(collective_id=0, has_side_effects=True, vmem_limit_bytes=67043328),
            name='moe',
        )(x4, meta, w_g[0], w_u[0], w_d[0])

    tok_spec = P(TOKEN_AXES, None)
    w_spec = P(EXPERT_AXES, None, None)
    return jax.shard_map(local_layer, mesh=mesh, in_specs=(tok_spec, tok_spec, tok_spec, w_spec, w_spec, w_spec), out_specs=tok_spec, check_vma=False)
```

```python
import functools

import jax
import jax.numpy as jnp
from jax import lax
from jax.experimental import pallas as pl
from jax.experimental.pallas import tpu as pltpu
from jax.sharding import PartitionSpec as P

TOKEN_AXES = ('ez', 'ey', 'ex')
EXPERT_AXES = ('ex', 'ey', 'ez')
MESH = pl.DeviceIdType.MESH
F32 = jnp.float32
BF16 = jnp.bfloat16

Z, Y, X = 0, 1, 2
D1 = (Y, Z, X)
D2 = (Z, X, Y)
D3 = (X, Y, Z)
A_IS_D1 = (True, False, True)
RING = 4
CORES = 2
CAP = 16
TOK = 128
LEAD = (CORES, RING, RING, RING)


NQ = 6
W1, W2 = (0, 1, 2), (3, 4, 5)


def split_width(hid):
    tiles = hid // 128
    second = tiles * 3 // 8
    first = tiles - second
    thirds = lambda n: [n - 2 * (n // 3), n // 3, n // 3]
    return tuple(n * 128 for n in thirds(first) + thirds(second))


def moe_kernel(widths, fdim, f_tile, x_ref, ids_ref, gates_ref, w1_hbm, w3_hbm, w2_hbm, y_ref, *scr):
    it = iter(scr)
    take = lambda n: [next(it) for _ in range(n)]
    gat, til, rec = take(NQ), take(NQ), take(NQ)
    meta, sel, comb = take(3), take(3), take(3)
    pas3, pas4, pas5 = take(NQ), take(NQ), take(NQ)
    part, prec, pas6 = take(NQ), take(NQ), take(NQ)
    w1, w3, w2, act, meta_ref = take(5)
    send_sem, recv_sem, w_sem, credit = take(4)

    offs = [sum(widths[:q]) for q in range(NQ)]
    ez, ey, ex = lax.axis_index('ez'), lax.axis_index('ey'), lax.axis_index('ex')
    core = lax.rem(ex, CORES)
    pos = (ez, ey, ex // CORES)
    mod = lambda v: lax.rem(v + RING, RING)
    other = 1 - core

    strides = (1, RING, 2 * RING * RING)

    def turned(v, r):
        return [v[d] * (1 - r) + v[(d + 1) % 3] * r for d in range(3)]

    def peer(dim, off, c, lane=None):
        r = core if lane is None else lane
        q = [mod(pos[j] + off * ((1 - r) * int(j == dim) + r * int(j == (dim + 1) % 3))) for j in range(3)]
        return (q[0], q[1], q[2] * CORES + c)

    counter = [0]

    def send(src, dst, dev):
        i = counter[0]
        counter[0] += 1
        cp = pltpu.make_async_remote_copy(src, dst, send_sem.at[i], recv_sem.at[i], device_id=dev, device_id_type=MESH)
        cp.start()
        return cp

    meta_ref[0:8] = ids_ref[...].astype(F32)
    meta_ref[8:16] = gates_ref[...]
    bar = pltpu.get_barrier_semaphore()
    npeer = 0
    for dim in range(3):
        for off in (1, -1):
            for c in (core, other):
                pl.semaphore_signal(bar, inc=1, device_id=peer(dim, off, c, 0), device_id_type=MESH)
                npeer += 1
    pl.semaphore_signal(bar, inc=1, device_id=peer(0, 0, other), device_id_type=MESH)
    w_copies = [pltpu.make_async_copy(s, d, w_sem.at[i]) for i, (s, d) in enumerate(((w1_hbm, w1), (w3_hbm, w3), (w2_hbm, w2)))]
    pl.semaphore_wait(bar, npeer + 1)

    DIRS = (1, -1)
    d1 = [D1[q % 3] for q in range(NQ)]
    d2 = [D2[q % 3] for q in range(NQ)]
    d3 = [D3[q % 3] for q in range(NQ)]
    a1 = [A_IS_D1[q % 3] for q in range(NQ)]
    lpos, lstr = turned(pos, core), turned(strides, core)
    opos = turned(pos, other)
    p1 = [lpos[d] for d in d1]
    p2 = [lpos[d] for d in d2]
    p3 = [lpos[d] for d in d3]
    p3_other = [opos[d] for d in d3]
    xcol = [x_ref.at[:, :, :, pl.ds(offs[q], widths[q])] for q in range(NQ)]
    unwaited = []

    def chunk(q, r):
        return gat[q].at[:, :, p2[q], mod(p1[q] + r)]

    m1 = [[None, None] for _ in range(3)]
    mf1 = [None] * 3
    m2 = [[None, None] for _ in range(3)]
    mf2 = [None] * 3
    g1 = [[None, None] for _ in range(NQ)]
    f1 = [[None, None] for _ in range(NQ)]
    g2 = [[[None] * 4, [None] * 4] for _ in range(NQ)]
    f2 = [[None] * 4 for _ in range(NQ)]

    def first_sends(wave):
        for q in wave:
            for i, d in enumerate(DIRS):
                if q < 3:
                    m1[q][i] = send(meta_ref, meta[q].at[p2[q], p1[q]], peer(d1[q], d, core))
                g1[q][i] = send(xcol[q], chunk(q, 0), peer(d1[q], d, core))
        for q in wave:
            for i, d in enumerate(DIRS):
                g2[q][i][0] = send(xcol[q], chunk(q, 0), peer(d2[q], d, core))

    def first_forwards(wave):
        for q in wave:
            for i, d in enumerate(DIRS):
                if q < 3:
                    m1[q][i].wait_recv()
                    if i == 0:
                        src = meta[q].at[p2[q], mod(p1[q] - 1)]
                        mf1[q] = send(src, src, peer(d1[q], 1, core))
                g1[q][i].wait_recv()
                half = chunk(q, -d).at[i]
                f1[q][i] = send(half, half, peer(d1[q], d, core))
        for q in wave:
            for i, d in enumerate(DIRS):
                for r in (1, 3):
                    g2[q][i][r] = send(chunk(q, r), chunk(q, r), peer(d2[q], d, core))

    def forward2(q, i, r):
        g2[q][i][r].wait_recv()
        src = gat[q].at[:, :, mod(p2[q] - DIRS[i]), mod(p1[q] + r)]
        f2[q][r] = send(src, src, peer(d2[q], DIRS[i], core))

    first_sends(W1)
    first_sends(W2)
    for c in w_copies:
        c.start()
    for q in range(NQ):
        gat[q][:, :, p2[q], p1[q]] = x_ref[:, :, :, offs[q]:offs[q] + widths[q]]
    for k in range(3):
        meta[k][p2[k], p1[k]] = meta_ref[...]
    first_forwards(W1)
    for k in range(3):
        mf1[k].wait_recv()
        for i, d in enumerate(DIRS):
            row = meta[k].at[p2[k]]
            m2[k][i] = send(row, row, peer(d2[k], d, core))
    first_forwards(W2)
    for q in W1 + W2:
        forward2(q, 0, 0)
        for i, d in enumerate(DIRS):
            f1[q][i].wait_recv()
        for i, d in enumerate(DIRS):
            g2[q][i][2] = send(chunk(q, 2), chunk(q, 2), peer(d2[q], d, core))
    for k in range(3):
        for i in range(2):
            m2[k][i].wait_recv()
        src = meta[k].at[mod(p2[k] - 1)]
        mf2[k] = send(src, src, peer(d2[k], 1, core))

    tri = (lax.broadcasted_iota(jnp.int32, (TOK, TOK), 0) < lax.broadcasted_iota(jnp.int32, (TOK, TOK), 1)).astype(BF16)
    i8 = lax.broadcasted_iota(jnp.int32, (8, 1), 0)
    slot = lax.broadcasted_iota(jnp.int32, (8, CAP, TOK), 1).astype(F32)

    def experts8(k):
        base = lpos[D1[k]] * lstr[D1[k]] + lpos[D2[k]] * lstr[D2[k]]
        return (base + (i8 & 3) * lstr[D3[k]] + (i8 >> 2) * (RING * RING)).astype(F32)

    def picked(ids, evec):
        m = (ids[0:1, :] == evec).astype(F32)
        for j in range(1, 8):
            m = m + (ids[j:j + 1, :] == evec).astype(F32)
        return m

    def rank_of(m):
        rank = jnp.dot(m.astype(BF16), tri, preferred_element_type=F32)
        return jnp.where(m > 0.5, rank, -1.0)

    def onehot(k, i):
        evec = experts8(k)
        rm = rank_of(jnp.concatenate([picked(meta[k][i, j, 0:8], evec) for j in range(4)], axis=0))
        for j in range(4):
            hot = (rm[j * 8:(j + 1) * 8][:, None, :] == slot).astype(F32)
            sel[k][i, j] = hot.reshape(TOK, TOK).astype(BF16)

    def select(q, i):
        k, w = q % 3, widths[q]
        for j in range(4):
            rows = gat[q][:, :, i, j].reshape(TOK, w)
            out = jnp.dot(sel[k][i, j], rows, preferred_element_type=F32).astype(BF16).reshape(CORES, RING, CAP, w)
            if a1[q]:
                til[q][:, :, j, i] = out
            else:
                til[q][:, :, i, j] = out

    def loop(n, f):
        def body(i, carry):
            f(i)
            return carry
        lax.fori_loop(0, n, body, 0)

    for k in range(3):
        onehot(k, p2[k])
    for q in W1 + W2:
        select(q, p2[q])
    for q in W1:
        forward2(q, 0, 1)
        forward2(q, 1, 3)
    for k in range(3):
        mf2[k].wait_recv()
        loop(3, lambda i, k=k: onehot(k, mod(p2[k] + 1 + i)))
    for q in W2:
        forward2(q, 0, 1)
        forward2(q, 1, 3)
    for q in W1 + W2:
        forward2(q, 1, 2)

    def gathered(q, near):
        if near:
            for i, r in ((0, 2), (0, 3), (1, 0), (1, 1)):
                g2[q][i][r].wait_recv()
            loop(2, lambda i, q=q: select(q, mod(p2[q] - 1 + 2 * i)))
        else:
            for r in range(4):
                f2[q][r].wait_recv()
            select(q, mod(p2[q] + 2))
            done = g1[q] + f1[q] + g2[q][0] + g2[q][1] + f2[q]
            if q < 3:
                done = done + m1[q] + [mf1[q]] + m2[q] + [mf2[q]]
            for c in done:
                c.wait_send()

    def sub(ref, q, c, d, half=None):
        a = slice(None) if half is None else pl.ds(2 * half, 2)
        return (ref.at[c, d, a], ref.at[c, a, d], ref.at[c, a, :, d])[q % 3]

    def til_block(ref, q, c, d, half=None):
        return ref.at[c, d] if half is None else ref.at[c, d, pl.ds(2 * half, 2)]

    class Leg:
        def __init__(self, q, cr, lane, src, src_block, dst, dst_block, pas):
            self.q, self.cr, self.lane, self.src, self.dst = q, cr, lane, src, dst
            self.src_block, self.dst_block, self.pas = src_block, dst_block, pas
            self.c = core if cr == 0 else other
            self.p = p3[q] if lane is core else p3_other[q]
            self.first, self.direct = [], []

        def out(self, d, half=None):
            return self.src_block(self.src, self.q, self.c, d, half)

        def into(self, d, half=None):
            return self.dst_block(self.dst, self.q, core, d, half)

        def far(self):
            for i, d in enumerate(DIRS):
                self.first.append(send(self.out(mod(self.p + 2), i), self.pas.at[i, self.cr], peer(d3[self.q], d, core, self.lane)))

        def near(self):
            for i, d in enumerate(DIRS):
                self.direct.append(send(self.out(mod(self.p + d)), self.into(self.p), peer(d3[self.q], d, self.c, self.lane)))
            if self.cr == 1:
                self.direct.append(send(self.out(self.p), self.into(self.p), peer(d3[self.q], 0, other, self.lane)))

        def forward(self):
            for i, d in enumerate(DIRS):
                self.first[i].wait_recv()
                self.direct.append(send(self.pas.at[i, self.cr], self.into(mod(self.p - d), i), peer(d3[self.q], d, self.c, self.lane)))

        def arrive(self):
            for cp in self.direct:
                cp.wait_recv()

        def sent(self):
            for cp in self.first + self.direct:
                cp.wait_send()

    def keep3(q):
        v = til[q][core, p3[q]]
        if q % 3 == 0:
            rec[q][core, p3[q]] = v
        elif q % 3 == 1:
            rec[q][core, :, p3[q]] = v
        else:
            rec[q][core, :, :, p3[q]] = v

    def keep4(q):
        if q % 3 == 0:
            v = til[q][core, p3[q]]
        elif q % 3 == 1:
            v = til[q][core, :, p3[q]]
        else:
            v = til[q][core, :, :, p3[q]]
        gat[q][core, p3[q]] = v

    x3 = [[Leg(q, cr, core, til[q], til_block, rec[q], sub, pas3[q]) for cr in range(2)] for q in range(NQ)]
    for q in W1:
        gathered(q, True)
    for q in W1:
        gathered(q, False)
        x3[q][0].far()
        x3[q][0].near()
    for q in W2:
        gathered(q, True)
    for q in W2:
        gathered(q, False)
        x3[q][0].far()
    for q in W1:
        x3[q][1].far()
    for q in W1:
        x3[q][0].forward()
    for q in W2:
        x3[q][0].near()
        x3[q][1].far()
    for q in W2:
        x3[q][0].forward()
    for q in W1 + W2:
        x3[q][1].near()
    for q in W1 + W2:
        keep3(q)
    for q in W1 + W2:
        x3[q][1].forward()
    for c in w_copies:
        c.wait()

    x4 = [[Leg(q, cr, core if cr == 0 else other, til[q], sub, gat[q], til_block, pas4[q]) for cr in range(2)] for q in range(NQ)]
    rows = 2 * RING * RING * CAP
    for cr in range(2):
        c = core if cr == 0 else other
        for q in range(NQ):
            x3[q][cr].arrive()
        for q in range(NQ):
            x3[q][cr].sent()

        def hidden(i, c=c):
            xs = jnp.concatenate([rec[q][c, pl.ds(2 * i, 2)].reshape(rows, widths[q]) for q in range(NQ)], axis=1)
            for f in range(fdim // f_tile):
                cols = slice(f * f_tile, (f + 1) * f_tile)
                hg = jnp.dot(xs, w1[:, cols], preferred_element_type=F32)
                hu = jnp.dot(xs, w3[:, cols], preferred_element_type=F32)
                act[i, :, cols] = (hg * jax.nn.sigmoid(hg) * hu).astype(BF16)

        def down(wave, c=c):
            def step(i):
                lo, hi = offs[wave[0]], offs[wave[-1]] + widths[wave[-1]]
                o = jnp.dot(act[i], w2[:, lo:hi], preferred_element_type=F32).astype(BF16)
                for q in wave:
                    part_q = o[:, offs[q] - lo:offs[q] - lo + widths[q]]
                    til[q][c, pl.ds(2 * i, 2)] = part_q.reshape(2, RING, RING, CAP, widths[q])
            loop(2, step)

        loop(2, hidden)
        if cr == 1:
            for q in W1 + W2:
                x4[q][0].forward()
        down(W1)
        for q in W1:
            x4[q][cr].far()
        for q in W1:
            x4[q][cr].near()
        down(W2)
        for q in W2:
            x4[q][cr].far()
        if cr == 1:
            for q in W1:
                x4[q][1].forward()
        for q in W2:
            x4[q][cr].near()
        if cr == 0:
            for q in W1 + W2:
                keep4(q)
    for k in range(3):
        for i, d in enumerate(DIRS):
            pl.semaphore_signal(credit.at[k, i], inc=1, device_id=peer(D1[k], d, core), device_id_type=MESH)

    def weights(k, i):
        mrow = meta[k][i, p1[k]]
        ids, gates = mrow[0:8], mrow[8:16]
        own = lpos[D2[k]] * lstr[D2[k]]
        ms, gs = [], []
        for b in range(4):
            idx = i8 + b * 8
            d3e, d1e, ce = idx & 3, (idx >> 2) & 3, idx >> 4
            evec = (own + d3e * lstr[D3[k]] + d1e * lstr[D1[k]] + ce * (RING * RING)).astype(F32)
            m = jnp.zeros((8, TOK), F32)
            g = jnp.zeros((8, TOK), F32)
            for j in range(8):
                hit = ids[j:j + 1, :] == evec
                m = m + hit.astype(F32)
                g = g + jnp.where(hit, gates[j:j + 1, :], 0.0)
            ms.append(m)
            gs.append(g)
        rm = rank_of(jnp.concatenate(ms, axis=0))
        for b in range(4):
            hot = jnp.where(rm[b * 8:(b + 1) * 8][:, None, :] == slot, gs[b][:, None, :], 0.0).reshape(TOK, TOK).T
            hi = hot.astype(BF16)
            r1 = hot - hi.astype(F32)
            mid = r1.astype(BF16)
            lo = (r1 - mid.astype(F32)).astype(BF16)
            at = slice((b % 2) * TOK, (b % 2 + 1) * TOK)
            comb[k][i, b // 2, 0, :, at] = hi
            comb[k][i, b // 2, 1, :, at] = mid
            comb[k][i, b // 2, 2, :, at] = lo

    for q in W2:
        x4[q][1].forward()
    for k in range(3):
        loop(4, lambda i, k=k: weights(k, i))

    def from_src(ref, q, d, half=None):
        cs = slice(None) if half is None else half
        return ref.at[cs, :, d] if a1[q] else ref.at[cs, :, :, d]

    x5 = [([], []) for _ in range(NQ)]

    def arrive4(q):
        for cr in range(2):
            x4[q][cr].arrive()
        if q < 3:
            for i in range(2):
                pl.semaphore_wait(credit.at[q, i], 1)

    def far5(q):
        for i, d in enumerate(DIRS):
            x5[q][0].append(send(from_src(gat[q], q, mod(p1[q] + 2), i), pas5[q].at[i], peer(d1[q], d, core)))

    def near5(q):
        for i, d in enumerate(DIRS):
            x5[q][1].append(send(from_src(gat[q], q, mod(p1[q] + d)), rec[q].at[:, p1[q]], peer(d1[q], d, core)))

    def keep5(q):
        if a1[q]:
            rec[q][:, p1[q]] = gat[q][:, :, p1[q]]
        else:
            rec[q][:, p1[q]] = gat[q][:, :, :, p1[q]]

    def forward5(q):
        for i, d in enumerate(DIRS):
            x5[q][0][i].wait_recv()
            x5[q][1].append(send(pas5[q].at[i], rec[q].at[i, mod(p1[q] - d)], peer(d1[q], d, core)))

    for q in W1:
        arrive4(q)
        far5(q)
        near5(q)
    for q in W1:
        keep5(q)
    for q in W2:
        arrive4(q)
        far5(q)
    for q in W1:
        forward5(q)
    for q in W2:
        near5(q)
    for q in W2:
        keep5(q)
    for q in W2:
        forward5(q)

    x6 = [([], []) for _ in range(NQ)]
    half_tok = TOK // 2

    def combine(q):
        for cp in x5[q][1]:
            cp.wait_recv()
        k, w = q % 3, widths[q]

        def step(i):
            acc = jnp.zeros((TOK, w), F32)
            for c in range(2):
                o = rec[q][c, :, :, i].reshape(2 * TOK, w)
                for t in range(3):
                    acc = acc + jnp.dot(comb[k][i, c, t], o, preferred_element_type=F32)
            part[q][i] = acc

        loop(4, step)

    def far6(q):
        for i, d in enumerate(DIRS):
            x6[q][0].append(send(part[q].at[mod(p2[q] + 2), pl.ds(i * half_tok, half_tok)], pas6[q].at[i], peer(d2[q], d, core)))

    def rows6(q, i, half):
        return part[q].at[mod(p2[q] + DIRS[i]), pl.ds(half * half_tok, half_tok)], prec[q].at[i, pl.ds(half * half_tok, half_tok)]

    def near6(q):
        for i, d in enumerate(DIRS):
            x6[q][1].append(send(*rows6(q, i, 1 - i), peer(d2[q], d, core)))

    def forward6(q):
        for i, d in enumerate(DIRS):
            x6[q][0][i].wait_recv()
            mine, there = rows6(q, i, i)
            mine[...] = mine[...] + pas6[q][i]
            x6[q][1].append(send(mine, there, peer(d2[q], d, core)))

    def final(q):
        for cp in x6[q][1]:
            cp.wait_recv()
        total = part[q][p2[q]] + prec[q][0] + prec[q][1]
        xk = x_ref[:, :, :, offs[q]:offs[q] + widths[q]].reshape(TOK, widths[q]).astype(F32)
        y_ref[:, offs[q]:offs[q] + widths[q]] = (xk + total).astype(BF16)

    for q in W1:
        combine(q)
        far6(q)
        near6(q)
    for q in W2:
        combine(q)
        far6(q)
    for q in W1:
        forward6(q)
    for q in W2:
        near6(q)
    for q in W2:
        forward6(q)
    for q in W1 + W2:
        final(q)
    for q in range(NQ):
        for cr in range(2):
            x4[q][cr].sent()
        for cp in x5[q][0] + x5[q][1] + x6[q][0] + x6[q][1]:
            cp.wait_send()


N_COPIES = 3 * 6 + NQ * (16 + 13 + 13 + 6 + 6)


def solution(mesh):
    def local_layer(x_loc, ids_loc, gates_loc, w_g, w_u, w_d):
        tok, hid = x_loc.shape
        fdim = w_g.shape[2]
        widths = split_width(hid)
        f_tile = 256 if fdim % 256 == 0 else fdim
        x4 = x_loc.reshape(CORES, RING, CAP, hid)
        scratch = []
        each = lambda f: scratch.extend(f(w) for w in widths)
        for _ in range(3):
            each(lambda w: pltpu.VMEM(LEAD + (CAP, w), BF16))
        scratch += [pltpu.VMEM((RING, RING, 16, TOK), F32)] * 3
        scratch += [pltpu.VMEM((RING, RING, TOK, TOK), BF16)] * 3
        scratch += [pltpu.VMEM((RING, 2, 3, TOK, 2 * TOK), BF16)] * 3
        each(lambda w: pltpu.VMEM((2, CORES, 2, RING, CAP, w), BF16))
        each(lambda w: pltpu.VMEM((2, CORES, 2, RING, CAP, w), BF16))
        each(lambda w: pltpu.VMEM((2, RING, RING, CAP, w), BF16))
        each(lambda w: pltpu.VMEM((RING, TOK, w), F32))
        each(lambda w: pltpu.VMEM((2, TOK, w), F32))
        each(lambda w: pltpu.VMEM((2, TOK // 2, w), F32))
        scratch += [
            pltpu.VMEM((hid, fdim), BF16),
            pltpu.VMEM((hid, fdim), BF16),
            pltpu.VMEM((fdim, hid), BF16),
            pltpu.VMEM((2, 2 * RING * RING * CAP, fdim), BF16),
            pltpu.VMEM((16, TOK), F32),
            pltpu.SemaphoreType.DMA((N_COPIES,)),
            pltpu.SemaphoreType.DMA((N_COPIES,)),
            pltpu.SemaphoreType.DMA((3,)),
            pltpu.SemaphoreType.REGULAR((3, 2)),
        ]
        vm = pl.BlockSpec(memory_space=pltpu.VMEM)
        hbm = pl.BlockSpec(memory_space=pl.ANY)
        return pl.pallas_call(
            functools.partial(moe_kernel, widths, fdim, f_tile),
            out_shape=jax.ShapeDtypeStruct((tok, hid), BF16),
            in_specs=[vm, vm, vm, hbm, hbm, hbm],
            out_specs=vm,
            scratch_shapes=scratch,
            compiler_params=pltpu.CompilerParams(collective_id=0, has_side_effects=True, vmem_limit_bytes=67043328),
            name='moe',
        )(x4, ids_loc.T, gates_loc.T, w_g[0], w_u[0], w_d[0])

    tok_spec = P(TOKEN_AXES, None)
    w_spec = P(EXPERT_AXES, None, None)
    return jax.shard_map(local_layer, mesh=mesh, in_specs=(tok_spec, tok_spec, tok_spec, w_spec, w_spec, w_spec), out_specs=tok_spec, check_vma=False)
```

```python
import functools

import jax
import jax.numpy as jnp
from jax import lax
from jax.experimental import pallas as pl
from jax.experimental.pallas import tpu as pltpu
from jax.sharding import PartitionSpec as P

TOKEN_AXES = ('ez', 'ey', 'ex')
EXPERT_AXES = ('ex', 'ey', 'ez')
MESH = pl.DeviceIdType.MESH
F32 = jnp.float32
BF16 = jnp.bfloat16

Z, Y, X = 0, 1, 2
D1 = (Y, Z, X)
D2 = (Z, X, Y)
D3 = (X, Y, Z)
A_IS_D1 = (True, False, True)
RING = 4
CORES = 2
CAP = 16
TOK = 128
LEAD = (CORES, RING, RING, RING)


NQ = 6
W1, W2 = (0, 1, 2), (3, 4, 5)


def split_width(hid):
    tiles = hid // 128
    second = tiles * 3 // 8
    first = tiles - second
    thirds = lambda n: [n - 2 * (n // 3), n // 3, n // 3]
    return tuple(n * 128 for n in thirds(first) + thirds(second))


def moe_kernel(widths, fdim, f_tile, x_hbm, ids_hbm, gates_hbm, w1_hbm, w3_hbm, w2_hbm, y_hbm, *scr):
    it = iter(scr)
    take = lambda n: [next(it) for _ in range(n)]
    gat, til, rec = take(NQ), take(NQ), take(NQ)
    meta, sel, comb = take(3), take(3), take(3)
    pas3, pas4, pas5 = take(NQ), take(NQ), take(NQ)
    part, prec, pas6 = take(NQ), take(NQ), take(NQ)
    w1, w3, w2, act, meta_ref = take(5)
    x_ref, ids_ref, gates_ref, y_ref = take(4)
    send_sem, recv_sem, w_sem, in_sem, out_sem, credit = take(6)
    loads = [pltpu.make_async_copy(s, d, in_sem.at[i]) for i, (s, d) in enumerate(((ids_hbm, ids_ref), (gates_hbm, gates_ref), (x_hbm, x_ref)))]
    for c in loads:
        c.start()

    offs = [sum(widths[:q]) for q in range(NQ)]
    ez, ey, ex = lax.axis_index('ez'), lax.axis_index('ey'), lax.axis_index('ex')
    core = lax.rem(ex, CORES)
    pos = (ez, ey, ex // CORES)
    mod = lambda v: lax.rem(v + RING, RING)
    other = 1 - core

    strides = (1, RING, 2 * RING * RING)

    def turned(v, r):
        return [v[d] * (1 - r) + v[(d + 1) % 3] * r for d in range(3)]

    def peer(dim, off, c, lane=None):
        r = core if lane is None else lane
        q = [mod(pos[j] + off * ((1 - r) * int(j == dim) + r * int(j == (dim + 1) % 3))) for j in range(3)]
        return (q[0], q[1], q[2] * CORES + c)

    counter = [0]

    def send(src, dst, dev):
        i = counter[0]
        counter[0] += 1
        cp = pltpu.make_async_remote_copy(src, dst, send_sem.at[i], recv_sem.at[i], device_id=dev, device_id_type=MESH)
        cp.start()
        return cp

    bar = pltpu.get_barrier_semaphore()
    npeer = 0
    for dim in range(3):
        for off in (1, -1):
            for c in (core, other):
                pl.semaphore_signal(bar, inc=1, device_id=peer(dim, off, c, 0), device_id_type=MESH)
                npeer += 1
    pl.semaphore_signal(bar, inc=1, device_id=peer(0, 0, other), device_id_type=MESH)
    w_copies = [pltpu.make_async_copy(s, d, w_sem.at[i]) for i, (s, d) in enumerate(((w1_hbm, w1), (w3_hbm, w3), (w2_hbm, w2)))]
    for c in loads[:2]:
        c.wait()
    meta_ref[0:8] = ids_ref[...].astype(F32)
    meta_ref[8:16] = gates_ref[...]
    loads[2].wait()
    pl.semaphore_wait(bar, npeer + 1)

    DIRS = (1, -1)
    d1 = [D1[q % 3] for q in range(NQ)]
    d2 = [D2[q % 3] for q in range(NQ)]
    d3 = [D3[q % 3] for q in range(NQ)]
    a1 = [A_IS_D1[q % 3] for q in range(NQ)]
    lpos, lstr = turned(pos, core), turned(strides, core)
    opos = turned(pos, other)
    p1 = [lpos[d] for d in d1]
    p2 = [lpos[d] for d in d2]
    p3 = [lpos[d] for d in d3]
    p3_other = [opos[d] for d in d3]
    xcol = [x_ref.at[:, :, :, pl.ds(offs[q], widths[q])] for q in range(NQ)]
    unwaited = []

    def chunk(q, r):
        return gat[q].at[:, :, p2[q], mod(p1[q] + r)]

    m1 = [[None, None] for _ in range(3)]
    mf1 = [None] * 3
    m2 = [[None, None] for _ in range(3)]
    mf2 = [None] * 3
    g1 = [[None, None] for _ in range(NQ)]
    f1 = [[None, None] for _ in range(NQ)]
    g2 = [[[None] * 4, [None] * 4] for _ in range(NQ)]
    f2 = [[None] * 4 for _ in range(NQ)]

    def first_sends(wave):
        for q in wave:
            for i, d in enumerate(DIRS):
                if q < 3:
                    m1[q][i] = send(meta_ref, meta[q].at[p2[q], p1[q]], peer(d1[q], d, core))
                g1[q][i] = send(xcol[q], chunk(q, 0), peer(d1[q], d, core))
        for q in wave:
            for i, d in enumerate(DIRS):
                g2[q][i][0] = send(xcol[q], chunk(q, 0), peer(d2[q], d, core))

    def first_forwards(wave):
        for q in wave:
            for i, d in enumerate(DIRS):
                if q < 3:
                    m1[q][i].wait_recv()
                    if i == 0:
                        src = meta[q].at[p2[q], mod(p1[q] - 1)]
                        mf1[q] = send(src, src, peer(d1[q], 1, core))
                g1[q][i].wait_recv()
                half = chunk(q, -d).at[i]
                f1[q][i] = send(half, half, peer(d1[q], d, core))
        for q in wave:
            for i, d in enumerate(DIRS):
                for r in (1, 3):
                    g2[q][i][r] = send(chunk(q, r), chunk(q, r), peer(d2[q], d, core))

    def forward2(q, i, r):
        g2[q][i][r].wait_recv()
        src = gat[q].at[:, :, mod(p2[q] - DIRS[i]), mod(p1[q] + r)]
        f2[q][r] = send(src, src, peer(d2[q], DIRS[i], core))

    first_sends(W1)
    first_sends(W2)
    for c in w_copies:
        c.start()
    for q in range(NQ):
        gat[q][:, :, p2[q], p1[q]] = x_ref[:, :, :, offs[q]:offs[q] + widths[q]]
    for k in range(3):
        meta[k][p2[k], p1[k]] = meta_ref[...]
    first_forwards(W1)
    for k in range(3):
        mf1[k].wait_recv()
        for i, d in enumerate(DIRS):
            row = meta[k].at[p2[k]]
            m2[k][i] = send(row, row, peer(d2[k], d, core))

    def last_chunk(wave):
        for q in wave:
            for i, d in enumerate(DIRS):
                f1[q][i].wait_recv()
            for i, d in enumerate(DIRS):
                g2[q][i][2] = send(chunk(q, 2), chunk(q, 2), peer(d2[q], d, core))

    for q in W1:
        forward2(q, 0, 0)
    last_chunk(W1)
    first_forwards(W2)
    for k in range(3):
        for i in range(2):
            m2[k][i].wait_recv()
        src = meta[k].at[mod(p2[k] - 1)]
        mf2[k] = send(src, src, peer(d2[k], 1, core))

    tri = (lax.broadcasted_iota(jnp.int32, (TOK, TOK), 0) < lax.broadcasted_iota(jnp.int32, (TOK, TOK), 1)).astype(BF16)
    i8 = lax.broadcasted_iota(jnp.int32, (8, 1), 0)
    slot = lax.broadcasted_iota(jnp.int32, (8, CAP, TOK), 1).astype(F32)

    def experts8(k):
        base = lpos[D1[k]] * lstr[D1[k]] + lpos[D2[k]] * lstr[D2[k]]
        return (base + (i8 & 3) * lstr[D3[k]] + (i8 >> 2) * (RING * RING)).astype(F32)

    def picked(ids, evec):
        m = (ids[0:1, :] == evec).astype(F32)
        for j in range(1, 8):
            m = m + (ids[j:j + 1, :] == evec).astype(F32)
        return m

    def rank_of(m):
        rank = jnp.dot(m.astype(BF16), tri, preferred_element_type=F32)
        return jnp.where(m > 0.5, rank, -1.0)

    def onehot(k, i):
        evec = experts8(k)
        rm = rank_of(jnp.concatenate([picked(meta[k][i, j, 0:8], evec) for j in range(4)], axis=0))
        for j in range(4):
            hot = (rm[j * 8:(j + 1) * 8][:, None, :] == slot).astype(F32)
            sel[k][i, j] = hot.reshape(TOK, TOK).astype(BF16)

    def select(q, i):
        k, w = q % 3, widths[q]
        for j in range(4):
            rows = gat[q][:, :, i, j].reshape(TOK, w)
            out = jnp.dot(sel[k][i, j], rows, preferred_element_type=F32).astype(BF16).reshape(CORES, RING, CAP, w)
            if a1[q]:
                til[q][:, :, j, i] = out
            else:
                til[q][:, :, i, j] = out

    def loop(n, f):
        def body(i, carry):
            f(i)
            return carry
        lax.fori_loop(0, n, body, 0)

    for k in range(3):
        onehot(k, p2[k])
    for q in W1:
        forward2(q, 0, 1)
        forward2(q, 1, 3)
    for q in W1:
        select(q, p2[q])
    for q in W1:
        forward2(q, 1, 2)
    for q in W2:
        forward2(q, 0, 0)
    last_chunk(W2)
    for k in range(3):
        mf2[k].wait_recv()
        loop(3, lambda i, k=k: onehot(k, mod(p2[k] + 1 + i)))

    def gathered(q, near):
        if near:
            for i, r in ((0, 2), (0, 3), (1, 0), (1, 1)):
                g2[q][i][r].wait_recv()
            loop(2, lambda i, q=q: select(q, mod(p2[q] - 1 + 2 * i)))
        else:
            for r in range(4):
                f2[q][r].wait_recv()
            select(q, mod(p2[q] + 2))
            done = g1[q] + f1[q] + g2[q][0] + g2[q][1] + f2[q]
            if q < 3:
                done = done + m1[q] + [mf1[q]] + m2[q] + [mf2[q]]
            for c in done:
                c.wait_send()

    def sub(ref, q, c, d, half=None):
        a = slice(None) if half is None else pl.ds(2 * half, 2)
        return (ref.at[c, d, a], ref.at[c, a, d], ref.at[c, a, :, d])[q % 3]

    def til_block(ref, q, c, d, half=None):
        return ref.at[c, d] if half is None else ref.at[c, d, pl.ds(2 * half, 2)]

    class Leg:
        def __init__(self, q, cr, lane, src, src_block, dst, dst_block, pas):
            self.q, self.cr, self.lane, self.src, self.dst = q, cr, lane, src, dst
            self.src_block, self.dst_block, self.pas = src_block, dst_block, pas
            self.c = core if cr == 0 else other
            self.p = p3[q] if lane is core else p3_other[q]
            self.first, self.direct = [], []

        def out(self, d, half=None):
            return self.src_block(self.src, self.q, self.c, d, half)

        def into(self, d, half=None):
            return self.dst_block(self.dst, self.q, core, d, half)

        def far(self):
            for i, d in enumerate(DIRS):
                self.first.append(send(self.out(mod(self.p + 2), i), self.pas.at[i, self.cr], peer(d3[self.q], d, core, self.lane)))

        def near(self):
            for i, d in enumerate(DIRS):
                self.direct.append(send(self.out(mod(self.p + d)), self.into(self.p), peer(d3[self.q], d, self.c, self.lane)))
            if self.cr == 1:
                self.direct.append(send(self.out(self.p), self.into(self.p), peer(d3[self.q], 0, other, self.lane)))

        def forward(self):
            for i, d in enumerate(DIRS):
                self.first[i].wait_recv()
                self.direct.append(send(self.pas.at[i, self.cr], self.into(mod(self.p - d), i), peer(d3[self.q], d, self.c, self.lane)))

        def arrive(self):
            for cp in self.direct:
                cp.wait_recv()

        def sent(self):
            for cp in self.first + self.direct:
                cp.wait_send()

    def keep3(q):
        v = til[q][core, p3[q]]
        if q % 3 == 0:
            rec[q][core, p3[q]] = v
        elif q % 3 == 1:
            rec[q][core, :, p3[q]] = v
        else:
            rec[q][core, :, :, p3[q]] = v

    def keep4(q):
        if q % 3 == 0:
            v = til[q][core, p3[q]]
        elif q % 3 == 1:
            v = til[q][core, :, p3[q]]
        else:
            v = til[q][core, :, :, p3[q]]
        gat[q][core, p3[q]] = v

    x3 = [[Leg(q, cr, core, til[q], til_block, rec[q], sub, pas3[q]) for cr in range(2)] for q in range(NQ)]
    for q in W1:
        gathered(q, True)
    for q in W2:
        forward2(q, 0, 1)
        forward2(q, 1, 3)
    for q in W2:
        select(q, p2[q])
    for q in W1:
        gathered(q, False)
        x3[q][0].far()
    for q in W2:
        forward2(q, 1, 2)
    for q in W1:
        x3[q][0].near()
        x3[q][1].far()
    for q in W2:
        gathered(q, True)
    for q in W1:
        x3[q][0].forward()
    for q in W2:
        gathered(q, False)
        x3[q][0].far()
    for q in W2:
        x3[q][0].near()
        x3[q][1].far()
    for q in W2:
        x3[q][0].forward()
    for q in W1 + W2:
        x3[q][1].near()
    for q in W1 + W2:
        keep3(q)
    for q in W1 + W2:
        x3[q][1].forward()
    for c in w_copies:
        c.wait()

    x4 = [[Leg(q, cr, core if cr == 0 else other, til[q], sub, gat[q], til_block, pas4[q]) for cr in range(2)] for q in range(NQ)]
    rows = 2 * RING * RING * CAP
    for cr in range(2):
        c = core if cr == 0 else other
        for q in range(NQ):
            x3[q][cr].arrive()
        for q in range(NQ):
            x3[q][cr].sent()

        def hidden(i, c=c):
            xs = jnp.concatenate([rec[q][c, pl.ds(2 * i, 2)].reshape(rows, widths[q]) for q in range(NQ)], axis=1)
            for f in range(fdim // f_tile):
                cols = slice(f * f_tile, (f + 1) * f_tile)
                hg = jnp.dot(xs, w1[:, cols], preferred_element_type=F32)
                hu = jnp.dot(xs, w3[:, cols], preferred_element_type=F32)
                act[i, :, cols] = (hg * jax.nn.sigmoid(hg) * hu).astype(BF16)

        def down(wave, c=c):
            def step(i):
                lo, hi = offs[wave[0]], offs[wave[-1]] + widths[wave[-1]]
                o = jnp.dot(act[i], w2[:, lo:hi], preferred_element_type=F32).astype(BF16)
                for q in wave:
                    part_q = o[:, offs[q] - lo:offs[q] - lo + widths[q]]
                    til[q][c, pl.ds(2 * i, 2)] = part_q.reshape(2, RING, RING, CAP, widths[q])
            loop(2, step)

        loop(2, hidden)
        if cr == 1:
            for q in W1 + W2:
                x4[q][0].forward()
        down(W1)
        for q in W1:
            x4[q][cr].far()
        for q in W1:
            x4[q][cr].near()
        down(W2)
        for q in W2:
            x4[q][cr].far()
        if cr == 1:
            for q in W1:
                x4[q][1].forward()
        for q in W2:
            x4[q][cr].near()
        if cr == 0:
            for q in W1 + W2:
                keep4(q)
    for k in range(3):
        for i, d in enumerate(DIRS):
            pl.semaphore_signal(credit.at[k, i], inc=1, device_id=peer(D1[k], d, core), device_id_type=MESH)

    def weights(k, i):
        mrow = meta[k][i, p1[k]]
        ids, gates = mrow[0:8], mrow[8:16]
        own = lpos[D2[k]] * lstr[D2[k]]
        ms, gs = [], []
        for b in range(4):
            idx = i8 + b * 8
            d3e, d1e, ce = idx & 3, (idx >> 2) & 3, idx >> 4
            evec = (own + d3e * lstr[D3[k]] + d1e * lstr[D1[k]] + ce * (RING * RING)).astype(F32)
            m = jnp.zeros((8, TOK), F32)
            g = jnp.zeros((8, TOK), F32)
            for j in range(8):
                hit = ids[j:j + 1, :] == evec
                m = m + hit.astype(F32)
                g = g + jnp.where(hit, gates[j:j + 1, :], 0.0)
            ms.append(m)
            gs.append(g)
        rm = rank_of(jnp.concatenate(ms, axis=0))
        for b in range(4):
            hot = jnp.where(rm[b * 8:(b + 1) * 8][:, None, :] == slot, gs[b][:, None, :], 0.0).reshape(TOK, TOK).T
            hi = hot.astype(BF16)
            r1 = hot - hi.astype(F32)
            mid = r1.astype(BF16)
            lo = (r1 - mid.astype(F32)).astype(BF16)
            at = slice((b % 2) * TOK, (b % 2 + 1) * TOK)
            comb[k][i, b // 2, 0, :, at] = hi
            comb[k][i, b // 2, 1, :, at] = mid
            comb[k][i, b // 2, 2, :, at] = lo

    for q in W2:
        x4[q][1].forward()
    for k in range(3):
        loop(4, lambda i, k=k: weights(k, i))

    def from_src(ref, q, d, half=None):
        cs = slice(None) if half is None else half
        return ref.at[cs, :, d] if a1[q] else ref.at[cs, :, :, d]

    x5 = [([], []) for _ in range(NQ)]

    def arrive4(q):
        for cr in range(2):
            x4[q][cr].arrive()
        if q < 3:
            for i in range(2):
                pl.semaphore_wait(credit.at[q, i], 1)

    def far5(q):
        for i, d in enumerate(DIRS):
            x5[q][0].append(send(from_src(gat[q], q, mod(p1[q] + 2), i), pas5[q].at[i], peer(d1[q], d, core)))

    def near5(q):
        for i, d in enumerate(DIRS):
            x5[q][1].append(send(from_src(gat[q], q, mod(p1[q] + d)), rec[q].at[:, p1[q]], peer(d1[q], d, core)))

    def keep5(q):
        if a1[q]:
            rec[q][:, p1[q]] = gat[q][:, :, p1[q]]
        else:
            rec[q][:, p1[q]] = gat[q][:, :, :, p1[q]]

    def forward5(q):
        for i, d in enumerate(DIRS):
            x5[q][0][i].wait_recv()
            x5[q][1].append(send(pas5[q].at[i], rec[q].at[i, mod(p1[q] - d)], peer(d1[q], d, core)))

    for q in W1:
        arrive4(q)
        far5(q)
        near5(q)
    for q in W1:
        keep5(q)
    for q in W2:
        arrive4(q)
        far5(q)
    for q in W1:
        forward5(q)
    for q in W2:
        near5(q)
    for q in W2:
        keep5(q)
    for q in W2:
        forward5(q)

    x6 = [([], []) for _ in range(NQ)]
    half_tok = TOK // 2

    def combine(q):
        for cp in x5[q][1]:
            cp.wait_recv()
        k, w = q % 3, widths[q]

        def step(i):
            acc = jnp.zeros((TOK, w), F32)
            for c in range(2):
                o = rec[q][c, :, :, i].reshape(2 * TOK, w)
                for t in range(3):
                    acc = acc + jnp.dot(comb[k][i, c, t], o, preferred_element_type=F32)
            part[q][i] = acc

        return step

    def far6(q):
        for i, d in enumerate(DIRS):
            x6[q][0].append(send(part[q].at[mod(p2[q] + 2), pl.ds(i * half_tok, half_tok)], pas6[q].at[i], peer(d2[q], d, core)))

    def rows6(q, i, half):
        return part[q].at[mod(p2[q] + DIRS[i]), pl.ds(half * half_tok, half_tok)], prec[q].at[i, pl.ds(half * half_tok, half_tok)]

    def near6(q):
        for i, d in enumerate(DIRS):
            x6[q][1].append(send(*rows6(q, i, 1 - i), peer(d2[q], d, core)))

    def forward6(q):
        for i, d in enumerate(DIRS):
            x6[q][0][i].wait_recv()
            mine, there = rows6(q, i, i)
            mine[...] = mine[...] + pas6[q][i]
            x6[q][1].append(send(mine, there, peer(d2[q], d, core)))

    def final(q):
        for cp in x6[q][1]:
            cp.wait_recv()
        total = part[q][p2[q]] + prec[q][0] + prec[q][1]
        xk = x_ref[:, :, :, offs[q]:offs[q] + widths[q]].reshape(TOK, widths[q]).astype(F32)
        y_ref[:, offs[q]:offs[q] + widths[q]] = (xk + total).astype(BF16)
        cols = pl.ds(offs[q], widths[q])
        out = pltpu.make_async_copy(y_ref.at[:, cols], y_hbm.at[:, cols], out_sem.at[q])
        out.start()
        return out

    def far_sum(q):
        step = combine(q)
        step(mod(p2[q] + 2))
        far6(q)
        return step

    steps = {}
    for q in W1:
        steps[q] = far_sum(q)
    for q in W1:
        loop(3, lambda i, q=q: steps[q](mod(p2[q] + 3 + i)))
        near6(q)
    for q in W2:
        steps[q] = far_sum(q)
    for q in W1:
        forward6(q)
    for q in W2:
        loop(3, lambda i, q=q: steps[q](mod(p2[q] + 3 + i)))
        near6(q)
    for q in W2:
        forward6(q)
    outs = [final(q) for q in W1 + W2]
    for c in outs:
        c.wait()
    for q in range(NQ):
        for cr in range(2):
            x4[q][cr].sent()
        for cp in x5[q][0] + x5[q][1] + x6[q][0] + x6[q][1]:
            cp.wait_send()


N_COPIES = 3 * 6 + NQ * (16 + 13 + 13 + 6 + 6)


def solution(mesh):
    def local_layer(x_loc, ids_loc, gates_loc, w_g, w_u, w_d):
        tok, hid = x_loc.shape
        fdim = w_g.shape[2]
        widths = split_width(hid)
        f_tile = 256 if fdim % 256 == 0 else fdim
        x4 = x_loc.reshape(CORES, RING, CAP, hid)
        scratch = []
        each = lambda f: scratch.extend(f(w) for w in widths)
        for _ in range(3):
            each(lambda w: pltpu.VMEM(LEAD + (CAP, w), BF16))
        scratch += [pltpu.VMEM((RING, RING, 16, TOK), F32)] * 3
        scratch += [pltpu.VMEM((RING, RING, TOK, TOK), BF16)] * 3
        scratch += [pltpu.VMEM((RING, 2, 3, TOK, 2 * TOK), BF16)] * 3
        each(lambda w: pltpu.VMEM((2, CORES, 2, RING, CAP, w), BF16))
        each(lambda w: pltpu.VMEM((2, CORES, 2, RING, CAP, w), BF16))
        each(lambda w: pltpu.VMEM((2, RING, RING, CAP, w), BF16))
        each(lambda w: pltpu.VMEM((RING, TOK, w), F32))
        each(lambda w: pltpu.VMEM((2, TOK, w), F32))
        each(lambda w: pltpu.VMEM((2, TOK // 2, w), F32))
        scratch += [
            pltpu.VMEM((hid, fdim), BF16),
            pltpu.VMEM((hid, fdim), BF16),
            pltpu.VMEM((fdim, hid), BF16),
            pltpu.VMEM((2, 2 * RING * RING * CAP, fdim), BF16),
            pltpu.VMEM((16, TOK), F32),
            pltpu.VMEM(x4.shape, BF16),
            pltpu.VMEM((8, TOK), jnp.int32),
            pltpu.VMEM((8, TOK), F32),
            pltpu.VMEM((tok, hid), BF16),
            pltpu.SemaphoreType.DMA((N_COPIES,)),
            pltpu.SemaphoreType.DMA((N_COPIES,)),
            pltpu.SemaphoreType.DMA((3,)),
            pltpu.SemaphoreType.DMA((3,)),
            pltpu.SemaphoreType.DMA((NQ,)),
            pltpu.SemaphoreType.REGULAR((3, 2)),
        ]
        hbm = pl.BlockSpec(memory_space=pl.ANY)
        return pl.pallas_call(
            functools.partial(moe_kernel, widths, fdim, f_tile),
            out_shape=jax.ShapeDtypeStruct((tok, hid), BF16),
            in_specs=[hbm] * 6,
            out_specs=hbm,
            scratch_shapes=scratch,
            compiler_params=pltpu.CompilerParams(collective_id=0, has_side_effects=True, vmem_limit_bytes=62914560),
            name='moe',
        )(x4, ids_loc.T, gates_loc.T, w_g[0], w_u[0], w_d[0])

    tok_spec = P(TOKEN_AXES, None)
    w_spec = P(EXPERT_AXES, None, None)
    return jax.shard_map(local_layer, mesh=mesh, in_specs=(tok_spec, tok_spec, tok_spec, w_spec, w_spec, w_spec), out_specs=tok_spec, check_vma=False)
```

```python
import functools

import jax
import jax.numpy as jnp
from jax import lax
from jax.experimental import pallas as pl
from jax.experimental.pallas import tpu as pltpu
from jax.sharding import PartitionSpec as P

TOKEN_AXES = ('ez', 'ey', 'ex')
EXPERT_AXES = ('ex', 'ey', 'ez')
MESH = pl.DeviceIdType.MESH
F32 = jnp.float32
BF16 = jnp.bfloat16
BF16_MAX = float(jnp.finfo(jnp.bfloat16).max)

Z, Y, X = 0, 1, 2
D1 = (Y, Z, X)
D2 = (Z, X, Y)
D3 = (X, Y, Z)
A_IS_D1 = (True, False, True)
RING = 4
CORES = 2
CAP = 16
TOK = 128
LEAD = (CORES, RING, RING, RING)


NQ = 6
W1, W2 = (0, 1, 2), (3, 4, 5)


def split_width(hid):
    tiles = hid // 128
    second = tiles * 7 // 16
    first = tiles - second
    thirds = lambda n: [n - 2 * (n // 3), n // 3, n // 3]
    return tuple(n * 128 for n in thirds(first) + thirds(second))


def moe_kernel(widths, fdim, f_tile, x_hbm, ids_hbm, gates_hbm, w1_hbm, w3_hbm, w2_hbm, y_hbm, *scr):
    it = iter(scr)
    take = lambda n: [next(it) for _ in range(n)]
    gat, til, rec = take(NQ), take(NQ), take(NQ)
    meta, sel, comb = take(3), take(3), take(3)
    pas3, pas4, pas5 = take(NQ), take(NQ), take(NQ)
    part, prec, pas6 = take(NQ), take(NQ), take(NQ)
    w1, w3, w2, act, meta_ref = take(5)
    x_ref, ids_ref, gates_ref, y_ref = take(4)
    send_sem, recv_sem, w_sem, in_sem, out_sem, credit = take(6)
    loads = [pltpu.make_async_copy(s, d, in_sem.at[i]) for i, (s, d) in enumerate(((ids_hbm, ids_ref), (gates_hbm, gates_ref), (x_hbm, x_ref)))]
    for c in loads:
        c.start()

    offs = [sum(widths[:q]) for q in range(NQ)]
    ez, ey, ex = lax.axis_index('ez'), lax.axis_index('ey'), lax.axis_index('ex')
    core = lax.rem(ex, CORES)
    pos = (ez, ey, ex // CORES)
    mod = lambda v: lax.rem(v + RING, RING)
    other = 1 - core

    strides = (1, RING, 2 * RING * RING)

    def turned(v, r):
        return [v[d] * (1 - r) + v[(d + 1) % 3] * r for d in range(3)]

    def peer(dim, off, c, lane=None):
        r = core if lane is None else lane
        q = [mod(pos[j] + off * ((1 - r) * int(j == dim) + r * int(j == (dim + 1) % 3))) for j in range(3)]
        return (q[0], q[1], q[2] * CORES + c)

    counter = [0]

    def send(src, dst, dev):
        i = counter[0]
        counter[0] += 1
        cp = pltpu.make_async_remote_copy(src, dst, send_sem.at[i], recv_sem.at[i], device_id=dev, device_id_type=MESH)
        cp.start()
        return cp

    bar = pltpu.get_barrier_semaphore()
    npeer = 0
    for dim in range(3):
        for off in (1, -1):
            for c in (core, other):
                pl.semaphore_signal(bar, inc=1, device_id=peer(dim, off, c, 0), device_id_type=MESH)
                npeer += 1
    pl.semaphore_signal(bar, inc=1, device_id=peer(0, 0, other), device_id_type=MESH)
    w_copies = [pltpu.make_async_copy(s, d, w_sem.at[i]) for i, (s, d) in enumerate(((w1_hbm, w1), (w3_hbm, w3), (w2_hbm, w2)))]
    for c in loads[:2]:
        c.wait()
    meta_ref[0:8] = ids_ref[...].astype(F32)
    meta_ref[8:16] = gates_ref[...]
    loads[2].wait()
    pl.semaphore_wait(bar, npeer + 1)

    DIRS = (1, -1)
    d1 = [D1[q % 3] for q in range(NQ)]
    d2 = [D2[q % 3] for q in range(NQ)]
    d3 = [D3[q % 3] for q in range(NQ)]
    a1 = [A_IS_D1[q % 3] for q in range(NQ)]
    lpos, lstr = turned(pos, core), turned(strides, core)
    opos = turned(pos, other)
    p1 = [lpos[d] for d in d1]
    p2 = [lpos[d] for d in d2]
    p3 = [lpos[d] for d in d3]
    p3_other = [opos[d] for d in d3]
    xcol = [x_ref.at[:, :, :, pl.ds(offs[q], widths[q])] for q in range(NQ)]
    unwaited = []

    def chunk(q, r):
        return gat[q].at[:, :, p2[q], mod(p1[q] + r)]

    m1 = [[None, None] for _ in range(3)]
    mf1 = [None] * 3
    m2 = [[None, None] for _ in range(3)]
    mf2 = [None] * 3
    g1 = [[None, None] for _ in range(NQ)]
    f1 = [[None, None] for _ in range(NQ)]
    g2 = [[[None] * 4, [None] * 4] for _ in range(NQ)]
    f2 = [[None] * 4 for _ in range(NQ)]

    def first_sends(wave):
        for q in wave:
            for i, d in enumerate(DIRS):
                if q < 3:
                    m1[q][i] = send(meta_ref, meta[q].at[p2[q], p1[q]], peer(d1[q], d, core))
                g1[q][i] = send(xcol[q], chunk(q, 0), peer(d1[q], d, core))
        for q in wave:
            for i, d in enumerate(DIRS):
                g2[q][i][0] = send(xcol[q], chunk(q, 0), peer(d2[q], d, core))

    def first_forwards(wave):
        for q in wave:
            for i, d in enumerate(DIRS):
                if q < 3:
                    m1[q][i].wait_recv()
                    if i == 0:
                        src = meta[q].at[p2[q], mod(p1[q] - 1)]
                        mf1[q] = send(src, src, peer(d1[q], 1, core))
                g1[q][i].wait_recv()
                half = chunk(q, -d).at[i]
                f1[q][i] = send(half, half, peer(d1[q], d, core))
        for q in wave:
            for i, d in enumerate(DIRS):
                for r in (1, 3):
                    g2[q][i][r] = send(chunk(q, r), chunk(q, r), peer(d2[q], d, core))

    def forward2(q, i, r):
        g2[q][i][r].wait_recv()
        src = gat[q].at[:, :, mod(p2[q] - DIRS[i]), mod(p1[q] + r)]
        f2[q][r] = send(src, src, peer(d2[q], DIRS[i], core))

    first_sends(W1)
    first_sends(W2)
    for c in w_copies:
        c.start()
    for q in range(NQ):
        gat[q][:, :, p2[q], p1[q]] = x_ref[:, :, :, offs[q]:offs[q] + widths[q]]
    for k in range(3):
        meta[k][p2[k], p1[k]] = meta_ref[...]
    first_forwards(W1)
    for k in range(3):
        mf1[k].wait_recv()
        for i, d in enumerate(DIRS):
            row = meta[k].at[p2[k]]
            m2[k][i] = send(row, row, peer(d2[k], d, core))

    def last_chunk(wave):
        for q in wave:
            for i, d in enumerate(DIRS):
                f1[q][i].wait_recv()
            for i, d in enumerate(DIRS):
                g2[q][i][2] = send(chunk(q, 2), chunk(q, 2), peer(d2[q], d, core))

    for q in W1:
        forward2(q, 0, 0)
    last_chunk(W1)
    first_forwards(W2)
    for k in range(3):
        for i in range(2):
            m2[k][i].wait_recv()
        src = meta[k].at[mod(p2[k] - 1)]
        mf2[k] = send(src, src, peer(d2[k], 1, core))

    tri = (lax.broadcasted_iota(jnp.int32, (TOK, TOK), 0) < lax.broadcasted_iota(jnp.int32, (TOK, TOK), 1)).astype(BF16)
    i8 = lax.broadcasted_iota(jnp.int32, (8, 1), 0)
    slot = lax.broadcasted_iota(jnp.int32, (8, CAP, TOK), 1).astype(F32)

    def experts8(k):
        base = lpos[D1[k]] * lstr[D1[k]] + lpos[D2[k]] * lstr[D2[k]]
        return (base + (i8 & 3) * lstr[D3[k]] + (i8 >> 2) * (RING * RING)).astype(F32)

    def picked(ids, evec):
        m = (ids[0:1, :] == evec).astype(F32)
        for j in range(1, 8):
            m = m + (ids[j:j + 1, :] == evec).astype(F32)
        return m

    def rank_of(m):
        rank = jnp.dot(m.astype(BF16), tri, preferred_element_type=F32)
        return jnp.where(m > 0.5, rank, -1.0)

    def onehot(k, i):
        evec = experts8(k)
        rm = rank_of(jnp.concatenate([picked(meta[k][i, j, 0:8], evec) for j in range(4)], axis=0))
        for j in range(4):
            hot = (rm[j * 8:(j + 1) * 8][:, None, :] == slot).astype(F32)
            sel[k][i, j] = hot.reshape(TOK, TOK).astype(BF16)

    def select(q, i):
        k, w = q % 3, widths[q]
        for j in range(4):
            rows = gat[q][:, :, i, j].reshape(TOK, w)
            out = jnp.dot(sel[k][i, j], rows, preferred_element_type=F32).astype(BF16).reshape(CORES, RING, CAP, w)
            if a1[q]:
                til[q][:, :, j, i] = out
            else:
                til[q][:, :, i, j] = out

    def loop(n, f):
        def body(i, carry):
            f(i)
            return carry
        lax.fori_loop(0, n, body, 0)

    for k in range(3):
        onehot(k, p2[k])
    for q in W1:
        forward2(q, 0, 1)
        forward2(q, 1, 3)
    for q in W1:
        select(q, p2[q])
    for q in W1:
        forward2(q, 1, 2)
    for q in W2:
        forward2(q, 0, 0)
    last_chunk(W2)
    for k in range(3):
        mf2[k].wait_recv()
        loop(3, lambda i, k=k: onehot(k, mod(p2[k] + 1 + i)))

    def gathered(q, near):
        if near:
            for i, r in ((0, 2), (0, 3), (1, 0), (1, 1)):
                g2[q][i][r].wait_recv()
            loop(2, lambda i, q=q: select(q, mod(p2[q] - 1 + 2 * i)))
        else:
            for r in range(4):
                f2[q][r].wait_recv()
            select(q, mod(p2[q] + 2))
            done = g1[q] + f1[q] + g2[q][0] + g2[q][1] + f2[q]
            if q < 3:
                done = done + m1[q] + [mf1[q]] + m2[q] + [mf2[q]]
            for c in done:
                c.wait_send()

    def sub(ref, q, c, d, half=None):
        a = slice(None) if half is None else pl.ds(2 * half, 2)
        return (ref.at[c, d, a], ref.at[c, a, d], ref.at[c, a, :, d])[q % 3]

    def til_block(ref, q, c, d, half=None):
        return ref.at[c, d] if half is None else ref.at[c, d, pl.ds(2 * half, 2)]

    class Leg:
        def __init__(self, q, cr, lane, src, src_block, dst, dst_block, pas):
            self.q, self.cr, self.lane, self.src, self.dst = q, cr, lane, src, dst
            self.src_block, self.dst_block, self.pas = src_block, dst_block, pas
            self.c = core if cr == 0 else other
            self.p = p3[q] if lane is core else p3_other[q]
            self.first, self.direct = [], []

        def out(self, d, half=None):
            return self.src_block(self.src, self.q, self.c, d, half)

        def into(self, d, half=None):
            return self.dst_block(self.dst, self.q, core, d, half)

        def far(self):
            for i, d in enumerate(DIRS):
                self.first.append(send(self.out(mod(self.p + 2), i), self.pas.at[i, self.cr], peer(d3[self.q], d, core, self.lane)))

        def near(self):
            for i, d in enumerate(DIRS):
                self.direct.append(send(self.out(mod(self.p + d)), self.into(self.p), peer(d3[self.q], d, self.c, self.lane)))
            if self.cr == 1:
                self.direct.append(send(self.out(self.p), self.into(self.p), peer(d3[self.q], 0, other, self.lane)))

        def forward(self):
            for i, d in enumerate(DIRS):
                self.first[i].wait_recv()
                self.direct.append(send(self.pas.at[i, self.cr], self.into(mod(self.p - d), i), peer(d3[self.q], d, self.c, self.lane)))

        def arrive(self):
            for cp in self.direct:
                cp.wait_recv()

        def sent(self):
            for cp in self.first + self.direct:
                cp.wait_send()

    def keep3(q):
        v = til[q][core, p3[q]]
        if q % 3 == 0:
            rec[q][core, p3[q]] = v
        elif q % 3 == 1:
            rec[q][core, :, p3[q]] = v
        else:
            rec[q][core, :, :, p3[q]] = v

    def keep4(q):
        if q % 3 == 0:
            v = til[q][core, p3[q]]
        elif q % 3 == 1:
            v = til[q][core, :, p3[q]]
        else:
            v = til[q][core, :, :, p3[q]]
        gat[q][core, p3[q]] = v

    x3 = [[Leg(q, cr, core, til[q], til_block, rec[q], sub, pas3[q]) for cr in range(2)] for q in range(NQ)]
    for q in W1:
        gathered(q, True)
    for q in W2:
        forward2(q, 0, 1)
        forward2(q, 1, 3)
    for q in W2:
        select(q, p2[q])
    for q in W1:
        gathered(q, False)
        x3[q][0].far()
    for q in W2:
        forward2(q, 1, 2)
    for q in W1:
        x3[q][0].near()
        x3[q][1].far()
    for q in W2:
        gathered(q, True)
    for q in W1:
        x3[q][0].forward()
    for q in W2:
        gathered(q, False)
        x3[q][0].far()
    for q in W2:
        x3[q][0].near()
        x3[q][1].far()
    for q in W2:
        x3[q][0].forward()
    for q in W1 + W2:
        x3[q][1].near()
    for q in W1 + W2:
        keep3(q)
    for q in W1 + W2:
        x3[q][1].forward()
    for c in w_copies:
        c.wait()

    x4 = [[Leg(q, cr, core if cr == 0 else other, til[q], sub, gat[q], til_block, pas4[q]) for cr in range(2)] for q in range(NQ)]
    rows = 2 * RING * RING * CAP
    for cr in range(2):
        c = core if cr == 0 else other
        for q in range(NQ):
            x3[q][cr].arrive()
        for q in range(NQ):
            x3[q][cr].sent()

        def hidden(i, c=c):
            xs = jnp.concatenate([rec[q][c, pl.ds(2 * i, 2)].reshape(rows, widths[q]) for q in range(NQ)], axis=1)
            for f in range(fdim // f_tile):
                cols = slice(f * f_tile, (f + 1) * f_tile)
                hg = jnp.dot(xs, w1[:, cols], preferred_element_type=F32)
                hu = jnp.dot(xs, w3[:, cols], preferred_element_type=F32)
                act[i, :, cols] = (hg * jax.nn.sigmoid(hg) * hu).astype(BF16)

        def down(wave, c=c):
            def step(i):
                lo, hi = offs[wave[0]], offs[wave[-1]] + widths[wave[-1]]
                o = jnp.dot(act[i], w2[:, lo:hi], preferred_element_type=F32).astype(BF16)
                for q in wave:
                    part_q = o[:, offs[q] - lo:offs[q] - lo + widths[q]]
                    til[q][c, pl.ds(2 * i, 2)] = part_q.reshape(2, RING, RING, CAP, widths[q])
            loop(2, step)

        loop(2, hidden)
        if cr == 1:
            for q in W1 + W2:
                x4[q][0].forward()
        down(W1)
        for q in W1:
            x4[q][cr].far()
        for q in W1:
            x4[q][cr].near()
        down(W2)
        for q in W2:
            x4[q][cr].far()
        if cr == 1:
            for q in W1:
                x4[q][1].forward()
        for q in W2:
            x4[q][cr].near()
        if cr == 0:
            for q in W1 + W2:
                keep4(q)
    for k in range(3):
        for i, d in enumerate(DIRS):
            pl.semaphore_signal(credit.at[k, i], inc=1, device_id=peer(D1[k], d, core), device_id_type=MESH)

    def weights(k, i):
        mrow = meta[k][i, p1[k]]
        ids, gates = mrow[0:8], mrow[8:16]
        own = lpos[D2[k]] * lstr[D2[k]]
        ms, gs = [], []
        for b in range(4):
            idx = i8 + b * 8
            d3e, d1e, ce = idx & 3, (idx >> 2) & 3, idx >> 4
            evec = (own + d3e * lstr[D3[k]] + d1e * lstr[D1[k]] + ce * (RING * RING)).astype(F32)
            m = jnp.zeros((8, TOK), F32)
            g = jnp.zeros((8, TOK), F32)
            for j in range(8):
                hit = ids[j:j + 1, :] == evec
                m = m + hit.astype(F32)
                g = g + jnp.where(hit, gates[j:j + 1, :], 0.0)
            ms.append(m)
            gs.append(g)
        rm = rank_of(jnp.concatenate(ms, axis=0))
        for b in range(4):
            hot = jnp.where(rm[b * 8:(b + 1) * 8][:, None, :] == slot, gs[b][:, None, :], 0.0).reshape(TOK, TOK).T
            hi = jnp.minimum(hot, BF16_MAX).astype(BF16)
            r1 = hot - hi.astype(F32)
            mid = r1.astype(BF16)
            lo = (r1 - mid.astype(F32)).astype(BF16)
            at = slice((b % 2) * TOK, (b % 2 + 1) * TOK)
            comb[k][i, b // 2, 0, :, at] = hi
            comb[k][i, b // 2, 1, :, at] = mid
            comb[k][i, b // 2, 2, :, at] = lo

    for q in W2:
        x4[q][1].forward()
    for k in range(3):
        loop(4, lambda i, k=k: weights(k, i))

    def from_src(ref, q, d, half=None):
        cs = slice(None) if half is None else half
        return ref.at[cs, :, d] if a1[q] else ref.at[cs, :, :, d]

    x5 = [([], []) for _ in range(NQ)]

    def arrive4(q):
        for cr in range(2):
            x4[q][cr].arrive()
        if q < 3:
            for i in range(2):
                pl.semaphore_wait(credit.at[q, i], 1)

    def far5(q):
        for i, d in enumerate(DIRS):
            x5[q][0].append(send(from_src(gat[q], q, mod(p1[q] + 2), i), pas5[q].at[i], peer(d1[q], d, core)))

    def near5(q):
        for i, d in enumerate(DIRS):
            x5[q][1].append(send(from_src(gat[q], q, mod(p1[q] + d)), rec[q].at[:, p1[q]], peer(d1[q], d, core)))

    def keep5(q):
        if a1[q]:
            rec[q][:, p1[q]] = gat[q][:, :, p1[q]]
        else:
            rec[q][:, p1[q]] = gat[q][:, :, :, p1[q]]

    def forward5(q):
        for i, d in enumerate(DIRS):
            x5[q][0][i].wait_recv()
            x5[q][1].append(send(pas5[q].at[i], rec[q].at[i, mod(p1[q] - d)], peer(d1[q], d, core)))

    for q in W1:
        arrive4(q)
        far5(q)
        near5(q)
    for q in W1:
        keep5(q)
    for q in W2:
        arrive4(q)
        far5(q)
    for q in W1:
        forward5(q)
    for q in W2:
        near5(q)
    for q in W2:
        keep5(q)
    for q in W2:
        forward5(q)

    x6 = [([], []) for _ in range(NQ)]
    half_tok = TOK // 2

    def combine(q):
        for cp in x5[q][1]:
            cp.wait_recv()
        k, w = q % 3, widths[q]

        def step(i):
            acc = jnp.zeros((TOK, w), F32)
            for c in range(2):
                o = rec[q][c, :, :, i].reshape(2 * TOK, w)
                for t in range(3):
                    acc = acc + jnp.dot(comb[k][i, c, t], o, preferred_element_type=F32)
            part[q][i] = acc

        return step

    def far6(q):
        for i, d in enumerate(DIRS):
            x6[q][0].append(send(part[q].at[mod(p2[q] + 2), pl.ds(i * half_tok, half_tok)], pas6[q].at[i], peer(d2[q], d, core)))

    def rows6(q, i, half):
        return part[q].at[mod(p2[q] + DIRS[i]), pl.ds(half * half_tok, half_tok)], prec[q].at[i, pl.ds(half * half_tok, half_tok)]

    def near6(q):
        for i, d in enumerate(DIRS):
            x6[q][1].append(send(*rows6(q, i, 1 - i), peer(d2[q], d, core)))

    def forward6(q):
        for i, d in enumerate(DIRS):
            x6[q][0][i].wait_recv()
            mine, there = rows6(q, i, i)
            mine[...] = mine[...] + pas6[q][i]
            x6[q][1].append(send(mine, there, peer(d2[q], d, core)))

    def final(q):
        for cp in x6[q][1]:
            cp.wait_recv()
        total = part[q][p2[q]] + prec[q][0] + prec[q][1]
        xk = x_ref[:, :, :, offs[q]:offs[q] + widths[q]].reshape(TOK, widths[q]).astype(F32)
        y_ref[:, offs[q]:offs[q] + widths[q]] = (xk + total).astype(BF16)
        cols = pl.ds(offs[q], widths[q])
        out = pltpu.make_async_copy(y_ref.at[:, cols], y_hbm.at[:, cols], out_sem.at[q])
        out.start()
        return out

    def far_sum(q):
        step = combine(q)
        step(mod(p2[q] + 2))
        far6(q)
        return step

    steps = {}
    for q in W1:
        steps[q] = far_sum(q)
    for q in W1:
        loop(3, lambda i, q=q: steps[q](mod(p2[q] + 3 + i)))
        near6(q)
    for q in W2:
        steps[q] = far_sum(q)
    for q in W1:
        forward6(q)
    for q in W2:
        loop(3, lambda i, q=q: steps[q](mod(p2[q] + 3 + i)))
        near6(q)
    for q in W2:
        forward6(q)
    outs = [final(q) for q in W1 + W2]
    for c in outs:
        c.wait()
    for q in range(NQ):
        for cr in range(2):
            x4[q][cr].sent()
        for cp in x5[q][0] + x5[q][1] + x6[q][0] + x6[q][1]:
            cp.wait_send()


N_COPIES = 3 * 6 + NQ * (16 + 13 + 13 + 6 + 6)


def solution(mesh):
    def local_layer(x_loc, ids_loc, gates_loc, w_g, w_u, w_d):
        tok, hid = x_loc.shape
        fdim = w_g.shape[2]
        widths = split_width(hid)
        f_tile = 256 if fdim % 256 == 0 else fdim
        x4 = x_loc.reshape(CORES, RING, CAP, hid)
        scratch = []
        each = lambda f: scratch.extend(f(w) for w in widths)
        for _ in range(3):
            each(lambda w: pltpu.VMEM(LEAD + (CAP, w), BF16))
        scratch += [pltpu.VMEM((RING, RING, 16, TOK), F32)] * 3
        scratch += [pltpu.VMEM((RING, RING, TOK, TOK), BF16)] * 3
        scratch += [pltpu.VMEM((RING, 2, 3, TOK, 2 * TOK), BF16)] * 3
        each(lambda w: pltpu.VMEM((2, CORES, 2, RING, CAP, w), BF16))
        each(lambda w: pltpu.VMEM((2, CORES, 2, RING, CAP, w), BF16))
        each(lambda w: pltpu.VMEM((2, RING, RING, CAP, w), BF16))
        each(lambda w: pltpu.VMEM((RING, TOK, w), F32))
        each(lambda w: pltpu.VMEM((2, TOK, w), F32))
        each(lambda w: pltpu.VMEM((2, TOK // 2, w), F32))
        scratch += [
            pltpu.VMEM((hid, fdim), BF16),
            pltpu.VMEM((hid, fdim), BF16),
            pltpu.VMEM((fdim, hid), BF16),
            pltpu.VMEM((2, 2 * RING * RING * CAP, fdim), BF16),
            pltpu.VMEM((16, TOK), F32),
            pltpu.VMEM(x4.shape, BF16),
            pltpu.VMEM((8, TOK), jnp.int32),
            pltpu.VMEM((8, TOK), F32),
            pltpu.VMEM((tok, hid), BF16),
            pltpu.SemaphoreType.DMA((N_COPIES,)),
            pltpu.SemaphoreType.DMA((N_COPIES,)),
            pltpu.SemaphoreType.DMA((3,)),
            pltpu.SemaphoreType.DMA((3,)),
            pltpu.SemaphoreType.DMA((NQ,)),
            pltpu.SemaphoreType.REGULAR((3, 2)),
        ]
        hbm = pl.BlockSpec(memory_space=pl.ANY)
        return pl.pallas_call(
            functools.partial(moe_kernel, widths, fdim, f_tile),
            out_shape=jax.ShapeDtypeStruct((tok, hid), BF16),
            in_specs=[hbm] * 6,
            out_specs=hbm,
            scratch_shapes=scratch,
            compiler_params=pltpu.CompilerParams(collective_id=0, has_side_effects=True, vmem_limit_bytes=62914560),
            name='moe',
        )(x4, ids_loc.T, gates_loc.T, w_g[0], w_u[0], w_d[0])

    tok_spec = P(TOKEN_AXES, None)
    w_spec = P(EXPERT_AXES, None, None)
    return jax.shard_map(local_layer, mesh=mesh, in_specs=(tok_spec, tok_spec, tok_spec, w_spec, w_spec, w_spec), out_specs=tok_spec, check_vma=False)
```

```python
import functools

import jax
import jax.numpy as jnp
from jax import lax
from jax.experimental import pallas as pl
from jax.experimental.pallas import tpu as pltpu
from jax.sharding import PartitionSpec as P

TOKEN_AXES = ('ez', 'ey', 'ex')
EXPERT_AXES = ('ex', 'ey', 'ez')
MESH = pl.DeviceIdType.MESH
F32 = jnp.float32
BF16 = jnp.bfloat16
BF16_MAX = float(jnp.finfo(jnp.bfloat16).max)

Z, Y, X = 0, 1, 2
D1 = (Y, Z, X)
D2 = (Z, X, Y)
D3 = (X, Y, Z)
A_IS_D1 = (True, False, True)
RING = 4
CORES = 2
CAP = 16
TOK = 128
LEAD = (CORES, RING, RING, RING)


NQ = 6
W1, W2 = (0, 1, 2), (3, 4, 5)


def split_width(hid):
    tiles = hid // 128
    second = tiles * 7 // 16
    first = tiles - second
    thirds = lambda n: [n - 2 * (n // 3), n // 3, n // 3]
    return tuple(n * 128 for n in thirds(first) + thirds(second))


def moe_kernel(widths, fdim, f_tile, x_hbm, ids_hbm, gates_hbm, w1_hbm, w3_hbm, w2_hbm, y_hbm, *scr):
    it = iter(scr)
    take = lambda n: [next(it) for _ in range(n)]
    gat, til, rec = take(NQ), take(NQ), take(NQ)
    meta, sel, comb = take(3), take(3), take(3)
    pas3, pas4, pas5 = take(NQ), take(NQ), take(NQ)
    part, prec, pas6 = take(NQ), take(NQ), take(NQ)
    w1, w3, w2, act, meta_ref = take(5)
    x_ref, ids_ref, gates_ref, y_ref = take(4)
    send_sem, recv_sem, w_sem, in_sem, out_sem, credit = take(6)
    loads = [pltpu.make_async_copy(s, d, in_sem.at[i]) for i, (s, d) in enumerate(((ids_hbm, ids_ref), (gates_hbm, gates_ref), (x_hbm, x_ref)))]
    for c in loads:
        c.start()

    offs = [sum(widths[:q]) for q in range(NQ)]
    ez, ey, ex = lax.axis_index('ez'), lax.axis_index('ey'), lax.axis_index('ex')
    core = lax.rem(ex, CORES)
    pos = (ez, ey, ex // CORES)
    mod = lambda v: lax.rem(v + RING, RING)
    other = 1 - core

    strides = (1, RING, 2 * RING * RING)

    def turned(v, r):
        return [v[d] * (1 - r) + v[(d + 1) % 3] * r for d in range(3)]

    def peer(dim, off, c, lane=None):
        r = core if lane is None else lane
        q = [mod(pos[j] + off * ((1 - r) * int(j == dim) + r * int(j == (dim + 1) % 3))) for j in range(3)]
        return (q[0], q[1], q[2] * CORES + c)

    counter = [0]

    def send(src, dst, dev):
        i = counter[0]
        counter[0] += 1
        cp = pltpu.make_async_remote_copy(src, dst, send_sem.at[i], recv_sem.at[i], device_id=dev, device_id_type=MESH)
        cp.start()
        return cp

    bar = pltpu.get_barrier_semaphore()
    npeer = 0
    for dim in range(3):
        for off in (1, -1):
            for c in (core, other):
                pl.semaphore_signal(bar, inc=1, device_id=peer(dim, off, c, 0), device_id_type=MESH)
                npeer += 1
    pl.semaphore_signal(bar, inc=1, device_id=peer(0, 0, other), device_id_type=MESH)
    w_copies = [pltpu.make_async_copy(s, d, w_sem.at[i]) for i, (s, d) in enumerate(((w1_hbm, w1), (w3_hbm, w3), (w2_hbm, w2)))]
    for c in loads[:2]:
        c.wait()
    meta_ref[0:8] = ids_ref[...].astype(F32)
    meta_ref[8:16] = gates_ref[...]
    loads[2].wait()
    pl.semaphore_wait(bar, npeer + 1)

    DIRS = (1, -1)
    d1 = [D1[q % 3] for q in range(NQ)]
    d2 = [D2[q % 3] for q in range(NQ)]
    d3 = [D3[q % 3] for q in range(NQ)]
    a1 = [A_IS_D1[q % 3] for q in range(NQ)]
    lpos, lstr = turned(pos, core), turned(strides, core)
    opos = turned(pos, other)
    p1 = [lpos[d] for d in d1]
    p2 = [lpos[d] for d in d2]
    p3 = [lpos[d] for d in d3]
    p3_other = [opos[d] for d in d3]
    xcol = [x_ref.at[:, :, :, pl.ds(offs[q], widths[q])] for q in range(NQ)]
    unwaited = []

    def chunk(q, r):
        return gat[q].at[:, :, p2[q], mod(p1[q] + r)]

    m1 = [[None, None] for _ in range(3)]
    mf1 = [None] * 3
    m2 = [[None, None] for _ in range(3)]
    mf2 = [None] * 3
    g1 = [[None, None] for _ in range(NQ)]
    f1 = [[None, None] for _ in range(NQ)]
    g2 = [[[None] * 4, [None] * 4] for _ in range(NQ)]
    f2 = [[None] * 4 for _ in range(NQ)]

    def first_sends(wave):
        for q in wave:
            for i, d in enumerate(DIRS):
                if q < 3:
                    m1[q][i] = send(meta_ref, meta[q].at[p2[q], p1[q]], peer(d1[q], d, core))
                g1[q][i] = send(xcol[q], chunk(q, 0), peer(d1[q], d, core))
        for q in wave:
            for i, d in enumerate(DIRS):
                g2[q][i][0] = send(xcol[q], chunk(q, 0), peer(d2[q], d, core))

    def first_forwards(wave):
        for q in wave:
            for i, d in enumerate(DIRS):
                if q < 3:
                    m1[q][i].wait_recv()
                    if i == 0:
                        src = meta[q].at[p2[q], mod(p1[q] - 1)]
                        mf1[q] = send(src, src, peer(d1[q], 1, core))
                g1[q][i].wait_recv()
                half = chunk(q, -d).at[i]
                f1[q][i] = send(half, half, peer(d1[q], d, core))
        for q in wave:
            for i, d in enumerate(DIRS):
                for r in (1, 3):
                    g2[q][i][r] = send(chunk(q, r), chunk(q, r), peer(d2[q], d, core))

    def forward2(q, i, r):
        g2[q][i][r].wait_recv()
        src = gat[q].at[:, :, mod(p2[q] - DIRS[i]), mod(p1[q] + r)]
        f2[q][r] = send(src, src, peer(d2[q], DIRS[i], core))

    first_sends(W1)
    first_sends(W2)
    for c in w_copies:
        c.start()
    for q in range(NQ):
        gat[q][:, :, p2[q], p1[q]] = x_ref[:, :, :, offs[q]:offs[q] + widths[q]]
    for k in range(3):
        meta[k][p2[k], p1[k]] = meta_ref[...]
    first_forwards(W1)
    for k in range(3):
        mf1[k].wait_recv()
        for i, d in enumerate(DIRS):
            row = meta[k].at[p2[k]]
            m2[k][i] = send(row, row, peer(d2[k], d, core))

    def last_chunk(wave):
        for q in wave:
            for i, d in enumerate(DIRS):
                f1[q][i].wait_recv()
            for i, d in enumerate(DIRS):
                g2[q][i][2] = send(chunk(q, 2), chunk(q, 2), peer(d2[q], d, core))

    for q in W1:
        forward2(q, 0, 0)
    last_chunk(W1)
    first_forwards(W2)
    for k in range(3):
        for i in range(2):
            m2[k][i].wait_recv()
        src = meta[k].at[mod(p2[k] - 1)]
        mf2[k] = send(src, src, peer(d2[k], 1, core))

    tri = (lax.broadcasted_iota(jnp.int32, (TOK, TOK), 0) < lax.broadcasted_iota(jnp.int32, (TOK, TOK), 1)).astype(BF16)
    i8 = lax.broadcasted_iota(jnp.int32, (8, 1), 0)
    slot = lax.broadcasted_iota(jnp.int32, (8, CAP, TOK), 1).astype(F32)

    def experts8(k):
        base = lpos[D1[k]] * lstr[D1[k]] + lpos[D2[k]] * lstr[D2[k]]
        return (base + (i8 & 3) * lstr[D3[k]] + (i8 >> 2) * (RING * RING)).astype(F32)

    def picked(ids, evec):
        m = (ids[0:1, :] == evec).astype(F32)
        for j in range(1, 8):
            m = m + (ids[j:j + 1, :] == evec).astype(F32)
        return m

    def rank_of(m):
        rank = jnp.dot(m.astype(BF16), tri, preferred_element_type=F32)
        return jnp.where(m > 0.5, rank, -1.0)

    def onehot(k, i):
        evec = experts8(k)
        rm = rank_of(jnp.concatenate([picked(meta[k][i, j, 0:8], evec) for j in range(4)], axis=0))
        for j in range(4):
            hot = (rm[j * 8:(j + 1) * 8][:, None, :] == slot).astype(F32)
            sel[k][i, j] = hot.reshape(TOK, TOK).astype(BF16)

    def select(q, i):
        k, w = q % 3, widths[q]
        for j in range(4):
            rows = gat[q][:, :, i, j].reshape(TOK, w)
            out = jnp.dot(sel[k][i, j], rows, preferred_element_type=F32).astype(BF16).reshape(CORES, RING, CAP, w)
            if a1[q]:
                til[q][:, :, j, i] = out
            else:
                til[q][:, :, i, j] = out

    def loop(n, f):
        def body(i, carry):
            f(i)
            return carry
        lax.fori_loop(0, n, body, 0)

    for k in range(3):
        onehot(k, p2[k])
    for q in W1:
        forward2(q, 0, 1)
        forward2(q, 1, 3)
    for q in W1:
        select(q, p2[q])
    for q in W1:
        forward2(q, 1, 2)
    for q in W2:
        forward2(q, 0, 0)
    last_chunk(W2)
    for k in range(3):
        mf2[k].wait_recv()
        loop(3, lambda i, k=k: onehot(k, mod(p2[k] + 1 + i)))

    def gathered(q, near):
        if near:
            for i, r in ((0, 2), (0, 3), (1, 0), (1, 1)):
                g2[q][i][r].wait_recv()
            loop(2, lambda i, q=q: select(q, mod(p2[q] - 1 + 2 * i)))
        else:
            for r in range(4):
                f2[q][r].wait_recv()
            select(q, mod(p2[q] + 2))
            done = g1[q] + f1[q] + g2[q][0] + g2[q][1] + f2[q]
            if q < 3:
                done = done + m1[q] + [mf1[q]] + m2[q] + [mf2[q]]
            for c in done:
                c.wait_send()

    def sub(ref, q, c, d, half=None):
        a = slice(None) if half is None else pl.ds(2 * half, 2)
        return (ref.at[c, d, a], ref.at[c, a, d], ref.at[c, a, :, d])[q % 3]

    def til_block(ref, q, c, d, half=None):
        return ref.at[c, d] if half is None else ref.at[c, d, pl.ds(2 * half, 2)]

    class Leg:
        def __init__(self, q, cr, lane, src, src_block, dst, dst_block, pas):
            self.q, self.cr, self.lane, self.src, self.dst = q, cr, lane, src, dst
            self.src_block, self.dst_block, self.pas = src_block, dst_block, pas
            self.c = core if cr == 0 else other
            self.p = p3[q] if lane is core else p3_other[q]
            self.first, self.direct = [], []

        def out(self, d, half=None):
            return self.src_block(self.src, self.q, self.c, d, half)

        def into(self, d, half=None):
            return self.dst_block(self.dst, self.q, core, d, half)

        def far(self):
            for i, d in enumerate(DIRS):
                self.first.append(send(self.out(mod(self.p + 2), i), self.pas.at[i, self.cr], peer(d3[self.q], d, core, self.lane)))

        def near(self):
            for i, d in enumerate(DIRS):
                self.direct.append(send(self.out(mod(self.p + d)), self.into(self.p), peer(d3[self.q], d, self.c, self.lane)))
            if self.cr == 1:
                self.direct.append(send(self.out(self.p), self.into(self.p), peer(d3[self.q], 0, other, self.lane)))

        def forward(self):
            for i, d in enumerate(DIRS):
                self.first[i].wait_recv()
                self.direct.append(send(self.pas.at[i, self.cr], self.into(mod(self.p - d), i), peer(d3[self.q], d, self.c, self.lane)))

        def arrive(self):
            for cp in self.direct:
                cp.wait_recv()

        def sent(self):
            for cp in self.first + self.direct:
                cp.wait_send()

    def keep3(q):
        v = til[q][core, p3[q]]
        if q % 3 == 0:
            rec[q][core, p3[q]] = v
        elif q % 3 == 1:
            rec[q][core, :, p3[q]] = v
        else:
            rec[q][core, :, :, p3[q]] = v

    def keep4(q):
        if q % 3 == 0:
            v = til[q][core, p3[q]]
        elif q % 3 == 1:
            v = til[q][core, :, p3[q]]
        else:
            v = til[q][core, :, :, p3[q]]
        gat[q][core, p3[q]] = v

    x3 = [[Leg(q, cr, core, til[q], til_block, rec[q], sub, pas3[q]) for cr in range(2)] for q in range(NQ)]
    for q in W1:
        gathered(q, True)
    for q in W2:
        forward2(q, 0, 1)
        forward2(q, 1, 3)
    for q in W2:
        select(q, p2[q])
    for q in W1:
        gathered(q, False)
        x3[q][0].far()
    for q in W2:
        forward2(q, 1, 2)
    for q in W1:
        x3[q][0].near()
    for q in W2:
        gathered(q, True)
    for q in W1:
        x3[q][0].forward()
    for q in W2:
        gathered(q, False)
        x3[q][0].far()
    for q in W2:
        x3[q][0].near()
    for q in W1:
        x3[q][1].far()
    for q in W2:
        x3[q][0].forward()
    for q in W2:
        x3[q][1].far()
    for q in W1 + W2:
        x3[q][1].near()
    for q in W1 + W2:
        keep3(q)
    for c in w_copies:
        c.wait()

    x4 = [[Leg(q, cr, core if cr == 0 else other, til[q], sub, gat[q], til_block, pas4[q]) for cr in range(2)] for q in range(NQ)]
    rows = 2 * RING * RING * CAP
    for cr in range(2):
        c = core if cr == 0 else other
        for q in range(NQ):
            x3[q][cr].arrive()
        for q in range(NQ):
            x3[q][cr].sent()

        def hidden(i, c=c):
            xs = jnp.concatenate([rec[q][c, pl.ds(2 * i, 2)].reshape(rows, widths[q]) for q in range(NQ)], axis=1)
            for f in range(fdim // f_tile):
                cols = slice(f * f_tile, (f + 1) * f_tile)
                hg = jnp.dot(xs, w1[:, cols], preferred_element_type=F32)
                hu = jnp.dot(xs, w3[:, cols], preferred_element_type=F32)
                act[i, :, cols] = (hg * jax.nn.sigmoid(hg) * hu).astype(BF16)

        def down(wave, c=c):
            def step(i):
                lo, hi = offs[wave[0]], offs[wave[-1]] + widths[wave[-1]]
                o = jnp.dot(act[i], w2[:, lo:hi], preferred_element_type=F32).astype(BF16)
                for q in wave:
                    part_q = o[:, offs[q] - lo:offs[q] - lo + widths[q]]
                    til[q][c, pl.ds(2 * i, 2)] = part_q.reshape(2, RING, RING, CAP, widths[q])
            loop(2, step)

        hidden(0)
        if cr == 0:
            for q in W1 + W2:
                x3[q][1].forward()
        hidden(1)
        if cr == 1:
            for q in W1 + W2:
                x4[q][0].forward()
        down(W1)
        for q in W1:
            x4[q][cr].far()
        for q in W1:
            x4[q][cr].near()
        down(W2)
        for q in W2:
            x4[q][cr].far()
        if cr == 1:
            for q in W1:
                x4[q][1].forward()
        for q in W2:
            x4[q][cr].near()
        if cr == 0:
            for q in W1 + W2:
                keep4(q)
    for k in range(3):
        for i, d in enumerate(DIRS):
            pl.semaphore_signal(credit.at[k, i], inc=1, device_id=peer(D1[k], d, core), device_id_type=MESH)

    def weights(k, i):
        mrow = meta[k][i, p1[k]]
        ids, gates = mrow[0:8], mrow[8:16]
        own = lpos[D2[k]] * lstr[D2[k]]
        ms, gs = [], []
        for b in range(4):
            idx = i8 + b * 8
            d3e, d1e, ce = idx & 3, (idx >> 2) & 3, idx >> 4
            evec = (own + d3e * lstr[D3[k]] + d1e * lstr[D1[k]] + ce * (RING * RING)).astype(F32)
            m = jnp.zeros((8, TOK), F32)
            g = jnp.zeros((8, TOK), F32)
            for j in range(8):
                hit = ids[j:j + 1, :] == evec
                m = m + hit.astype(F32)
                g = g + jnp.where(hit, gates[j:j + 1, :], 0.0)
            ms.append(m)
            gs.append(g)
        rm = rank_of(jnp.concatenate(ms, axis=0))
        for b in range(4):
            hot = jnp.where(rm[b * 8:(b + 1) * 8][:, None, :] == slot, gs[b][:, None, :], 0.0).reshape(TOK, TOK).T
            hi = jnp.minimum(hot, BF16_MAX).astype(BF16)
            r1 = hot - hi.astype(F32)
            mid = r1.astype(BF16)
            lo = (r1 - mid.astype(F32)).astype(BF16)
            at = slice((b % 2) * TOK, (b % 2 + 1) * TOK)
            comb[k][i, b // 2, 0, :, at] = hi
            comb[k][i, b // 2, 1, :, at] = mid
            comb[k][i, b // 2, 2, :, at] = lo

    for q in W2:
        x4[q][1].forward()
    for k in range(3):
        loop(4, lambda i, k=k: weights(k, i))

    def from_src(ref, q, d, half=None):
        cs = slice(None) if half is None else half
        return ref.at[cs, :, d] if a1[q] else ref.at[cs, :, :, d]

    x5 = [([], []) for _ in range(NQ)]

    def arrive4(q):
        for cr in range(2):
            x4[q][cr].arrive()
        if q < 3:
            for i in range(2):
                pl.semaphore_wait(credit.at[q, i], 1)

    def far5(q):
        for i, d in enumerate(DIRS):
            x5[q][0].append(send(from_src(gat[q], q, mod(p1[q] + 2), i), pas5[q].at[i], peer(d1[q], d, core)))

    def near5(q):
        for i, d in enumerate(DIRS):
            x5[q][1].append(send(from_src(gat[q], q, mod(p1[q] + d)), rec[q].at[:, p1[q]], peer(d1[q], d, core)))

    def keep5(q):
        if a1[q]:
            rec[q][:, p1[q]] = gat[q][:, :, p1[q]]
        else:
            rec[q][:, p1[q]] = gat[q][:, :, :, p1[q]]

    def forward5(q):
        for i, d in enumerate(DIRS):
            x5[q][0][i].wait_recv()
            x5[q][1].append(send(pas5[q].at[i], rec[q].at[i, mod(p1[q] - d)], peer(d1[q], d, core)))

    for q in W1:
        arrive4(q)
        far5(q)
        near5(q)
    for q in W1:
        keep5(q)
    for q in W2:
        arrive4(q)
        far5(q)
    for q in W1:
        forward5(q)
    for q in W2:
        near5(q)
    for q in W2:
        keep5(q)
    for q in W2:
        forward5(q)

    x6 = [([], []) for _ in range(NQ)]
    half_tok = TOK // 2

    def combine(q):
        for cp in x5[q][1]:
            cp.wait_recv()
        k, w = q % 3, widths[q]

        def step(i):
            acc = jnp.zeros((TOK, w), F32)
            for c in range(2):
                o = rec[q][c, :, :, i].reshape(2 * TOK, w)
                for t in range(3):
                    acc = acc + jnp.dot(comb[k][i, c, t], o, preferred_element_type=F32)
            part[q][i] = acc

        return step

    def far6(q):
        for i, d in enumerate(DIRS):
            x6[q][0].append(send(part[q].at[mod(p2[q] + 2), pl.ds(i * half_tok, half_tok)], pas6[q].at[i], peer(d2[q], d, core)))

    def rows6(q, i, half):
        return part[q].at[mod(p2[q] + DIRS[i]), pl.ds(half * half_tok, half_tok)], prec[q].at[i, pl.ds(half * half_tok, half_tok)]

    def near6(q):
        for i, d in enumerate(DIRS):
            x6[q][1].append(send(*rows6(q, i, 1 - i), peer(d2[q], d, core)))

    def forward6(q):
        for i, d in enumerate(DIRS):
            x6[q][0][i].wait_recv()
            mine, there = rows6(q, i, i)
            mine[...] = mine[...] + pas6[q][i]
            x6[q][1].append(send(mine, there, peer(d2[q], d, core)))

    def final(q):
        for cp in x6[q][1]:
            cp.wait_recv()
        total = part[q][p2[q]] + prec[q][0] + prec[q][1]
        xk = x_ref[:, :, :, offs[q]:offs[q] + widths[q]].reshape(TOK, widths[q]).astype(F32)
        y_ref[:, offs[q]:offs[q] + widths[q]] = (xk + total).astype(BF16)
        cols = pl.ds(offs[q], widths[q])
        out = pltpu.make_async_copy(y_ref.at[:, cols], y_hbm.at[:, cols], out_sem.at[q])
        out.start()
        return out

    def far_sum(q):
        step = combine(q)
        step(mod(p2[q] + 2))
        far6(q)
        return step

    steps = {}
    for q in W1:
        steps[q] = far_sum(q)
    for q in W1:
        loop(3, lambda i, q=q: steps[q](mod(p2[q] + 3 + i)))
        near6(q)
    for q in W2:
        steps[q] = far_sum(q)
    for q in W1:
        forward6(q)
    for q in W2:
        loop(3, lambda i, q=q: steps[q](mod(p2[q] + 3 + i)))
        near6(q)
    for q in W2:
        forward6(q)
    outs = [final(q) for q in W1 + W2]
    for c in outs:
        c.wait()
    for q in range(NQ):
        for cr in range(2):
            x4[q][cr].sent()
        for cp in x5[q][0] + x5[q][1] + x6[q][0] + x6[q][1]:
            cp.wait_send()


N_COPIES = 3 * 6 + NQ * (16 + 13 + 13 + 6 + 6)


def solution(mesh):
    def local_layer(x_loc, ids_loc, gates_loc, w_g, w_u, w_d):
        tok, hid = x_loc.shape
        fdim = w_g.shape[2]
        widths = split_width(hid)
        f_tile = 256 if fdim % 256 == 0 else fdim
        x4 = x_loc.reshape(CORES, RING, CAP, hid)
        scratch = []
        each = lambda f: scratch.extend(f(w) for w in widths)
        for _ in range(3):
            each(lambda w: pltpu.VMEM(LEAD + (CAP, w), BF16))
        scratch += [pltpu.VMEM((RING, RING, 16, TOK), F32)] * 3
        scratch += [pltpu.VMEM((RING, RING, TOK, TOK), BF16)] * 3
        scratch += [pltpu.VMEM((RING, 2, 3, TOK, 2 * TOK), BF16)] * 3
        each(lambda w: pltpu.VMEM((2, CORES, 2, RING, CAP, w), BF16))
        each(lambda w: pltpu.VMEM((2, CORES, 2, RING, CAP, w), BF16))
        each(lambda w: pltpu.VMEM((2, RING, RING, CAP, w), BF16))
        each(lambda w: pltpu.VMEM((RING, TOK, w), F32))
        each(lambda w: pltpu.VMEM((2, TOK, w), F32))
        each(lambda w: pltpu.VMEM((2, TOK // 2, w), F32))
        scratch += [
            pltpu.VMEM((hid, fdim), BF16),
            pltpu.VMEM((hid, fdim), BF16),
            pltpu.VMEM((fdim, hid), BF16),
            pltpu.VMEM((2, 2 * RING * RING * CAP, fdim), BF16),
            pltpu.VMEM((16, TOK), F32),
            pltpu.VMEM(x4.shape, BF16),
            pltpu.VMEM((8, TOK), jnp.int32),
            pltpu.VMEM((8, TOK), F32),
            pltpu.VMEM((tok, hid), BF16),
            pltpu.SemaphoreType.DMA((N_COPIES,)),
            pltpu.SemaphoreType.DMA((N_COPIES,)),
            pltpu.SemaphoreType.DMA((3,)),
            pltpu.SemaphoreType.DMA((3,)),
            pltpu.SemaphoreType.DMA((NQ,)),
            pltpu.SemaphoreType.REGULAR((3, 2)),
        ]
        hbm = pl.BlockSpec(memory_space=pl.ANY)
        return pl.pallas_call(
            functools.partial(moe_kernel, widths, fdim, f_tile),
            out_shape=jax.ShapeDtypeStruct((tok, hid), BF16),
            in_specs=[hbm] * 6,
            out_specs=hbm,
            scratch_shapes=scratch,
            compiler_params=pltpu.CompilerParams(collective_id=0, has_side_effects=True, vmem_limit_bytes=62914560),
            name='moe',
        )(x4, ids_loc.T, gates_loc.T, w_g[0], w_u[0], w_d[0])

    tok_spec = P(TOKEN_AXES, None)
    w_spec = P(EXPERT_AXES, None, None)
    return jax.shard_map(local_layer, mesh=mesh, in_specs=(tok_spec, tok_spec, tok_spec, w_spec, w_spec, w_spec), out_specs=tok_spec, check_vma=False)
```

```python
import functools

import jax
import jax.numpy as jnp
from jax import lax
from jax.experimental import pallas as pl
from jax.experimental.pallas import tpu as pltpu
from jax.sharding import PartitionSpec as P

TOKEN_AXES = ('ez', 'ey', 'ex')
EXPERT_AXES = ('ex', 'ey', 'ez')
MESH = pl.DeviceIdType.MESH
F32 = jnp.float32
BF16 = jnp.bfloat16
BF16_MAX = float(jnp.finfo(jnp.bfloat16).max)

Z, Y, X = 0, 1, 2
D1 = (Y, Z, X)
D2 = (Z, X, Y)
D3 = (X, Y, Z)
A_IS_D1 = (True, False, True)
RING = 4
CORES = 2
CAP = 16
TOK = 128
LEAD = (CORES, RING, RING, RING)


NQ = 6
W1, W2 = (0, 1, 2), (3, 4, 5)


def split_width(hid):
    tiles = hid // 128
    second = tiles * 7 // 16
    first = tiles - second
    thirds = lambda n: [n - 2 * (n // 3), n // 3, n // 3]
    return tuple(n * 128 for n in thirds(first) + thirds(second))


def moe_kernel(widths, fdim, f_tile, x_hbm, ids_hbm, gates_hbm, w1_hbm, w3_hbm, w2_hbm, y_hbm, *scr):
    it = iter(scr)
    take = lambda n: [next(it) for _ in range(n)]
    gat, til, rec = take(NQ), take(NQ), take(NQ)
    meta, sel, comb = take(3), take(3), take(3)
    pas3, pas4, pas5 = take(NQ), take(NQ), take(NQ)
    part, prec, pas6 = take(NQ), take(NQ), take(NQ)
    w1, w3, w2, act, meta_ref = take(5)
    x_ref, ids_ref, gates_ref, y_ref = take(4)
    send_sem, recv_sem, w_sem, in_sem, out_sem, credit = take(6)
    loads = [pltpu.make_async_copy(s, d, in_sem.at[i]) for i, (s, d) in enumerate(((ids_hbm, ids_ref), (gates_hbm, gates_ref), (x_hbm, x_ref)))]
    for c in loads:
        c.start()

    offs = [sum(widths[:q]) for q in range(NQ)]
    ez, ey, ex = lax.axis_index('ez'), lax.axis_index('ey'), lax.axis_index('ex')
    core = lax.rem(ex, CORES)
    pos = (ez, ey, ex // CORES)
    mod = lambda v: lax.rem(v + RING, RING)
    other = 1 - core

    strides = (1, RING, 2 * RING * RING)

    def turned(v, r):
        return [v[d] * (1 - r) + v[(d + 1) % 3] * r for d in range(3)]

    def peer(dim, off, c, lane=None):
        r = core if lane is None else lane
        q = [mod(pos[j] + off * ((1 - r) * int(j == dim) + r * int(j == (dim + 1) % 3))) for j in range(3)]
        return (q[0], q[1], q[2] * CORES + c)

    counter = [0]

    def send(src, dst, dev):
        i = counter[0]
        counter[0] += 1
        cp = pltpu.make_async_remote_copy(src, dst, send_sem.at[i], recv_sem.at[i], device_id=dev, device_id_type=MESH)
        cp.start()
        return cp

    bar = pltpu.get_barrier_semaphore()
    npeer = 0
    for dim in range(3):
        for off in (1, -1):
            for c in (core, other):
                pl.semaphore_signal(bar, inc=1, device_id=peer(dim, off, c, 0), device_id_type=MESH)
                npeer += 1
    pl.semaphore_signal(bar, inc=1, device_id=peer(0, 0, other), device_id_type=MESH)
    w_copies = [pltpu.make_async_copy(s, d, w_sem.at[i]) for i, (s, d) in enumerate(((w1_hbm, w1), (w3_hbm, w3), (w2_hbm, w2)))]
    for c in loads[:2]:
        c.wait()
    meta_ref[0:8] = ids_ref[...].astype(F32)
    meta_ref[8:16] = gates_ref[...]
    loads[2].wait()
    pl.semaphore_wait(bar, npeer + 1)

    DIRS = (1, -1)
    d1 = [D1[q % 3] for q in range(NQ)]
    d2 = [D2[q % 3] for q in range(NQ)]
    d3 = [D3[q % 3] for q in range(NQ)]
    a1 = [A_IS_D1[q % 3] for q in range(NQ)]
    lpos, lstr = turned(pos, core), turned(strides, core)
    opos = turned(pos, other)
    p1 = [lpos[d] for d in d1]
    p2 = [lpos[d] for d in d2]
    p3 = [lpos[d] for d in d3]
    p3_other = [opos[d] for d in d3]
    xcol = [x_ref.at[:, :, :, pl.ds(offs[q], widths[q])] for q in range(NQ)]
    unwaited = []

    def chunk(q, r):
        return gat[q].at[:, :, p2[q], mod(p1[q] + r)]

    m1 = [[None, None] for _ in range(3)]
    mf1 = [None] * 3
    m2 = [[None, None] for _ in range(3)]
    mf2 = [None] * 3
    g1 = [[None, None] for _ in range(NQ)]
    f1 = [[None, None] for _ in range(NQ)]
    g2 = [[[None] * 4, [None] * 4] for _ in range(NQ)]
    f2 = [[None] * 4 for _ in range(NQ)]

    def first_sends(wave):
        for q in wave:
            for i, d in enumerate(DIRS):
                if q < 3:
                    m1[q][i] = send(meta_ref, meta[q].at[p2[q], p1[q]], peer(d1[q], d, core))
                g1[q][i] = send(xcol[q], chunk(q, 0), peer(d1[q], d, core))
        for q in wave:
            for i, d in enumerate(DIRS):
                g2[q][i][0] = send(xcol[q], chunk(q, 0), peer(d2[q], d, core))

    def first_forwards(wave):
        for q in wave:
            for i, d in enumerate(DIRS):
                if q < 3:
                    m1[q][i].wait_recv()
                    if i == 0:
                        src = meta[q].at[p2[q], mod(p1[q] - 1)]
                        mf1[q] = send(src, src, peer(d1[q], 1, core))
                g1[q][i].wait_recv()
                half = chunk(q, -d).at[i]
                f1[q][i] = send(half, half, peer(d1[q], d, core))
        for q in wave:
            for i, d in enumerate(DIRS):
                for r in (1, 3):
                    g2[q][i][r] = send(chunk(q, r), chunk(q, r), peer(d2[q], d, core))

    def forward2(q, i, r):
        g2[q][i][r].wait_recv()
        src = gat[q].at[:, :, mod(p2[q] - DIRS[i]), mod(p1[q] + r)]
        f2[q][r] = send(src, src, peer(d2[q], DIRS[i], core))

    first_sends(W1)
    first_sends(W2)
    for c in w_copies:
        c.start()
    for q in range(NQ):
        gat[q][:, :, p2[q], p1[q]] = x_ref[:, :, :, offs[q]:offs[q] + widths[q]]
    for k in range(3):
        meta[k][p2[k], p1[k]] = meta_ref[...]
    first_forwards(W1)
    for k in range(3):
        mf1[k].wait_recv()
        for i, d in enumerate(DIRS):
            row = meta[k].at[p2[k]]
            m2[k][i] = send(row, row, peer(d2[k], d, core))

    def last_chunk(wave):
        for q in wave:
            for i, d in enumerate(DIRS):
                f1[q][i].wait_recv()
            for i, d in enumerate(DIRS):
                g2[q][i][2] = send(chunk(q, 2), chunk(q, 2), peer(d2[q], d, core))

    for q in W1:
        forward2(q, 0, 0)
    last_chunk(W1)
    first_forwards(W2)
    for k in range(3):
        for i in range(2):
            m2[k][i].wait_recv()
        src = meta[k].at[mod(p2[k] - 1)]
        mf2[k] = send(src, src, peer(d2[k], 1, core))

    tri = (lax.broadcasted_iota(jnp.int32, (TOK, TOK), 0) < lax.broadcasted_iota(jnp.int32, (TOK, TOK), 1)).astype(BF16)
    i8 = lax.broadcasted_iota(jnp.int32, (8, 1), 0)
    slot = lax.broadcasted_iota(jnp.int32, (8, CAP, TOK), 1).astype(F32)

    def experts8(k):
        base = lpos[D1[k]] * lstr[D1[k]] + lpos[D2[k]] * lstr[D2[k]]
        return (base + (i8 & 3) * lstr[D3[k]] + (i8 >> 2) * (RING * RING)).astype(F32)

    def picked(ids, evec):
        m = (ids[0:1, :] == evec).astype(F32)
        for j in range(1, 8):
            m = m + (ids[j:j + 1, :] == evec).astype(F32)
        return m

    def rank_of(m):
        rank = jnp.dot(m.astype(BF16), tri, preferred_element_type=F32)
        return jnp.where(m > 0.5, rank, -1.0)

    def onehot(k, i):
        evec = experts8(k)
        rm = rank_of(jnp.concatenate([picked(meta[k][i, j, 0:8], evec) for j in range(4)], axis=0))
        for j in range(4):
            hot = (rm[j * 8:(j + 1) * 8][:, None, :] == slot).astype(F32)
            sel[k][i, j] = hot.reshape(TOK, TOK).astype(BF16)

    def select(q, i):
        k, w = q % 3, widths[q]
        for j in range(4):
            rows = gat[q][:, :, i, j].reshape(TOK, w)
            out = jnp.dot(sel[k][i, j], rows, preferred_element_type=F32).astype(BF16).reshape(CORES, RING, CAP, w)
            if a1[q]:
                til[q][:, :, j, i] = out
            else:
                til[q][:, :, i, j] = out

    def loop(n, f):
        def body(i, carry):
            f(i)
            return carry
        lax.fori_loop(0, n, body, 0)

    for k in range(3):
        onehot(k, p2[k])
    for q in W1:
        forward2(q, 0, 1)
        forward2(q, 1, 3)
    for q in W1:
        select(q, p2[q])
    for q in W1:
        forward2(q, 1, 2)
    for q in W2:
        forward2(q, 0, 0)
    last_chunk(W2)
    for k in range(3):
        mf2[k].wait_recv()
    loop(3, lambda i: [onehot(k, mod(p2[k] + 1 + i)) for k in range(3)])

    def gathered(q, near):
        if near:
            for i, r in ((0, 2), (0, 3), (1, 0), (1, 1)):
                g2[q][i][r].wait_recv()
            loop(2, lambda i, q=q: select(q, mod(p2[q] - 1 + 2 * i)))
        else:
            for r in range(4):
                f2[q][r].wait_recv()
            select(q, mod(p2[q] + 2))
            done = g1[q] + f1[q] + g2[q][0] + g2[q][1] + f2[q]
            if q < 3:
                done = done + m1[q] + [mf1[q]] + m2[q] + [mf2[q]]
            for c in done:
                c.wait_send()

    def sub(ref, q, c, d, half=None):
        a = slice(None) if half is None else pl.ds(2 * half, 2)
        return (ref.at[c, d, a], ref.at[c, a, d], ref.at[c, a, :, d])[q % 3]

    def til_block(ref, q, c, d, half=None):
        return ref.at[c, d] if half is None else ref.at[c, d, pl.ds(2 * half, 2)]

    class Leg:
        def __init__(self, q, cr, lane, src, src_block, dst, dst_block, pas):
            self.q, self.cr, self.lane, self.src, self.dst = q, cr, lane, src, dst
            self.src_block, self.dst_block, self.pas = src_block, dst_block, pas
            self.c = core if cr == 0 else other
            self.p = p3[q] if lane is core else p3_other[q]
            self.first, self.direct = [], []

        def out(self, d, half=None):
            return self.src_block(self.src, self.q, self.c, d, half)

        def into(self, d, half=None):
            return self.dst_block(self.dst, self.q, core, d, half)

        def far(self):
            for i, d in enumerate(DIRS):
                self.first.append(send(self.out(mod(self.p + 2), i), self.pas.at[i, self.cr], peer(d3[self.q], d, core, self.lane)))

        def near(self):
            for i, d in enumerate(DIRS):
                self.direct.append(send(self.out(mod(self.p + d)), self.into(self.p), peer(d3[self.q], d, self.c, self.lane)))
            if self.cr == 1:
                self.direct.append(send(self.out(self.p), self.into(self.p), peer(d3[self.q], 0, other, self.lane)))

        def forward(self):
            for i, d in enumerate(DIRS):
                self.first[i].wait_recv()
                self.direct.append(send(self.pas.at[i, self.cr], self.into(mod(self.p - d), i), peer(d3[self.q], d, self.c, self.lane)))

        def arrive(self):
            for cp in self.direct:
                cp.wait_recv()

        def sent(self):
            for cp in self.first + self.direct:
                cp.wait_send()

    def keep3(q):
        v = til[q][core, p3[q]]
        if q % 3 == 0:
            rec[q][core, p3[q]] = v
        elif q % 3 == 1:
            rec[q][core, :, p3[q]] = v
        else:
            rec[q][core, :, :, p3[q]] = v

    def keep4(q):
        if q % 3 == 0:
            v = til[q][core, p3[q]]
        elif q % 3 == 1:
            v = til[q][core, :, p3[q]]
        else:
            v = til[q][core, :, :, p3[q]]
        gat[q][core, p3[q]] = v

    x3 = [[Leg(q, cr, core, til[q], til_block, rec[q], sub, pas3[q]) for cr in range(2)] for q in range(NQ)]
    for q in W1:
        gathered(q, True)
    for q in W2:
        forward2(q, 0, 1)
        forward2(q, 1, 3)
    for q in W2:
        select(q, p2[q])
    for q in W1:
        gathered(q, False)
        x3[q][0].far()
    for q in W2:
        forward2(q, 1, 2)
    for q in W1:
        x3[q][0].near()
    for q in W2:
        gathered(q, True)
    for q in W1:
        x3[q][0].forward()
    for q in W2:
        gathered(q, False)
        x3[q][0].far()
    for q in W2:
        x3[q][0].near()
    for q in W1:
        x3[q][1].far()
    for q in W2:
        x3[q][0].forward()
    for q in W2:
        x3[q][1].far()
    for q in W1 + W2:
        x3[q][1].near()
    for q in W1 + W2:
        keep3(q)
    for c in w_copies:
        c.wait()

    x4 = [[Leg(q, cr, core if cr == 0 else other, til[q], sub, gat[q], til_block, pas4[q]) for cr in range(2)] for q in range(NQ)]
    rows = 2 * RING * RING * CAP
    for cr in range(2):
        c = core if cr == 0 else other
        for q in range(NQ):
            x3[q][cr].arrive()
        for q in range(NQ):
            x3[q][cr].sent()

        def hidden(i, c=c):
            xs = jnp.concatenate([rec[q][c, pl.ds(2 * i, 2)].reshape(rows, widths[q]) for q in range(NQ)], axis=1)
            for f in range(fdim // f_tile):
                cols = slice(f * f_tile, (f + 1) * f_tile)
                hg = jnp.dot(xs, w1[:, cols], preferred_element_type=F32)
                hu = jnp.dot(xs, w3[:, cols], preferred_element_type=F32)
                act[i, :, cols] = (hg * jax.nn.sigmoid(hg) * hu).astype(BF16)

        def down(wave, c=c):
            def step(i):
                lo, hi = offs[wave[0]], offs[wave[-1]] + widths[wave[-1]]
                o = jnp.dot(act[i], w2[:, lo:hi], preferred_element_type=F32).astype(BF16)
                for q in wave:
                    part_q = o[:, offs[q] - lo:offs[q] - lo + widths[q]]
                    til[q][c, pl.ds(2 * i, 2)] = part_q.reshape(2, RING, RING, CAP, widths[q])
            loop(2, step)

        hidden(0)
        if cr == 0:
            for q in W1 + W2:
                x3[q][1].forward()
        hidden(1)
        if cr == 1:
            for q in W1 + W2:
                x4[q][0].forward()
        down(W1)
        for q in W1:
            x4[q][cr].far()
        for q in W1:
            x4[q][cr].near()
        down(W2)
        for q in W2:
            x4[q][cr].far()
        if cr == 1:
            for q in W1:
                x4[q][1].forward()
        for q in W2:
            x4[q][cr].near()
        if cr == 0:
            for q in W1 + W2:
                keep4(q)
    for k in range(3):
        for i, d in enumerate(DIRS):
            pl.semaphore_signal(credit.at[k, i], inc=1, device_id=peer(D1[k], d, core), device_id_type=MESH)

    def weights(k, i):
        mrow = meta[k][i, p1[k]]
        ids, gates = mrow[0:8], mrow[8:16]
        own = lpos[D2[k]] * lstr[D2[k]]
        ms, gs = [], []
        for b in range(4):
            idx = i8 + b * 8
            d3e, d1e, ce = idx & 3, (idx >> 2) & 3, idx >> 4
            evec = (own + d3e * lstr[D3[k]] + d1e * lstr[D1[k]] + ce * (RING * RING)).astype(F32)
            m = jnp.zeros((8, TOK), F32)
            g = jnp.zeros((8, TOK), F32)
            for j in range(8):
                hit = ids[j:j + 1, :] == evec
                m = m + hit.astype(F32)
                g = g + jnp.where(hit, gates[j:j + 1, :], 0.0)
            ms.append(m)
            gs.append(g)
        rm = rank_of(jnp.concatenate(ms, axis=0))
        for b in range(4):
            hot = jnp.where(rm[b * 8:(b + 1) * 8][:, None, :] == slot, gs[b][:, None, :], 0.0).reshape(TOK, TOK).T
            hi = jnp.minimum(hot, BF16_MAX).astype(BF16)
            r1 = hot - hi.astype(F32)
            mid = r1.astype(BF16)
            lo = (r1 - mid.astype(F32)).astype(BF16)
            at = slice((b % 2) * TOK, (b % 2 + 1) * TOK)
            comb[k][i, b // 2, 0, :, at] = hi
            comb[k][i, b // 2, 1, :, at] = mid
            comb[k][i, b // 2, 2, :, at] = lo

    for q in W2:
        x4[q][1].forward()
    loop(4, lambda i: [weights(k, i) for k in range(3)])

    def from_src(ref, q, d, half=None):
        cs = slice(None) if half is None else half
        return ref.at[cs, :, d] if a1[q] else ref.at[cs, :, :, d]

    x5 = [([], []) for _ in range(NQ)]

    def arrive4(q):
        for cr in range(2):
            x4[q][cr].arrive()
        if q < 3:
            for i in range(2):
                pl.semaphore_wait(credit.at[q, i], 1)

    def far5(q):
        for i, d in enumerate(DIRS):
            x5[q][0].append(send(from_src(gat[q], q, mod(p1[q] + 2), i), pas5[q].at[i], peer(d1[q], d, core)))

    def near5(q):
        for i, d in enumerate(DIRS):
            x5[q][1].append(send(from_src(gat[q], q, mod(p1[q] + d)), rec[q].at[:, p1[q]], peer(d1[q], d, core)))

    def keep5(q):
        if a1[q]:
            rec[q][:, p1[q]] = gat[q][:, :, p1[q]]
        else:
            rec[q][:, p1[q]] = gat[q][:, :, :, p1[q]]

    def forward5(q):
        for i, d in enumerate(DIRS):
            x5[q][0][i].wait_recv()
            x5[q][1].append(send(pas5[q].at[i], rec[q].at[i, mod(p1[q] - d)], peer(d1[q], d, core)))

    for q in W1:
        arrive4(q)
        far5(q)
        near5(q)
    for q in W1:
        keep5(q)
    for q in W2:
        arrive4(q)
        far5(q)
    for q in W1:
        forward5(q)
    for q in W2:
        near5(q)
    for q in W2:
        keep5(q)
    for q in W2:
        forward5(q)

    x6 = [([], []) for _ in range(NQ)]
    half_tok = TOK // 2

    def combine(q):
        for cp in x5[q][1]:
            cp.wait_recv()
        k, w = q % 3, widths[q]

        def step(i):
            acc = jnp.zeros((TOK, w), F32)
            for c in range(2):
                o = rec[q][c, :, :, i].reshape(2 * TOK, w)
                for t in range(3):
                    acc = acc + jnp.dot(comb[k][i, c, t], o, preferred_element_type=F32)
            part[q][i] = acc

        return step

    def far6(q):
        for i, d in enumerate(DIRS):
            x6[q][0].append(send(part[q].at[mod(p2[q] + 2), pl.ds(i * half_tok, half_tok)], pas6[q].at[i], peer(d2[q], d, core)))

    def rows6(q, i, half):
        return part[q].at[mod(p2[q] + DIRS[i]), pl.ds(half * half_tok, half_tok)], prec[q].at[i, pl.ds(half * half_tok, half_tok)]

    def near6(q):
        for i, d in enumerate(DIRS):
            x6[q][1].append(send(*rows6(q, i, 1 - i), peer(d2[q], d, core)))

    def forward6(q):
        for i, d in enumerate(DIRS):
            x6[q][0][i].wait_recv()
            mine, there = rows6(q, i, i)
            mine[...] = mine[...] + pas6[q][i]
            x6[q][1].append(send(mine, there, peer(d2[q], d, core)))

    def final(q):
        for cp in x6[q][1]:
            cp.wait_recv()
        total = part[q][p2[q]] + prec[q][0] + prec[q][1]
        xk = x_ref[:, :, :, offs[q]:offs[q] + widths[q]].reshape(TOK, widths[q]).astype(F32)
        y_ref[:, offs[q]:offs[q] + widths[q]] = (xk + total).astype(BF16)
        cols = pl.ds(offs[q], widths[q])
        out = pltpu.make_async_copy(y_ref.at[:, cols], y_hbm.at[:, cols], out_sem.at[q])
        out.start()
        return out

    def far_sum(q):
        step = combine(q)
        step(mod(p2[q] + 2))
        far6(q)
        return step

    steps = {}
    for q in W1:
        steps[q] = far_sum(q)
    loop(3, lambda i: [steps[q](mod(p2[q] + 3 + i)) for q in W1])
    for q in W1:
        near6(q)
    for q in W2:
        steps[q] = far_sum(q)
    for q in W1:
        forward6(q)
    loop(3, lambda i: [steps[q](mod(p2[q] + 3 + i)) for q in W2])
    for q in W2:
        near6(q)
    for q in W2:
        forward6(q)
    outs = [final(q) for q in W1 + W2]
    for c in outs:
        c.wait()
    for q in range(NQ):
        for cr in range(2):
            x4[q][cr].sent()
        for cp in x5[q][0] + x5[q][1] + x6[q][0] + x6[q][1]:
            cp.wait_send()


N_COPIES = 3 * 6 + NQ * (16 + 13 + 13 + 6 + 6)


def solution(mesh):
    def local_layer(x_loc, ids_loc, gates_loc, w_g, w_u, w_d):
        tok, hid = x_loc.shape
        fdim = w_g.shape[2]
        widths = split_width(hid)
        f_tile = 256 if fdim % 256 == 0 else fdim
        x4 = x_loc.reshape(CORES, RING, CAP, hid)
        scratch = []
        each = lambda f: scratch.extend(f(w) for w in widths)
        for _ in range(3):
            each(lambda w: pltpu.VMEM(LEAD + (CAP, w), BF16))
        scratch += [pltpu.VMEM((RING, RING, 16, TOK), F32)] * 3
        scratch += [pltpu.VMEM((RING, RING, TOK, TOK), BF16)] * 3
        scratch += [pltpu.VMEM((RING, 2, 3, TOK, 2 * TOK), BF16)] * 3
        each(lambda w: pltpu.VMEM((2, CORES, 2, RING, CAP, w), BF16))
        each(lambda w: pltpu.VMEM((2, CORES, 2, RING, CAP, w), BF16))
        each(lambda w: pltpu.VMEM((2, RING, RING, CAP, w), BF16))
        each(lambda w: pltpu.VMEM((RING, TOK, w), F32))
        each(lambda w: pltpu.VMEM((2, TOK, w), F32))
        each(lambda w: pltpu.VMEM((2, TOK // 2, w), F32))
        scratch += [
            pltpu.VMEM((hid, fdim), BF16),
            pltpu.VMEM((hid, fdim), BF16),
            pltpu.VMEM((fdim, hid), BF16),
            pltpu.VMEM((2, 2 * RING * RING * CAP, fdim), BF16),
            pltpu.VMEM((16, TOK), F32),
            pltpu.VMEM(x4.shape, BF16),
            pltpu.VMEM((8, TOK), jnp.int32),
            pltpu.VMEM((8, TOK), F32),
            pltpu.VMEM((tok, hid), BF16),
            pltpu.SemaphoreType.DMA((N_COPIES,)),
            pltpu.SemaphoreType.DMA((N_COPIES,)),
            pltpu.SemaphoreType.DMA((3,)),
            pltpu.SemaphoreType.DMA((3,)),
            pltpu.SemaphoreType.DMA((NQ,)),
            pltpu.SemaphoreType.REGULAR((3, 2)),
        ]
        hbm = pl.BlockSpec(memory_space=pl.ANY)
        return pl.pallas_call(
            functools.partial(moe_kernel, widths, fdim, f_tile),
            out_shape=jax.ShapeDtypeStruct((tok, hid), BF16),
            in_specs=[hbm] * 6,
            out_specs=hbm,
            scratch_shapes=scratch,
            compiler_params=pltpu.CompilerParams(collective_id=0, has_side_effects=True, vmem_limit_bytes=62914560),
            name='moe',
        )(x4, ids_loc.T, gates_loc.T, w_g[0], w_u[0], w_d[0])

    tok_spec = P(TOKEN_AXES, None)
    w_spec = P(EXPERT_AXES, None, None)
    return jax.shard_map(local_layer, mesh=mesh, in_specs=(tok_spec, tok_spec, tok_spec, w_spec, w_spec, w_spec), out_specs=tok_spec, check_vma=False)
```

```python
import functools

import jax
import jax.numpy as jnp
from jax import lax
from jax.experimental import pallas as pl
from jax.experimental.pallas import tpu as pltpu
from jax.sharding import PartitionSpec as P

TOKEN_AXES = ('ez', 'ey', 'ex')
EXPERT_AXES = ('ex', 'ey', 'ez')
MESH = pl.DeviceIdType.MESH
F32 = jnp.float32
BF16 = jnp.bfloat16
BF16_MAX = float(jnp.finfo(jnp.bfloat16).max)

Z, Y, X = 0, 1, 2
D1 = (Y, Z, X)
D2 = (Z, X, Y)
D3 = (X, Y, Z)
A_IS_D1 = (True, False, True)
RING = 4
CORES = 2
CAP = 16
TOK = 128
LEAD = (CORES, RING, RING, RING)


NQ = 6
W1, W2 = (0, 1, 2), (3, 4, 5)


def split_width(hid):
    tiles = hid // 128
    second = tiles * 7 // 16
    first = tiles - second
    thirds = lambda n: [n - 2 * (n // 3), n // 3, n // 3]
    return tuple(n * 128 for n in thirds(first) + thirds(second))


def moe_kernel(widths, fdim, f_tile, x_hbm, ids_hbm, gates_hbm, w1_hbm, w3_hbm, w2_hbm, y_hbm, *scr):
    it = iter(scr)
    take = lambda n: [next(it) for _ in range(n)]
    gat, til, rec = take(NQ), take(NQ), take(NQ)
    meta, sel, comb = take(3), take(3), take(3)
    pas3, pas4, pas5 = take(NQ), take(NQ), take(NQ)
    part, prec, pas6 = take(NQ), take(NQ), take(NQ)
    w1, w3, w2, act, meta_ref = take(5)
    x_ref, ids_ref, gates_ref, y_ref = take(4)
    send_sem, recv_sem, w_sem, in_sem, out_sem, credit = take(6)
    loads = [pltpu.make_async_copy(s, d, in_sem.at[i]) for i, (s, d) in enumerate(((ids_hbm, ids_ref), (gates_hbm, gates_ref), (x_hbm, x_ref)))]
    for c in loads:
        c.start()

    offs = [sum(widths[:q]) for q in range(NQ)]
    ez, ey, ex = lax.axis_index('ez'), lax.axis_index('ey'), lax.axis_index('ex')
    core = lax.rem(ex, CORES)
    pos = (ez, ey, ex // CORES)
    mod = lambda v: lax.rem(v + RING, RING)
    other = 1 - core

    strides = (1, RING, 2 * RING * RING)

    def turned(v, r):
        return [v[d] * (1 - r) + v[(d + 1) % 3] * r for d in range(3)]

    def peer(dim, off, c, lane=None):
        r = core if lane is None else lane
        q = [mod(pos[j] + off * ((1 - r) * int(j == dim) + r * int(j == (dim + 1) % 3))) for j in range(3)]
        return (q[0], q[1], q[2] * CORES + c)

    counter = [0]

    def send(src, dst, dev):
        i = counter[0]
        counter[0] += 1
        cp = pltpu.make_async_remote_copy(src, dst, send_sem.at[i], recv_sem.at[i], device_id=dev, device_id_type=MESH)
        cp.start()
        return cp

    bar = pltpu.get_barrier_semaphore()
    npeer = 0
    for dim in range(3):
        for off in (1, -1):
            for c in (core, other):
                pl.semaphore_signal(bar, inc=1, device_id=peer(dim, off, c, 0), device_id_type=MESH)
                npeer += 1
    pl.semaphore_signal(bar, inc=1, device_id=peer(0, 0, other), device_id_type=MESH)
    w_copies = [pltpu.make_async_copy(s, d, w_sem.at[i]) for i, (s, d) in enumerate(((w1_hbm, w1), (w3_hbm, w3), (w2_hbm, w2)))]
    for c in loads[:2]:
        c.wait()
    meta_ref[0:8] = ids_ref[...].astype(F32)
    meta_ref[8:16] = gates_ref[...]
    loads[2].wait()
    pl.semaphore_wait(bar, npeer + 1)

    DIRS = (1, -1)
    d1 = [D1[q % 3] for q in range(NQ)]
    d2 = [D2[q % 3] for q in range(NQ)]
    d3 = [D3[q % 3] for q in range(NQ)]
    a1 = [A_IS_D1[q % 3] for q in range(NQ)]
    lpos, lstr = turned(pos, core), turned(strides, core)
    opos = turned(pos, other)
    p1 = [lpos[d] for d in d1]
    p2 = [lpos[d] for d in d2]
    p3 = [lpos[d] for d in d3]
    p3_other = [opos[d] for d in d3]
    xcol = [x_ref.at[:, :, :, pl.ds(offs[q], widths[q])] for q in range(NQ)]
    unwaited = []

    def chunk(q, r):
        return gat[q].at[:, :, p2[q], mod(p1[q] + r)]

    m1 = [[None, None] for _ in range(3)]
    mf1 = [None] * 3
    m2 = [[None, None] for _ in range(3)]
    mf2 = [None] * 3
    g1 = [[None, None] for _ in range(NQ)]
    f1 = [[None, None] for _ in range(NQ)]
    g2 = [[[None] * 4, [None] * 4] for _ in range(NQ)]
    f2 = [[None] * 4 for _ in range(NQ)]

    def first_sends(wave):
        for q in wave:
            for i, d in enumerate(DIRS):
                if q < 3:
                    m1[q][i] = send(meta_ref, meta[q].at[p2[q], p1[q]], peer(d1[q], d, core))
                g1[q][i] = send(xcol[q], chunk(q, 0), peer(d1[q], d, core))
        for q in wave:
            for i, d in enumerate(DIRS):
                g2[q][i][0] = send(xcol[q], chunk(q, 0), peer(d2[q], d, core))

    def first_forwards(wave):
        for q in wave:
            for i, d in enumerate(DIRS):
                if q < 3:
                    m1[q][i].wait_recv()
                    if i == 0:
                        src = meta[q].at[p2[q], mod(p1[q] - 1)]
                        mf1[q] = send(src, src, peer(d1[q], 1, core))
                g1[q][i].wait_recv()
                half = chunk(q, -d).at[i]
                f1[q][i] = send(half, half, peer(d1[q], d, core))
        for q in wave:
            for i, d in enumerate(DIRS):
                for r in (1, 3):
                    g2[q][i][r] = send(chunk(q, r), chunk(q, r), peer(d2[q], d, core))

    def forward2(q, i, r):
        g2[q][i][r].wait_recv()
        src = gat[q].at[:, :, mod(p2[q] - DIRS[i]), mod(p1[q] + r)]
        f2[q][r] = send(src, src, peer(d2[q], DIRS[i], core))

    first_sends(W1)
    first_sends(W2)
    for c in w_copies:
        c.start()
    for q in range(NQ):
        gat[q][:, :, p2[q], p1[q]] = x_ref[:, :, :, offs[q]:offs[q] + widths[q]]
    for k in range(3):
        meta[k][p2[k], p1[k]] = meta_ref[...]
    first_forwards(W1)
    for k in range(3):
        mf1[k].wait_recv()
        for i, d in enumerate(DIRS):
            row = meta[k].at[p2[k]]
            m2[k][i] = send(row, row, peer(d2[k], d, core))

    def last_chunk(wave):
        for q in wave:
            for i, d in enumerate(DIRS):
                f1[q][i].wait_recv()
            for i, d in enumerate(DIRS):
                g2[q][i][2] = send(chunk(q, 2), chunk(q, 2), peer(d2[q], d, core))

    for q in W1:
        forward2(q, 0, 0)
    last_chunk(W1)
    first_forwards(W2)
    for k in range(3):
        for i in range(2):
            m2[k][i].wait_recv()
        src = meta[k].at[mod(p2[k] - 1)]
        mf2[k] = send(src, src, peer(d2[k], 1, core))

    tri = (lax.broadcasted_iota(jnp.int32, (TOK, TOK), 0) < lax.broadcasted_iota(jnp.int32, (TOK, TOK), 1)).astype(BF16)
    i8 = lax.broadcasted_iota(jnp.int32, (8, 1), 0)
    slot = lax.broadcasted_iota(jnp.int32, (8, CAP, TOK), 1).astype(F32)

    def experts8(k):
        base = lpos[D1[k]] * lstr[D1[k]] + lpos[D2[k]] * lstr[D2[k]]
        return (base + (i8 & 3) * lstr[D3[k]] + (i8 >> 2) * (RING * RING)).astype(F32)

    def picked(ids, evec):
        m = (ids[0:1, :] == evec).astype(F32)
        for j in range(1, 8):
            m = m + (ids[j:j + 1, :] == evec).astype(F32)
        return m

    def rank_of(m):
        rank = jnp.dot(m.astype(BF16), tri, preferred_element_type=F32)
        return jnp.where(m > 0.5, rank, -1.0)

    def onehot(k, i):
        evec = experts8(k)
        rm = rank_of(jnp.concatenate([picked(meta[k][i, j, 0:8], evec) for j in range(4)], axis=0))
        for j in range(4):
            hot = (rm[j * 8:(j + 1) * 8][:, None, :] == slot).astype(F32)
            sel[k][i, j] = hot.reshape(TOK, TOK).astype(BF16)

    def select(q, i):
        k, w = q % 3, widths[q]
        for j in range(4):
            rows = gat[q][:, :, i, j].reshape(TOK, w)
            out = jnp.dot(sel[k][i, j], rows, preferred_element_type=F32).astype(BF16).reshape(CORES, RING, CAP, w)
            if a1[q]:
                til[q][:, :, j, i] = out
            else:
                til[q][:, :, i, j] = out

    def loop(n, f):
        def body(i, carry):
            f(i)
            return carry
        lax.fori_loop(0, n, body, 0)

    for k in range(3):
        onehot(k, p2[k])
    for q in W1:
        forward2(q, 0, 1)
        forward2(q, 1, 3)
    for q in W1:
        select(q, p2[q])
    for q in W1:
        forward2(q, 1, 2)
    for q in W2:
        forward2(q, 0, 0)
    last_chunk(W2)
    for k in range(3):
        mf2[k].wait_recv()
    loop(3, lambda i: [onehot(k, mod(p2[k] + 1 + i)) for k in range(3)])

    def gathered(q, near):
        if near:
            for i, r in ((0, 2), (0, 3), (1, 0), (1, 1)):
                g2[q][i][r].wait_recv()
            loop(2, lambda i, q=q: select(q, mod(p2[q] - 1 + 2 * i)))
        else:
            for r in range(4):
                f2[q][r].wait_recv()
            select(q, mod(p2[q] + 2))
            done = g1[q] + f1[q] + g2[q][0] + g2[q][1] + f2[q]
            if q < 3:
                done = done + m1[q] + [mf1[q]] + m2[q] + [mf2[q]]
            for c in done:
                c.wait_send()

    def sub(ref, q, c, d, half=None):
        a = slice(None) if half is None else pl.ds(2 * half, 2)
        return (ref.at[c, d, a], ref.at[c, a, d], ref.at[c, a, :, d])[q % 3]

    def til_block(ref, q, c, d, half=None):
        return ref.at[c, d] if half is None else ref.at[c, d, pl.ds(2 * half, 2)]

    class Leg:
        def __init__(self, q, cr, lane, src, src_block, dst, dst_block, pas):
            self.q, self.cr, self.lane, self.src, self.dst = q, cr, lane, src, dst
            self.src_block, self.dst_block, self.pas = src_block, dst_block, pas
            self.c = core if cr == 0 else other
            self.p = p3[q] if lane is core else p3_other[q]
            self.first, self.direct = [], []

        def out(self, d, half=None):
            return self.src_block(self.src, self.q, self.c, d, half)

        def into(self, d, half=None):
            return self.dst_block(self.dst, self.q, core, d, half)

        def far(self):
            for i, d in enumerate(DIRS):
                self.first.append(send(self.out(mod(self.p + 2), i), self.pas.at[i, self.cr], peer(d3[self.q], d, core, self.lane)))

        def near(self):
            for i, d in enumerate(DIRS):
                self.direct.append(send(self.out(mod(self.p + d)), self.into(self.p), peer(d3[self.q], d, self.c, self.lane)))
            if self.cr == 1:
                self.direct.append(send(self.out(self.p), self.into(self.p), peer(d3[self.q], 0, other, self.lane)))

        def forward(self):
            for i, d in enumerate(DIRS):
                self.first[i].wait_recv()
                self.direct.append(send(self.pas.at[i, self.cr], self.into(mod(self.p - d), i), peer(d3[self.q], d, self.c, self.lane)))

        def arrive(self):
            for cp in self.direct:
                cp.wait_recv()

        def sent(self):
            for cp in self.first + self.direct:
                cp.wait_send()

    def keep3(q):
        v = til[q][core, p3[q]]
        if q % 3 == 0:
            rec[q][core, p3[q]] = v
        elif q % 3 == 1:
            rec[q][core, :, p3[q]] = v
        else:
            rec[q][core, :, :, p3[q]] = v

    def keep4(q):
        if q % 3 == 0:
            v = til[q][core, p3[q]]
        elif q % 3 == 1:
            v = til[q][core, :, p3[q]]
        else:
            v = til[q][core, :, :, p3[q]]
        gat[q][core, p3[q]] = v

    x3 = [[Leg(q, cr, core, til[q], til_block, rec[q], sub, pas3[q]) for cr in range(2)] for q in range(NQ)]
    for q in W1:
        gathered(q, True)
    for q in W2:
        forward2(q, 0, 1)
        forward2(q, 1, 3)
    for q in W2:
        select(q, p2[q])
    for q in W1:
        gathered(q, False)
        x3[q][0].far()
    for q in W2:
        forward2(q, 1, 2)
    for q in W1:
        x3[q][0].near()
    for q in W2:
        gathered(q, True)
    for q in W1:
        x3[q][0].forward()
    for q in W2:
        gathered(q, False)
        x3[q][0].far()
    for q in W2:
        x3[q][0].near()
    for q in W1:
        x3[q][1].far()
    for q in W2:
        x3[q][0].forward()
    for q in W2:
        x3[q][1].far()
    for q in W1 + W2:
        x3[q][1].near()
    for q in W1 + W2:
        keep3(q)
    def weights(k, i):
        mrow = meta[k][i, p1[k]]
        ids, gates = mrow[0:8], mrow[8:16]
        own = lpos[D2[k]] * lstr[D2[k]]
        ms, gs = [], []
        for b in range(4):
            idx = i8 + b * 8
            d3e, d1e, ce = idx & 3, (idx >> 2) & 3, idx >> 4
            evec = (own + d3e * lstr[D3[k]] + d1e * lstr[D1[k]] + ce * (RING * RING)).astype(F32)
            m = jnp.zeros((8, TOK), F32)
            g = jnp.zeros((8, TOK), F32)
            for j in range(8):
                hit = ids[j:j + 1, :] == evec
                m = m + hit.astype(F32)
                g = g + jnp.where(hit, gates[j:j + 1, :], 0.0)
            ms.append(m)
            gs.append(g)
        rm = rank_of(jnp.concatenate(ms, axis=0))
        for b in range(4):
            hot = jnp.where(rm[b * 8:(b + 1) * 8][:, None, :] == slot, gs[b][:, None, :], 0.0).reshape(TOK, TOK).T
            hi = jnp.minimum(hot, BF16_MAX).astype(BF16)
            r1 = hot - hi.astype(F32)
            mid = r1.astype(BF16)
            lo = (r1 - mid.astype(F32)).astype(BF16)
            at = slice((b % 2) * TOK, (b % 2 + 1) * TOK)
            comb[k][i, b // 2, 0, :, at] = hi
            comb[k][i, b // 2, 1, :, at] = mid
            comb[k][i, b // 2, 2, :, at] = lo

    loop(4, lambda i: [weights(k, i) for k in range(3)])
    for c in w_copies:
        c.wait()

    x4 = [[Leg(q, cr, core if cr == 0 else other, til[q], sub, gat[q], til_block, pas4[q]) for cr in range(2)] for q in range(NQ)]
    rows = 2 * RING * RING * CAP
    for cr in range(2):
        c = core if cr == 0 else other
        for q in range(NQ):
            x3[q][cr].arrive()
        for q in range(NQ):
            x3[q][cr].sent()

        def hidden(i, c=c):
            xs = jnp.concatenate([rec[q][c, pl.ds(2 * i, 2)].reshape(rows, widths[q]) for q in range(NQ)], axis=1)
            for f in range(fdim // f_tile):
                cols = slice(f * f_tile, (f + 1) * f_tile)
                hg = jnp.dot(xs, w1[:, cols], preferred_element_type=F32)
                hu = jnp.dot(xs, w3[:, cols], preferred_element_type=F32)
                act[i, :, cols] = (hg * jax.nn.sigmoid(hg) * hu).astype(BF16)

        def down(wave, c=c):
            def step(i):
                lo, hi = offs[wave[0]], offs[wave[-1]] + widths[wave[-1]]
                o = jnp.dot(act[i], w2[:, lo:hi], preferred_element_type=F32).astype(BF16)
                for q in wave:
                    part_q = o[:, offs[q] - lo:offs[q] - lo + widths[q]]
                    til[q][c, pl.ds(2 * i, 2)] = part_q.reshape(2, RING, RING, CAP, widths[q])
            loop(2, step)

        hidden(0)
        if cr == 0:
            for q in W1 + W2:
                x3[q][1].forward()
        hidden(1)
        if cr == 1:
            for q in W1 + W2:
                x4[q][0].forward()
        down(W1)
        for q in W1:
            x4[q][cr].far()
        for q in W1:
            x4[q][cr].near()
        down(W2)
        for q in W2:
            x4[q][cr].far()
        if cr == 1:
            for q in W1:
                x4[q][1].forward()
        for q in W2:
            x4[q][cr].near()
        if cr == 0:
            for q in W1 + W2:
                keep4(q)
    for k in range(3):
        for i, d in enumerate(DIRS):
            pl.semaphore_signal(credit.at[k, i], inc=1, device_id=peer(D1[k], d, core), device_id_type=MESH)

    for q in W2:
        x4[q][1].forward()

    def from_src(ref, q, d, half=None):
        cs = slice(None) if half is None else half
        return ref.at[cs, :, d] if a1[q] else ref.at[cs, :, :, d]

    x5 = [([], []) for _ in range(NQ)]

    def arrive4(q):
        for cr in range(2):
            x4[q][cr].arrive()
        if q < 3:
            for i in range(2):
                pl.semaphore_wait(credit.at[q, i], 1)

    def far5(q):
        for i, d in enumerate(DIRS):
            x5[q][0].append(send(from_src(gat[q], q, mod(p1[q] + 2), i), pas5[q].at[i], peer(d1[q], d, core)))

    def near5(q):
        for i, d in enumerate(DIRS):
            x5[q][1].append(send(from_src(gat[q], q, mod(p1[q] + d)), rec[q].at[:, p1[q]], peer(d1[q], d, core)))

    def keep5(q):
        if a1[q]:
            rec[q][:, p1[q]] = gat[q][:, :, p1[q]]
        else:
            rec[q][:, p1[q]] = gat[q][:, :, :, p1[q]]

    def forward5(q):
        for i, d in enumerate(DIRS):
            x5[q][0][i].wait_recv()
            x5[q][1].append(send(pas5[q].at[i], rec[q].at[i, mod(p1[q] - d)], peer(d1[q], d, core)))

    for q in W1:
        arrive4(q)
        far5(q)
        near5(q)
    for q in W1:
        keep5(q)
    for q in W2:
        arrive4(q)
        far5(q)
    for q in W1:
        forward5(q)
    for q in W2:
        near5(q)
    for q in W2:
        keep5(q)
    for q in W2:
        forward5(q)

    x6 = [([], []) for _ in range(NQ)]
    half_tok = TOK // 2

    def combine(q):
        for cp in x5[q][1]:
            cp.wait_recv()
        k, w = q % 3, widths[q]

        def step(i):
            acc = jnp.zeros((TOK, w), F32)
            for c in range(2):
                o = rec[q][c, :, :, i].reshape(2 * TOK, w)
                for t in range(3):
                    acc = acc + jnp.dot(comb[k][i, c, t], o, preferred_element_type=F32)
            part[q][i] = acc

        return step

    def far6(q):
        for i, d in enumerate(DIRS):
            x6[q][0].append(send(part[q].at[mod(p2[q] + 2), pl.ds(i * half_tok, half_tok)], pas6[q].at[i], peer(d2[q], d, core)))

    def rows6(q, i, half):
        return part[q].at[mod(p2[q] + DIRS[i]), pl.ds(half * half_tok, half_tok)], prec[q].at[i, pl.ds(half * half_tok, half_tok)]

    def near6(q):
        for i, d in enumerate(DIRS):
            x6[q][1].append(send(*rows6(q, i, 1 - i), peer(d2[q], d, core)))

    def forward6(q):
        for i, d in enumerate(DIRS):
            x6[q][0][i].wait_recv()
            mine, there = rows6(q, i, i)
            mine[...] = mine[...] + pas6[q][i]
            x6[q][1].append(send(mine, there, peer(d2[q], d, core)))

    def final(q):
        for cp in x6[q][1]:
            cp.wait_recv()
        total = part[q][p2[q]] + prec[q][0] + prec[q][1]
        xk = x_ref[:, :, :, offs[q]:offs[q] + widths[q]].reshape(TOK, widths[q]).astype(F32)
        y_ref[:, offs[q]:offs[q] + widths[q]] = (xk + total).astype(BF16)
        cols = pl.ds(offs[q], widths[q])
        out = pltpu.make_async_copy(y_ref.at[:, cols], y_hbm.at[:, cols], out_sem.at[q])
        out.start()
        return out

    def far_sum(q):
        step = combine(q)
        step(mod(p2[q] + 2))
        far6(q)
        return step

    steps = {}
    for q in W1:
        steps[q] = far_sum(q)
    loop(3, lambda i: [steps[q](mod(p2[q] + 3 + i)) for q in W1])
    for q in W1:
        near6(q)
    for q in W2:
        steps[q] = far_sum(q)
    for q in W1:
        forward6(q)
    loop(3, lambda i: [steps[q](mod(p2[q] + 3 + i)) for q in W2])
    for q in W2:
        near6(q)
    for q in W2:
        forward6(q)
    outs = [final(q) for q in W1 + W2]
    for c in outs:
        c.wait()
    for q in range(NQ):
        for cr in range(2):
            x4[q][cr].sent()
        for cp in x5[q][0] + x5[q][1] + x6[q][0] + x6[q][1]:
            cp.wait_send()


N_COPIES = 3 * 6 + NQ * (16 + 13 + 13 + 6 + 6)


def solution(mesh):
    def local_layer(x_loc, ids_loc, gates_loc, w_g, w_u, w_d):
        tok, hid = x_loc.shape
        fdim = w_g.shape[2]
        widths = split_width(hid)
        f_tile = 256 if fdim % 256 == 0 else fdim
        x4 = x_loc.reshape(CORES, RING, CAP, hid)
        scratch = []
        each = lambda f: scratch.extend(f(w) for w in widths)
        for _ in range(3):
            each(lambda w: pltpu.VMEM(LEAD + (CAP, w), BF16))
        scratch += [pltpu.VMEM((RING, RING, 16, TOK), F32)] * 3
        scratch += [pltpu.VMEM((RING, RING, TOK, TOK), BF16)] * 3
        scratch += [pltpu.VMEM((RING, 2, 3, TOK, 2 * TOK), BF16)] * 3
        each(lambda w: pltpu.VMEM((2, CORES, 2, RING, CAP, w), BF16))
        each(lambda w: pltpu.VMEM((2, CORES, 2, RING, CAP, w), BF16))
        each(lambda w: pltpu.VMEM((2, RING, RING, CAP, w), BF16))
        each(lambda w: pltpu.VMEM((RING, TOK, w), F32))
        each(lambda w: pltpu.VMEM((2, TOK, w), F32))
        each(lambda w: pltpu.VMEM((2, TOK // 2, w), F32))
        scratch += [
            pltpu.VMEM((hid, fdim), BF16),
            pltpu.VMEM((hid, fdim), BF16),
            pltpu.VMEM((fdim, hid), BF16),
            pltpu.VMEM((2, 2 * RING * RING * CAP, fdim), BF16),
            pltpu.VMEM((16, TOK), F32),
            pltpu.VMEM(x4.shape, BF16),
            pltpu.VMEM((8, TOK), jnp.int32),
            pltpu.VMEM((8, TOK), F32),
            pltpu.VMEM((tok, hid), BF16),
            pltpu.SemaphoreType.DMA((N_COPIES,)),
            pltpu.SemaphoreType.DMA((N_COPIES,)),
            pltpu.SemaphoreType.DMA((3,)),
            pltpu.SemaphoreType.DMA((3,)),
            pltpu.SemaphoreType.DMA((NQ,)),
            pltpu.SemaphoreType.REGULAR((3, 2)),
        ]
        hbm = pl.BlockSpec(memory_space=pl.ANY)
        return pl.pallas_call(
            functools.partial(moe_kernel, widths, fdim, f_tile),
            out_shape=jax.ShapeDtypeStruct((tok, hid), BF16),
            in_specs=[hbm] * 6,
            out_specs=hbm,
            scratch_shapes=scratch,
            compiler_params=pltpu.CompilerParams(collective_id=0, has_side_effects=True, vmem_limit_bytes=62914560),
            name='moe',
        )(x4, ids_loc.T, gates_loc.T, w_g[0], w_u[0], w_d[0])

    tok_spec = P(TOKEN_AXES, None)
    w_spec = P(EXPERT_AXES, None, None)
    return jax.shard_map(local_layer, mesh=mesh, in_specs=(tok_spec, tok_spec, tok_spec, w_spec, w_spec, w_spec), out_specs=tok_spec, check_vma=False)
```

```python
import functools

import jax
import jax.numpy as jnp
from jax import lax
from jax.experimental import pallas as pl
from jax.experimental.pallas import tpu as pltpu
from jax.sharding import PartitionSpec as P

TOKEN_AXES = ('ez', 'ey', 'ex')
EXPERT_AXES = ('ex', 'ey', 'ez')
MESH = pl.DeviceIdType.MESH
F32 = jnp.float32
BF16 = jnp.bfloat16
BF16_MAX = float(jnp.finfo(jnp.bfloat16).max)

Z, Y, X = 0, 1, 2
D1 = (Y, Z, X)
D2 = (Z, X, Y)
D3 = (X, Y, Z)
A_IS_D1 = (True, False, True)
RING = 4
CORES = 2
CAP = 16
TOK = 128
LEAD = (CORES, RING, RING, RING)


NQ = 6
W1, W2 = (0, 1, 2), (3, 4, 5)


def split_width(hid):
    tiles = hid // 128
    second = tiles * 7 // 16
    first = tiles - second
    thirds = lambda n: [n - 2 * (n // 3), n // 3, n // 3]
    return tuple(n * 128 for n in thirds(first) + thirds(second))


def moe_kernel(widths, fdim, f_tile, x_hbm, ids_hbm, gates_hbm, w1_hbm, w3_hbm, w2_hbm, y_hbm, *scr):
    it = iter(scr)
    take = lambda n: [next(it) for _ in range(n)]
    gat, til, rec = take(NQ), take(NQ), take(NQ)
    meta, sel, comb = take(3), take(3), take(3)
    pas3, pas4, pas5 = take(NQ), take(NQ), take(NQ)
    part, prec, pas6 = take(NQ), take(NQ), take(NQ)
    w1, w3, w2, act, meta_ref = take(5)
    gates = take(3)
    x_ref, ids_ref, gates_ref, y_ref = take(4)
    send_sem, recv_sem, w_sem, in_sem, out_sem, credit = take(6)
    loads = [pltpu.make_async_copy(s, d, in_sem.at[i]) for i, (s, d) in enumerate(((ids_hbm, ids_ref), (gates_hbm, gates_ref), (x_hbm, x_ref)))]
    for c in loads:
        c.start()

    offs = [sum(widths[:q]) for q in range(NQ)]
    ez, ey, ex = lax.axis_index('ez'), lax.axis_index('ey'), lax.axis_index('ex')
    core = lax.rem(ex, CORES)
    pos = (ez, ey, ex // CORES)
    mod = lambda v: lax.rem(v + RING, RING)
    other = 1 - core

    strides = (1, RING, 2 * RING * RING)

    def turned(v, r):
        return [v[d] * (1 - r) + v[(d + 1) % 3] * r for d in range(3)]

    def peer(dim, off, c, lane=None):
        r = core if lane is None else lane
        q = [mod(pos[j] + off * ((1 - r) * int(j == dim) + r * int(j == (dim + 1) % 3))) for j in range(3)]
        return (q[0], q[1], q[2] * CORES + c)

    counter = [0]

    def send(src, dst, dev):
        i = counter[0]
        counter[0] += 1
        cp = pltpu.make_async_remote_copy(src, dst, send_sem.at[i], recv_sem.at[i], device_id=dev, device_id_type=MESH)
        cp.start()
        return cp

    bar = pltpu.get_barrier_semaphore()
    npeer = 0
    for dim in range(3):
        for off in (1, -1):
            for c in (core, other):
                pl.semaphore_signal(bar, inc=1, device_id=peer(dim, off, c, 0), device_id_type=MESH)
                npeer += 1
    pl.semaphore_signal(bar, inc=1, device_id=peer(0, 0, other), device_id_type=MESH)
    w_copies = [pltpu.make_async_copy(s, d, w_sem.at[i]) for i, (s, d) in enumerate(((w1_hbm, w1), (w3_hbm, w3), (w2_hbm, w2)))]
    for c in loads[:2]:
        c.wait()
    meta_ref[...] = ids_ref[...].astype(F32)
    loads[2].wait()
    pl.semaphore_wait(bar, npeer + 1)

    DIRS = (1, -1)
    d1 = [D1[q % 3] for q in range(NQ)]
    d2 = [D2[q % 3] for q in range(NQ)]
    d3 = [D3[q % 3] for q in range(NQ)]
    a1 = [A_IS_D1[q % 3] for q in range(NQ)]
    lpos, lstr = turned(pos, core), turned(strides, core)
    opos = turned(pos, other)
    p1 = [lpos[d] for d in d1]
    p2 = [lpos[d] for d in d2]
    p3 = [lpos[d] for d in d3]
    p3_other = [opos[d] for d in d3]
    xcol = [x_ref.at[:, :, :, pl.ds(offs[q], widths[q])] for q in range(NQ)]
    unwaited = []

    def chunk(q, r):
        return gat[q].at[:, :, p2[q], mod(p1[q] + r)]

    m1 = [[None, None] for _ in range(3)]
    mf1 = [None] * 3
    m2 = [[None, None] for _ in range(3)]
    mf2 = [None] * 3
    gm = [[None, None] for _ in range(3)]
    gmf = [None] * 3
    g1 = [[None, None] for _ in range(NQ)]
    f1 = [[None, None] for _ in range(NQ)]
    g2 = [[[None] * 4, [None] * 4] for _ in range(NQ)]
    f2 = [[None] * 4 for _ in range(NQ)]

    def first_sends(wave):
        for q in wave:
            for i, d in enumerate(DIRS):
                if q < 3:
                    m1[q][i] = send(meta_ref, meta[q].at[p2[q], p1[q]], peer(d1[q], d, core))
                g1[q][i] = send(xcol[q], chunk(q, 0), peer(d1[q], d, core))
        for q in wave:
            for i, d in enumerate(DIRS):
                g2[q][i][0] = send(xcol[q], chunk(q, 0), peer(d2[q], d, core))

    def first_forwards(wave):
        for q in wave:
            for i, d in enumerate(DIRS):
                if q < 3:
                    m1[q][i].wait_recv()
                    if i == 0:
                        src = meta[q].at[p2[q], mod(p1[q] - 1)]
                        mf1[q] = send(src, src, peer(d1[q], 1, core))
                g1[q][i].wait_recv()
                half = chunk(q, -d).at[i]
                f1[q][i] = send(half, half, peer(d1[q], d, core))
        for q in wave:
            for i, d in enumerate(DIRS):
                for r in (1, 3):
                    g2[q][i][r] = send(chunk(q, r), chunk(q, r), peer(d2[q], d, core))

    def forward2(q, i, r):
        g2[q][i][r].wait_recv()
        src = gat[q].at[:, :, mod(p2[q] - DIRS[i]), mod(p1[q] + r)]
        f2[q][r] = send(src, src, peer(d2[q], DIRS[i], core))

    first_sends(W1)
    first_sends(W2)
    for c in w_copies:
        c.start()
    for q in range(NQ):
        gat[q][:, :, p2[q], p1[q]] = x_ref[:, :, :, offs[q]:offs[q] + widths[q]]
    for k in range(3):
        meta[k][p2[k], p1[k]] = meta_ref[...]
        gates[k][p2[k]] = gates_ref[...]
    first_forwards(W1)
    for k in range(3):
        mf1[k].wait_recv()
        for i, d in enumerate(DIRS):
            row = meta[k].at[p2[k]]
            m2[k][i] = send(row, row, peer(d2[k], d, core))
            gm[k][i] = send(gates_ref, gates[k].at[p2[k]], peer(d2[k], d, core))

    def last_chunk(wave):
        for q in wave:
            for i, d in enumerate(DIRS):
                f1[q][i].wait_recv()
            for i, d in enumerate(DIRS):
                g2[q][i][2] = send(chunk(q, 2), chunk(q, 2), peer(d2[q], d, core))

    for q in W1:
        forward2(q, 0, 0)
    last_chunk(W1)
    first_forwards(W2)
    for k in range(3):
        for i in range(2):
            m2[k][i].wait_recv()
        src = meta[k].at[mod(p2[k] + 1)]
        mf2[k] = send(src, src, peer(d2[k], -1, core))
        for i in range(2):
            gm[k][i].wait_recv()
        src = gates[k].at[mod(p2[k] + 1)]
        gmf[k] = send(src, src, peer(d2[k], -1, core))

    tri = (lax.broadcasted_iota(jnp.int32, (TOK, TOK), 0) < lax.broadcasted_iota(jnp.int32, (TOK, TOK), 1)).astype(BF16)
    i8 = lax.broadcasted_iota(jnp.int32, (8, 1), 0)
    slot = lax.broadcasted_iota(jnp.int32, (8, CAP, TOK), 1).astype(F32)

    def experts8(k):
        base = lpos[D1[k]] * lstr[D1[k]] + lpos[D2[k]] * lstr[D2[k]]
        return (base + (i8 & 3) * lstr[D3[k]] + (i8 >> 2) * (RING * RING)).astype(F32)

    def picked(ids, evec):
        m = (ids[0:1, :] == evec).astype(F32)
        for j in range(1, 8):
            m = m + (ids[j:j + 1, :] == evec).astype(F32)
        return m

    def rank_of(m):
        rank = jnp.dot(m.astype(BF16), tri, preferred_element_type=F32)
        return jnp.where(m > 0.5, rank, -1.0)

    def onehot(k, i):
        evec = experts8(k)
        rm = rank_of(jnp.concatenate([picked(meta[k][i, j], evec) for j in range(4)], axis=0))
        for j in range(4):
            hot = (rm[j * 8:(j + 1) * 8][:, None, :] == slot).astype(F32)
            sel[k][i, j] = hot.reshape(TOK, TOK).astype(BF16)

    def select(q, i):
        k, w = q % 3, widths[q]
        for j in range(4):
            rows = gat[q][:, :, i, j].reshape(TOK, w)
            out = jnp.dot(sel[k][i, j], rows, preferred_element_type=F32).astype(BF16).reshape(CORES, RING, CAP, w)
            if a1[q]:
                til[q][:, :, j, i] = out
            else:
                til[q][:, :, i, j] = out

    def loop(n, f):
        def body(i, carry):
            f(i)
            return carry
        lax.fori_loop(0, n, body, 0)

    for k in range(3):
        onehot(k, p2[k])
    for q in W1:
        forward2(q, 0, 1)
        forward2(q, 1, 3)
    for q in W1:
        select(q, p2[q])
    for q in W1:
        forward2(q, 1, 2)
    for q in W2:
        forward2(q, 0, 0)
    last_chunk(W2)
    for k in range(3):
        mf2[k].wait_recv()
        gmf[k].wait_recv()
    loop(3, lambda i: [onehot(k, mod(p2[k] + 1 + i)) for k in range(3)])

    def gathered(q, near):
        if near:
            for i, r in ((0, 2), (0, 3), (1, 0), (1, 1)):
                g2[q][i][r].wait_recv()
            loop(2, lambda i, q=q: select(q, mod(p2[q] - 1 + 2 * i)))
        else:
            for r in range(4):
                f2[q][r].wait_recv()
            select(q, mod(p2[q] + 2))
            done = g1[q] + f1[q] + g2[q][0] + g2[q][1] + f2[q]
            if q < 3:
                done = done + m1[q] + [mf1[q]] + m2[q] + [mf2[q]] + gm[q] + [gmf[q]]
            for c in done:
                c.wait_send()

    def sub(ref, q, c, d, half=None):
        a = slice(None) if half is None else pl.ds(2 * half, 2)
        return (ref.at[c, d, a], ref.at[c, a, d], ref.at[c, a, :, d])[q % 3]

    def til_block(ref, q, c, d, half=None):
        return ref.at[c, d] if half is None else ref.at[c, d, pl.ds(2 * half, 2)]

    class Leg:
        def __init__(self, q, cr, lane, src, src_block, dst, dst_block, pas):
            self.q, self.cr, self.lane, self.src, self.dst = q, cr, lane, src, dst
            self.src_block, self.dst_block, self.pas = src_block, dst_block, pas
            self.c = core if cr == 0 else other
            self.p = p3[q] if lane is core else p3_other[q]
            self.first, self.direct = [], []

        def out(self, d, half=None):
            return self.src_block(self.src, self.q, self.c, d, half)

        def into(self, d, half=None):
            return self.dst_block(self.dst, self.q, core, d, half)

        def far(self):
            for i, d in enumerate(DIRS):
                self.first.append(send(self.out(mod(self.p + 2), i), self.pas.at[i, self.cr], peer(d3[self.q], d, core, self.lane)))

        def near(self):
            for i, d in enumerate(DIRS):
                self.direct.append(send(self.out(mod(self.p + d)), self.into(self.p), peer(d3[self.q], d, self.c, self.lane)))
            if self.cr == 1:
                self.direct.append(send(self.out(self.p), self.into(self.p), peer(d3[self.q], 0, other, self.lane)))

        def forward(self):
            for i, d in enumerate(DIRS):
                self.first[i].wait_recv()
                self.direct.append(send(self.pas.at[i, self.cr], self.into(mod(self.p - d), i), peer(d3[self.q], d, self.c, self.lane)))

        def arrive(self):
            for cp in self.direct:
                cp.wait_recv()

        def sent(self):
            for cp in self.first + self.direct:
                cp.wait_send()

    def keep3(q):
        v = til[q][core, p3[q]]
        if q % 3 == 0:
            rec[q][core, p3[q]] = v
        elif q % 3 == 1:
            rec[q][core, :, p3[q]] = v
        else:
            rec[q][core, :, :, p3[q]] = v

    def keep4(q):
        if q % 3 == 0:
            v = til[q][core, p3[q]]
        elif q % 3 == 1:
            v = til[q][core, :, p3[q]]
        else:
            v = til[q][core, :, :, p3[q]]
        gat[q][core, p3[q]] = v

    x3 = [[Leg(q, cr, core, til[q], til_block, rec[q], sub, pas3[q]) for cr in range(2)] for q in range(NQ)]
    for q in W1:
        gathered(q, True)
    for q in W2:
        forward2(q, 0, 1)
        forward2(q, 1, 3)
    for q in W2:
        select(q, p2[q])
    for q in W1:
        gathered(q, False)
        x3[q][0].far()
    for q in W2:
        forward2(q, 1, 2)
    for q in W1:
        x3[q][0].near()
    for q in W2:
        gathered(q, True)
    for q in W1:
        x3[q][0].forward()
    for q in W2:
        gathered(q, False)
        x3[q][0].far()
    for q in W2:
        x3[q][0].near()
    for q in W1:
        x3[q][1].far()
    for q in W2:
        x3[q][0].forward()
    for q in W2:
        x3[q][1].far()
    for q in W1 + W2:
        x3[q][1].near()
    for q in W1 + W2:
        keep3(q)
    def weights(k, i):
        ids, gval = meta[k][i, p1[k]], gates[k][i]
        own = lpos[D2[k]] * lstr[D2[k]]
        ms, gs = [], []
        for b in range(4):
            idx = i8 + b * 8
            d3e, d1e, ce = idx & 3, (idx >> 2) & 3, idx >> 4
            evec = (own + d3e * lstr[D3[k]] + d1e * lstr[D1[k]] + ce * (RING * RING)).astype(F32)
            m = jnp.zeros((8, TOK), F32)
            g = jnp.zeros((8, TOK), F32)
            for j in range(8):
                hit = ids[j:j + 1, :] == evec
                m = m + hit.astype(F32)
                g = g + jnp.where(hit, gval[j:j + 1, :], 0.0)
            ms.append(m)
            gs.append(g)
        rm = rank_of(jnp.concatenate(ms, axis=0))
        for b in range(4):
            hot = jnp.where(rm[b * 8:(b + 1) * 8][:, None, :] == slot, gs[b][:, None, :], 0.0).reshape(TOK, TOK).T
            hi = jnp.minimum(hot, BF16_MAX).astype(BF16)
            r1 = hot - hi.astype(F32)
            mid = r1.astype(BF16)
            lo = (r1 - mid.astype(F32)).astype(BF16)
            at = slice((b % 2) * TOK, (b % 2 + 1) * TOK)
            comb[k][i, b // 2, 0, :, at] = hi
            comb[k][i, b // 2, 1, :, at] = mid
            comb[k][i, b // 2, 2, :, at] = lo

    loop(4, lambda i: [weights(k, i) for k in range(3)])
    for c in w_copies:
        c.wait()

    x4 = [[Leg(q, cr, core if cr == 0 else other, til[q], sub, gat[q], til_block, pas4[q]) for cr in range(2)] for q in range(NQ)]
    rows = 2 * RING * RING * CAP
    for cr in range(2):
        c = core if cr == 0 else other
        for q in range(NQ):
            x3[q][cr].arrive()
        for q in range(NQ):
            x3[q][cr].sent()

        def hidden(i, c=c):
            xs = jnp.concatenate([rec[q][c, pl.ds(2 * i, 2)].reshape(rows, widths[q]) for q in range(NQ)], axis=1)
            for f in range(fdim // f_tile):
                cols = slice(f * f_tile, (f + 1) * f_tile)
                hg = jnp.dot(xs, w1[:, cols], preferred_element_type=F32)
                hu = jnp.dot(xs, w3[:, cols], preferred_element_type=F32)
                act[i, :, cols] = (hg * jax.nn.sigmoid(hg) * hu).astype(BF16)

        def down(wave, c=c):
            def step(i):
                lo, hi = offs[wave[0]], offs[wave[-1]] + widths[wave[-1]]
                o = jnp.dot(act[i], w2[:, lo:hi], preferred_element_type=F32).astype(BF16)
                for q in wave:
                    part_q = o[:, offs[q] - lo:offs[q] - lo + widths[q]]
                    til[q][c, pl.ds(2 * i, 2)] = part_q.reshape(2, RING, RING, CAP, widths[q])
            loop(2, step)

        hidden(0)
        if cr == 0:
            for q in W1 + W2:
                x3[q][1].forward()
        hidden(1)
        if cr == 1:
            for q in W1 + W2:
                x4[q][0].forward()
        down(W1)
        for q in W1:
            x4[q][cr].far()
        for q in W1:
            x4[q][cr].near()
        down(W2)
        for q in W2:
            x4[q][cr].far()
        if cr == 1:
            for q in W1:
                x4[q][1].forward()
        for q in W2:
            x4[q][cr].near()
        if cr == 0:
            for q in W1 + W2:
                keep4(q)
    for k in range(3):
        for i, d in enumerate(DIRS):
            pl.semaphore_signal(credit.at[k, i], inc=1, device_id=peer(D1[k], d, core), device_id_type=MESH)

    for q in W2:
        x4[q][1].forward()

    def from_src(ref, q, d, half=None):
        cs = slice(None) if half is None else half
        return ref.at[cs, :, d] if a1[q] else ref.at[cs, :, :, d]

    x5 = [([], []) for _ in range(NQ)]

    def arrive4(q):
        for cr in range(2):
            x4[q][cr].arrive()
        if q < 3:
            for i in range(2):
                pl.semaphore_wait(credit.at[q, i], 1)

    def far5(q):
        for i, d in enumerate(DIRS):
            x5[q][0].append(send(from_src(gat[q], q, mod(p1[q] + 2), i), pas5[q].at[i], peer(d1[q], d, core)))

    def near5(q):
        for i, d in enumerate(DIRS):
            x5[q][1].append(send(from_src(gat[q], q, mod(p1[q] + d)), rec[q].at[:, p1[q]], peer(d1[q], d, core)))

    def keep5(q):
        if a1[q]:
            rec[q][:, p1[q]] = gat[q][:, :, p1[q]]
        else:
            rec[q][:, p1[q]] = gat[q][:, :, :, p1[q]]

    def forward5(q):
        for i, d in enumerate(DIRS):
            x5[q][0][i].wait_recv()
            x5[q][1].append(send(pas5[q].at[i], rec[q].at[i, mod(p1[q] - d)], peer(d1[q], d, core)))

    for q in W1:
        arrive4(q)
        far5(q)
        near5(q)
    for q in W1:
        keep5(q)
    for q in W2:
        arrive4(q)
        far5(q)
    for q in W1:
        forward5(q)
    for q in W2:
        near5(q)
    for q in W2:
        keep5(q)
    for q in W2:
        forward5(q)

    x6 = [([], []) for _ in range(NQ)]
    half_tok = TOK // 2

    def combine(q):
        for cp in x5[q][1]:
            cp.wait_recv()
        k, w = q % 3, widths[q]

        def step(i):
            acc = jnp.zeros((TOK, w), F32)
            for c in range(2):
                o = rec[q][c, :, :, i].reshape(2 * TOK, w)
                for t in range(3):
                    acc = acc + jnp.dot(comb[k][i, c, t], o, preferred_element_type=F32)
            part[q][i] = acc

        return step

    def far6(q):
        for i, d in enumerate(DIRS):
            x6[q][0].append(send(part[q].at[mod(p2[q] + 2), pl.ds(i * half_tok, half_tok)], pas6[q].at[i], peer(d2[q], d, core)))

    def rows6(q, i, half):
        return part[q].at[mod(p2[q] + DIRS[i]), pl.ds(half * half_tok, half_tok)], prec[q].at[i, pl.ds(half * half_tok, half_tok)]

    def near6(q):
        for i, d in enumerate(DIRS):
            x6[q][1].append(send(*rows6(q, i, 1 - i), peer(d2[q], d, core)))

    def forward6(q):
        for i, d in enumerate(DIRS):
            x6[q][0][i].wait_recv()
            mine, there = rows6(q, i, i)
            mine[...] = mine[...] + pas6[q][i]
            x6[q][1].append(send(mine, there, peer(d2[q], d, core)))

    def final(q):
        for cp in x6[q][1]:
            cp.wait_recv()
        total = part[q][p2[q]] + prec[q][0] + prec[q][1]
        xk = x_ref[:, :, :, offs[q]:offs[q] + widths[q]].reshape(TOK, widths[q]).astype(F32)
        y_ref[:, offs[q]:offs[q] + widths[q]] = (xk + total).astype(BF16)
        cols = pl.ds(offs[q], widths[q])
        out = pltpu.make_async_copy(y_ref.at[:, cols], y_hbm.at[:, cols], out_sem.at[q])
        out.start()
        return out

    def far_sum(q):
        step = combine(q)
        step(mod(p2[q] + 2))
        far6(q)
        return step

    steps = {}
    for q in W1:
        steps[q] = far_sum(q)
    loop(3, lambda i: [steps[q](mod(p2[q] + 3 + i)) for q in W1])
    for q in W1:
        near6(q)
    for q in W2:
        steps[q] = far_sum(q)
    for q in W1:
        forward6(q)
    loop(3, lambda i: [steps[q](mod(p2[q] + 3 + i)) for q in W2])
    for q in W2:
        near6(q)
    for q in W2:
        forward6(q)
    outs = [final(q) for q in W1 + W2]
    for c in outs:
        c.wait()
    for q in range(NQ):
        for cr in range(2):
            x4[q][cr].sent()
        for cp in x5[q][0] + x5[q][1] + x6[q][0] + x6[q][1]:
            cp.wait_send()


N_COPIES = 3 * 9 + NQ * (16 + 13 + 13 + 6 + 6)


def solution(mesh):
    def local_layer(x_loc, ids_loc, gates_loc, w_g, w_u, w_d):
        tok, hid = x_loc.shape
        fdim = w_g.shape[2]
        widths = split_width(hid)
        f_tile = 256 if fdim % 256 == 0 else fdim
        x4 = x_loc.reshape(CORES, RING, CAP, hid)
        scratch = []
        each = lambda f: scratch.extend(f(w) for w in widths)
        for _ in range(3):
            each(lambda w: pltpu.VMEM(LEAD + (CAP, w), BF16))
        scratch += [pltpu.VMEM((RING, RING, 8, TOK), F32)] * 3
        scratch += [pltpu.VMEM((RING, RING, TOK, TOK), BF16)] * 3
        scratch += [pltpu.VMEM((RING, 2, 3, TOK, 2 * TOK), BF16)] * 3
        each(lambda w: pltpu.VMEM((2, CORES, 2, RING, CAP, w), BF16))
        each(lambda w: pltpu.VMEM((2, CORES, 2, RING, CAP, w), BF16))
        each(lambda w: pltpu.VMEM((2, RING, RING, CAP, w), BF16))
        each(lambda w: pltpu.VMEM((RING, TOK, w), F32))
        each(lambda w: pltpu.VMEM((2, TOK, w), F32))
        each(lambda w: pltpu.VMEM((2, TOK // 2, w), F32))
        scratch += [
            pltpu.VMEM((hid, fdim), BF16),
            pltpu.VMEM((hid, fdim), BF16),
            pltpu.VMEM((fdim, hid), BF16),
            pltpu.VMEM((2, 2 * RING * RING * CAP, fdim), BF16),
            pltpu.VMEM((8, TOK), F32),
            *[pltpu.VMEM((RING, 8, TOK), F32)] * 3,
            pltpu.VMEM(x4.shape, BF16),
            pltpu.VMEM((8, TOK), jnp.int32),
            pltpu.VMEM((8, TOK), F32),
            pltpu.VMEM((tok, hid), BF16),
            pltpu.SemaphoreType.DMA((N_COPIES,)),
            pltpu.SemaphoreType.DMA((N_COPIES,)),
            pltpu.SemaphoreType.DMA((3,)),
            pltpu.SemaphoreType.DMA((3,)),
            pltpu.SemaphoreType.DMA((NQ,)),
            pltpu.SemaphoreType.REGULAR((3, 2)),
        ]
        hbm = pl.BlockSpec(memory_space=pl.ANY)
        return pl.pallas_call(
            functools.partial(moe_kernel, widths, fdim, f_tile),
            out_shape=jax.ShapeDtypeStruct((tok, hid), BF16),
            in_specs=[hbm] * 6,
            out_specs=hbm,
            scratch_shapes=scratch,
            compiler_params=pltpu.CompilerParams(collective_id=0, has_side_effects=True, vmem_limit_bytes=62914560),
            name='moe',
        )(x4, ids_loc.T, gates_loc.T, w_g[0], w_u[0], w_d[0])

    tok_spec = P(TOKEN_AXES, None)
    w_spec = P(EXPERT_AXES, None, None)
    return jax.shard_map(local_layer, mesh=mesh, in_specs=(tok_spec, tok_spec, tok_spec, w_spec, w_spec, w_spec), out_specs=tok_spec, check_vma=False)
```

```python
import functools

import jax
import jax.numpy as jnp
from jax import lax
from jax.experimental import pallas as pl
from jax.experimental.pallas import tpu as pltpu
from jax.sharding import PartitionSpec as P

TOKEN_AXES = ('ez', 'ey', 'ex')
EXPERT_AXES = ('ex', 'ey', 'ez')
MESH = pl.DeviceIdType.MESH
F32 = jnp.float32
BF16 = jnp.bfloat16
BF16_MAX = float(jnp.finfo(jnp.bfloat16).max)

Z, Y, X = 0, 1, 2
D1 = (Y, Z, X)
D2 = (Z, X, Y)
D3 = (X, Y, Z)
A_IS_D1 = (True, False, True)
RING = 4
CORES = 2
CAP = 16
TOK = 128
LEAD = (CORES, RING, RING, RING)


NQ = 6
W1, W2 = (0, 1, 2), (3, 4, 5)


def split_width(hid):
    tiles = hid // 128
    second = tiles * 7 // 16
    first = tiles - second
    thirds = lambda n: [n - 2 * (n // 3), n // 3, n // 3]
    return tuple(n * 128 for n in thirds(first) + thirds(second))


def moe_kernel(widths, fdim, f_tile, x_hbm, ids_hbm, gates_hbm, w1_hbm, w3_hbm, w2_hbm, y_hbm, *scr):
    it = iter(scr)
    take = lambda n: [next(it) for _ in range(n)]
    gat, til, rec = take(NQ), take(NQ), take(NQ)
    meta, sel, comb = take(3), take(3), take(3)
    pas3, pas4, pas5 = take(NQ), take(NQ), take(NQ)
    part, prec, pas6 = take(NQ), take(NQ), take(NQ)
    w1, w3, w2, act, meta_ref = take(5)
    gates = take(3)
    x_ref, ids_ref, gates_ref, y_ref = take(4)
    send_sem, recv_sem, w_sem, in_sem, out_sem, credit = take(6)
    loads = [pltpu.make_async_copy(s, d, in_sem.at[i]) for i, (s, d) in enumerate(((ids_hbm, ids_ref), (gates_hbm, gates_ref), (x_hbm, x_ref)))]
    for c in loads:
        c.start()

    offs = [sum(widths[:q]) for q in range(NQ)]
    ez, ey, ex = lax.axis_index('ez'), lax.axis_index('ey'), lax.axis_index('ex')
    core = lax.rem(ex, CORES)
    pos = (ez, ey, ex // CORES)
    mod = lambda v: lax.rem(v + RING, RING)
    other = 1 - core

    strides = (1, RING, 2 * RING * RING)

    def turned(v, r):
        return [v[d] * (1 - r) + v[(d + 1) % 3] * r for d in range(3)]

    def peer(dim, off, c, lane=None):
        r = core if lane is None else lane
        q = [mod(pos[j] + off * ((1 - r) * int(j == dim) + r * int(j == (dim + 1) % 3))) for j in range(3)]
        return (q[0], q[1], q[2] * CORES + c)

    counter = [0]

    def send(src, dst, dev):
        i = counter[0]
        counter[0] += 1
        cp = pltpu.make_async_remote_copy(src, dst, send_sem.at[i], recv_sem.at[i], device_id=dev, device_id_type=MESH)
        cp.start()
        return cp

    bar = pltpu.get_barrier_semaphore()
    npeer = 0
    for dim in range(3):
        for off in (1, -1):
            for c in (core, other):
                pl.semaphore_signal(bar, inc=1, device_id=peer(dim, off, c, 0), device_id_type=MESH)
                npeer += 1
    pl.semaphore_signal(bar, inc=1, device_id=peer(0, 0, other), device_id_type=MESH)
    w_copies = [pltpu.make_async_copy(s, d, w_sem.at[i]) for i, (s, d) in enumerate(((w1_hbm, w1), (w3_hbm, w3), (w2_hbm, w2)))]
    for c in loads[:2]:
        c.wait()
    meta_ref[...] = ids_ref[...].astype(F32)
    loads[2].wait()
    pl.semaphore_wait(bar, npeer + 1)

    DIRS = (1, -1)
    d1 = [D1[q % 3] for q in range(NQ)]
    d2 = [D2[q % 3] for q in range(NQ)]
    d3 = [D3[q % 3] for q in range(NQ)]
    a1 = [A_IS_D1[q % 3] for q in range(NQ)]
    lpos, lstr = turned(pos, core), turned(strides, core)
    opos = turned(pos, other)
    p1 = [lpos[d] for d in d1]
    p2 = [lpos[d] for d in d2]
    p3 = [lpos[d] for d in d3]
    p3_other = [opos[d] for d in d3]
    xcol = [x_ref.at[:, :, :, pl.ds(offs[q], widths[q])] for q in range(NQ)]
    unwaited = []

    def chunk(q, r):
        return gat[q].at[:, :, p2[q], mod(p1[q] + r)]

    m1 = [[None, None] for _ in range(3)]
    mf1 = [None] * 3
    m2 = [[None, None] for _ in range(3)]
    mf2 = [None] * 3
    gm = [[None, None] for _ in range(3)]
    gmf = [None] * 3
    g1 = [[None, None] for _ in range(NQ)]
    f1 = [[None, None] for _ in range(NQ)]
    g2 = [[[None] * 4, [None] * 4] for _ in range(NQ)]
    f2 = [[None] * 4 for _ in range(NQ)]

    def first_sends(wave):
        for q in wave:
            for i, d in enumerate(DIRS):
                if q < 3:
                    m1[q][i] = send(meta_ref, meta[q].at[p2[q], p1[q]], peer(d1[q], d, core))
                g1[q][i] = send(xcol[q], chunk(q, 0), peer(d1[q], d, core))
        for q in wave:
            for i, d in enumerate(DIRS):
                g2[q][i][0] = send(xcol[q], chunk(q, 0), peer(d2[q], d, core))

    def first_forwards(wave):
        for q in wave:
            for i, d in enumerate(DIRS):
                if q < 3:
                    m1[q][i].wait_recv()
                    if i == 0:
                        src = meta[q].at[p2[q], mod(p1[q] - 1)]
                        mf1[q] = send(src, src, peer(d1[q], 1, core))
                g1[q][i].wait_recv()
                half = chunk(q, -d).at[i]
                f1[q][i] = send(half, half, peer(d1[q], d, core))
        for q in wave:
            for i, d in enumerate(DIRS):
                for r in (1, 3):
                    g2[q][i][r] = send(chunk(q, r), chunk(q, r), peer(d2[q], d, core))

    def forward2(q, i, r):
        g2[q][i][r].wait_recv()
        src = gat[q].at[:, :, mod(p2[q] - DIRS[i]), mod(p1[q] + r)]
        f2[q][r] = send(src, src, peer(d2[q], DIRS[i], core))

    first_sends(W1)
    first_sends(W2)
    for c in w_copies:
        c.start()
    for q in range(NQ):
        gat[q][:, :, p2[q], p1[q]] = x_ref[:, :, :, offs[q]:offs[q] + widths[q]]
    for k in range(3):
        meta[k][p2[k], p1[k]] = meta_ref[...]
        gates[k][p2[k]] = gates_ref[...]
    first_forwards(W1)
    for k in range(3):
        mf1[k].wait_recv()
        for i, d in enumerate(DIRS):
            row = meta[k].at[p2[k]]
            m2[k][i] = send(row, row, peer(d2[k], d, core))
            gm[k][i] = send(gates_ref, gates[k].at[p2[k]], peer(d2[k], d, core))

    def last_chunk(wave):
        for q in wave:
            for i, d in enumerate(DIRS):
                f1[q][i].wait_recv()
            for i, d in enumerate(DIRS):
                g2[q][i][2] = send(chunk(q, 2), chunk(q, 2), peer(d2[q], d, core))

    for q in W1:
        forward2(q, 0, 0)
    last_chunk(W1)
    first_forwards(W2)
    for k in range(3):
        for i in range(2):
            m2[k][i].wait_recv()
        src = meta[k].at[mod(p2[k] + 1)]
        mf2[k] = send(src, src, peer(d2[k], -1, core))
        for i in range(2):
            gm[k][i].wait_recv()
        src = gates[k].at[mod(p2[k] + 1)]
        gmf[k] = send(src, src, peer(d2[k], -1, core))

    tri = (lax.broadcasted_iota(jnp.int32, (TOK, TOK), 0) < lax.broadcasted_iota(jnp.int32, (TOK, TOK), 1)).astype(BF16)
    i8 = lax.broadcasted_iota(jnp.int32, (8, 1), 0)
    slot = lax.broadcasted_iota(jnp.int32, (8, CAP, TOK), 1).astype(F32)

    def experts8(k):
        base = lpos[D1[k]] * lstr[D1[k]] + lpos[D2[k]] * lstr[D2[k]]
        return (base + (i8 & 3) * lstr[D3[k]] + (i8 >> 2) * (RING * RING)).astype(F32)

    def picked(ids, evec):
        m = (ids[0:1, :] == evec).astype(F32)
        for j in range(1, 8):
            m = m + (ids[j:j + 1, :] == evec).astype(F32)
        return m

    def rank_of(m):
        rank = jnp.dot(m.astype(BF16), tri, preferred_element_type=F32)
        return jnp.where(m > 0.5, rank, -1.0)

    def onehot(k, i):
        evec = experts8(k)
        rm = rank_of(jnp.concatenate([picked(meta[k][i, j], evec) for j in range(4)], axis=0))
        for j in range(4):
            hot = (rm[j * 8:(j + 1) * 8][:, None, :] == slot).astype(F32)
            sel[k][i, j] = hot.reshape(TOK, TOK).astype(BF16)

    def select(q, i):
        k, w = q % 3, widths[q]
        for j in range(4):
            rows = gat[q][:, :, i, j].reshape(TOK, w)
            out = jnp.dot(sel[k][i, j], rows, preferred_element_type=F32).astype(BF16).reshape(CORES, RING, CAP, w)
            if a1[q]:
                til[q][:, :, j, i] = out
            else:
                til[q][:, :, i, j] = out

    def loop(n, f):
        def body(i, carry):
            f(i)
            return carry
        lax.fori_loop(0, n, body, 0)

    for k in range(3):
        onehot(k, p2[k])
    for q in W1:
        forward2(q, 0, 1)
        forward2(q, 1, 3)
    for q in W1:
        select(q, p2[q])
    for q in W1:
        forward2(q, 1, 2)
    for q in W2:
        forward2(q, 0, 0)
    last_chunk(W2)
    loop(2, lambda i: [onehot(k, mod(p2[k] - 1 + 2 * i)) for k in range(3)])

    def gathered(q, near):
        if near:
            for i, r in ((0, 2), (0, 3), (1, 0), (1, 1)):
                g2[q][i][r].wait_recv()
            loop(2, lambda i, q=q: select(q, mod(p2[q] - 1 + 2 * i)))
        else:
            for r in range(4):
                f2[q][r].wait_recv()
            select(q, mod(p2[q] + 2))
            done = g1[q] + f1[q] + g2[q][0] + g2[q][1] + f2[q]
            if q < 3:
                done = done + m1[q] + [mf1[q]] + m2[q] + [mf2[q]] + gm[q] + [gmf[q]]
            for c in done:
                c.wait_send()

    def sub(ref, q, c, d, half=None):
        a = slice(None) if half is None else pl.ds(2 * half, 2)
        return (ref.at[c, d, a], ref.at[c, a, d], ref.at[c, a, :, d])[q % 3]

    def til_block(ref, q, c, d, half=None):
        return ref.at[c, d] if half is None else ref.at[c, d, pl.ds(2 * half, 2)]

    class Leg:
        def __init__(self, q, cr, lane, src, src_block, dst, dst_block, pas):
            self.q, self.cr, self.lane, self.src, self.dst = q, cr, lane, src, dst
            self.src_block, self.dst_block, self.pas = src_block, dst_block, pas
            self.c = core if cr == 0 else other
            self.p = p3[q] if lane is core else p3_other[q]
            self.first, self.direct = [], []

        def out(self, d, half=None):
            return self.src_block(self.src, self.q, self.c, d, half)

        def into(self, d, half=None):
            return self.dst_block(self.dst, self.q, core, d, half)

        def far(self):
            for i, d in enumerate(DIRS):
                self.first.append(send(self.out(mod(self.p + 2), i), self.pas.at[i, self.cr], peer(d3[self.q], d, core, self.lane)))

        def near(self):
            for i, d in enumerate(DIRS):
                self.direct.append(send(self.out(mod(self.p + d)), self.into(self.p), peer(d3[self.q], d, self.c, self.lane)))
            if self.cr == 1:
                self.direct.append(send(self.out(self.p), self.into(self.p), peer(d3[self.q], 0, other, self.lane)))

        def forward(self):
            for i, d in enumerate(DIRS):
                self.first[i].wait_recv()
                self.direct.append(send(self.pas.at[i, self.cr], self.into(mod(self.p - d), i), peer(d3[self.q], d, self.c, self.lane)))

        def arrive(self):
            for cp in self.direct:
                cp.wait_recv()

        def sent(self):
            for cp in self.first + self.direct:
                cp.wait_send()

    def keep3(q):
        v = til[q][core, p3[q]]
        if q % 3 == 0:
            rec[q][core, p3[q]] = v
        elif q % 3 == 1:
            rec[q][core, :, p3[q]] = v
        else:
            rec[q][core, :, :, p3[q]] = v

    def keep4(q):
        if q % 3 == 0:
            v = til[q][core, p3[q]]
        elif q % 3 == 1:
            v = til[q][core, :, p3[q]]
        else:
            v = til[q][core, :, :, p3[q]]
        gat[q][core, p3[q]] = v

    x3 = [[Leg(q, cr, core, til[q], til_block, rec[q], sub, pas3[q]) for cr in range(2)] for q in range(NQ)]
    for q in W1:
        gathered(q, True)
    for q in W2:
        forward2(q, 0, 1)
        forward2(q, 1, 3)
    for q in W2:
        select(q, p2[q])
    for k in range(3):
        mf2[k].wait_recv()
        gmf[k].wait_recv()
    for k in range(3):
        onehot(k, mod(p2[k] + 2))
    for q in W1:
        gathered(q, False)
        x3[q][0].far()
    for q in W2:
        forward2(q, 1, 2)
    for q in W1:
        x3[q][0].near()
    for q in W2:
        gathered(q, True)
    for q in W1:
        x3[q][0].forward()
    for q in W2:
        gathered(q, False)
        x3[q][0].far()
    for q in W2:
        x3[q][0].near()
    for q in W1:
        x3[q][1].far()
    for q in W2:
        x3[q][0].forward()
    for q in W2:
        x3[q][1].far()
    for q in W1 + W2:
        x3[q][1].near()
    for q in W1 + W2:
        keep3(q)
    def weights(k, i):
        ids, gval = meta[k][i, p1[k]], gates[k][i]
        own = lpos[D2[k]] * lstr[D2[k]]
        ms, gs = [], []
        for b in range(4):
            idx = i8 + b * 8
            d3e, d1e, ce = idx & 3, (idx >> 2) & 3, idx >> 4
            evec = (own + d3e * lstr[D3[k]] + d1e * lstr[D1[k]] + ce * (RING * RING)).astype(F32)
            m = jnp.zeros((8, TOK), F32)
            g = jnp.zeros((8, TOK), F32)
            for j in range(8):
                hit = ids[j:j + 1, :] == evec
                m = m + hit.astype(F32)
                g = g + jnp.where(hit, gval[j:j + 1, :], 0.0)
            ms.append(m)
            gs.append(g)
        rm = rank_of(jnp.concatenate(ms, axis=0))
        for b in range(4):
            hot = jnp.where(rm[b * 8:(b + 1) * 8][:, None, :] == slot, gs[b][:, None, :], 0.0).reshape(TOK, TOK).T
            hi = jnp.minimum(hot, BF16_MAX).astype(BF16)
            r1 = hot - hi.astype(F32)
            mid = r1.astype(BF16)
            lo = (r1 - mid.astype(F32)).astype(BF16)
            at = slice((b % 2) * TOK, (b % 2 + 1) * TOK)
            comb[k][i, b // 2, 0, :, at] = hi
            comb[k][i, b // 2, 1, :, at] = mid
            comb[k][i, b // 2, 2, :, at] = lo

    loop(4, lambda i: [weights(k, i) for k in range(3)])
    for c in w_copies:
        c.wait()

    x4 = [[Leg(q, cr, core if cr == 0 else other, til[q], sub, gat[q], til_block, pas4[q]) for cr in range(2)] for q in range(NQ)]
    rows = 2 * RING * RING * CAP
    for cr in range(2):
        c = core if cr == 0 else other
        for q in range(NQ):
            x3[q][cr].arrive()
        for q in range(NQ):
            x3[q][cr].sent()

        def hidden(i, c=c):
            xs = jnp.concatenate([rec[q][c, pl.ds(2 * i, 2)].reshape(rows, widths[q]) for q in range(NQ)], axis=1)
            for f in range(fdim // f_tile):
                cols = slice(f * f_tile, (f + 1) * f_tile)
                hg = jnp.dot(xs, w1[:, cols], preferred_element_type=F32)
                hu = jnp.dot(xs, w3[:, cols], preferred_element_type=F32)
                act[i, :, cols] = (hg * jax.nn.sigmoid(hg) * hu).astype(BF16)

        def down(wave, c=c):
            def step(i):
                lo, hi = offs[wave[0]], offs[wave[-1]] + widths[wave[-1]]
                o = jnp.dot(act[i], w2[:, lo:hi], preferred_element_type=F32).astype(BF16)
                for q in wave:
                    part_q = o[:, offs[q] - lo:offs[q] - lo + widths[q]]
                    til[q][c, pl.ds(2 * i, 2)] = part_q.reshape(2, RING, RING, CAP, widths[q])
            loop(2, step)

        hidden(0)
        if cr == 0:
            for q in W1 + W2:
                x3[q][1].forward()
        hidden(1)
        if cr == 1:
            for q in W1 + W2:
                x4[q][0].forward()
        down(W1)
        for q in W1:
            x4[q][cr].far()
        for q in W1:
            x4[q][cr].near()
        down(W2)
        for q in W2:
            x4[q][cr].far()
        if cr == 1:
            for q in W1:
                x4[q][1].forward()
        for q in W2:
            x4[q][cr].near()
        if cr == 0:
            for q in W1 + W2:
                keep4(q)
    for k in range(3):
        for i, d in enumerate(DIRS):
            pl.semaphore_signal(credit.at[k, i], inc=1, device_id=peer(D1[k], d, core), device_id_type=MESH)

    for q in W2:
        x4[q][1].forward()

    def from_src(ref, q, d, half=None):
        cs = slice(None) if half is None else half
        return ref.at[cs, :, d] if a1[q] else ref.at[cs, :, :, d]

    x5 = [([], []) for _ in range(NQ)]

    def arrive4(q):
        for cr in range(2):
            x4[q][cr].arrive()
        if q < 3:
            for i in range(2):
                pl.semaphore_wait(credit.at[q, i], 1)

    def far5(q):
        for i, d in enumerate(DIRS):
            x5[q][0].append(send(from_src(gat[q], q, mod(p1[q] + 2), i), pas5[q].at[i], peer(d1[q], d, core)))

    def near5(q):
        for i, d in enumerate(DIRS):
            x5[q][1].append(send(from_src(gat[q], q, mod(p1[q] + d)), rec[q].at[:, p1[q]], peer(d1[q], d, core)))

    def keep5(q):
        if a1[q]:
            rec[q][:, p1[q]] = gat[q][:, :, p1[q]]
        else:
            rec[q][:, p1[q]] = gat[q][:, :, :, p1[q]]

    def forward5(q):
        for i, d in enumerate(DIRS):
            x5[q][0][i].wait_recv()
            x5[q][1].append(send(pas5[q].at[i], rec[q].at[i, mod(p1[q] - d)], peer(d1[q], d, core)))

    for q in W1:
        arrive4(q)
        far5(q)
        near5(q)
    for q in W1:
        keep5(q)
    for q in W2:
        arrive4(q)
        far5(q)
    for q in W1:
        forward5(q)
    for q in W2:
        near5(q)
    for q in W2:
        keep5(q)
    for q in W2:
        forward5(q)

    x6 = [([], []) for _ in range(NQ)]
    half_tok = TOK // 2

    def combine(q):
        for cp in x5[q][1]:
            cp.wait_recv()
        k, w = q % 3, widths[q]

        def step(i):
            acc = jnp.zeros((TOK, w), F32)
            for c in range(2):
                o = rec[q][c, :, :, i].reshape(2 * TOK, w)
                for t in range(3):
                    acc = acc + jnp.dot(comb[k][i, c, t], o, preferred_element_type=F32)
            part[q][i] = acc

        return step

    def far6(q):
        for i, d in enumerate(DIRS):
            x6[q][0].append(send(part[q].at[mod(p2[q] + 2), pl.ds(i * half_tok, half_tok)], pas6[q].at[i], peer(d2[q], d, core)))

    def rows6(q, i, half):
        return part[q].at[mod(p2[q] + DIRS[i]), pl.ds(half * half_tok, half_tok)], prec[q].at[i, pl.ds(half * half_tok, half_tok)]

    def near6(q):
        for i, d in enumerate(DIRS):
            x6[q][1].append(send(*rows6(q, i, 1 - i), peer(d2[q], d, core)))

    def forward6(q):
        for i, d in enumerate(DIRS):
            x6[q][0][i].wait_recv()
            mine, there = rows6(q, i, i)
            mine[...] = mine[...] + pas6[q][i]
            x6[q][1].append(send(mine, there, peer(d2[q], d, core)))

    def final(q):
        for cp in x6[q][1]:
            cp.wait_recv()
        total = part[q][p2[q]] + prec[q][0] + prec[q][1]
        xk = x_ref[:, :, :, offs[q]:offs[q] + widths[q]].reshape(TOK, widths[q]).astype(F32)
        y_ref[:, offs[q]:offs[q] + widths[q]] = (xk + total).astype(BF16)
        cols = pl.ds(offs[q], widths[q])
        out = pltpu.make_async_copy(y_ref.at[:, cols], y_hbm.at[:, cols], out_sem.at[q])
        out.start()
        return out

    def far_sum(q):
        step = combine(q)
        step(mod(p2[q] + 2))
        far6(q)
        return step

    steps = {}
    for q in W1:
        steps[q] = far_sum(q)
    loop(3, lambda i: [steps[q](mod(p2[q] + 3 + i)) for q in W1])
    for q in W1:
        near6(q)
    for q in W2:
        steps[q] = far_sum(q)
    for q in W1:
        forward6(q)
    loop(3, lambda i: [steps[q](mod(p2[q] + 3 + i)) for q in W2])
    for q in W2:
        near6(q)
    for q in W2:
        forward6(q)
    outs = [final(q) for q in W1 + W2]
    for c in outs:
        c.wait()
    for q in range(NQ):
        for cr in range(2):
            x4[q][cr].sent()
        for cp in x5[q][0] + x5[q][1] + x6[q][0] + x6[q][1]:
            cp.wait_send()


N_COPIES = 3 * 9 + NQ * (16 + 13 + 13 + 6 + 6)


def solution(mesh):
    def local_layer(x_loc, ids_loc, gates_loc, w_g, w_u, w_d):
        tok, hid = x_loc.shape
        fdim = w_g.shape[2]
        widths = split_width(hid)
        f_tile = 256 if fdim % 256 == 0 else fdim
        x4 = x_loc.reshape(CORES, RING, CAP, hid)
        scratch = []
        each = lambda f: scratch.extend(f(w) for w in widths)
        for _ in range(3):
            each(lambda w: pltpu.VMEM(LEAD + (CAP, w), BF16))
        scratch += [pltpu.VMEM((RING, RING, 8, TOK), F32)] * 3
        scratch += [pltpu.VMEM((RING, RING, TOK, TOK), BF16)] * 3
        scratch += [pltpu.VMEM((RING, 2, 3, TOK, 2 * TOK), BF16)] * 3
        each(lambda w: pltpu.VMEM((2, CORES, 2, RING, CAP, w), BF16))
        each(lambda w: pltpu.VMEM((2, CORES, 2, RING, CAP, w), BF16))
        each(lambda w: pltpu.VMEM((2, RING, RING, CAP, w), BF16))
        each(lambda w: pltpu.VMEM((RING, TOK, w), F32))
        each(lambda w: pltpu.VMEM((2, TOK, w), F32))
        each(lambda w: pltpu.VMEM((2, TOK // 2, w), F32))
        scratch += [
            pltpu.VMEM((hid, fdim), BF16),
            pltpu.VMEM((hid, fdim), BF16),
            pltpu.VMEM((fdim, hid), BF16),
            pltpu.VMEM((2, 2 * RING * RING * CAP, fdim), BF16),
            pltpu.VMEM((8, TOK), F32),
            *[pltpu.VMEM((RING, 8, TOK), F32)] * 3,
            pltpu.VMEM(x4.shape, BF16),
            pltpu.VMEM((8, TOK), jnp.int32),
            pltpu.VMEM((8, TOK), F32),
            pltpu.VMEM((tok, hid), BF16),
            pltpu.SemaphoreType.DMA((N_COPIES,)),
            pltpu.SemaphoreType.DMA((N_COPIES,)),
            pltpu.SemaphoreType.DMA((3,)),
            pltpu.SemaphoreType.DMA((3,)),
            pltpu.SemaphoreType.DMA((NQ,)),
            pltpu.SemaphoreType.REGULAR((3, 2)),
        ]
        hbm = pl.BlockSpec(memory_space=pl.ANY)
        return pl.pallas_call(
            functools.partial(moe_kernel, widths, fdim, f_tile),
            out_shape=jax.ShapeDtypeStruct((tok, hid), BF16),
            in_specs=[hbm] * 6,
            out_specs=hbm,
            scratch_shapes=scratch,
            compiler_params=pltpu.CompilerParams(collective_id=0, has_side_effects=True, vmem_limit_bytes=62914560),
            name='moe',
        )(x4, ids_loc.T, gates_loc.T, w_g[0], w_u[0], w_d[0])

    tok_spec = P(TOKEN_AXES, None)
    w_spec = P(EXPERT_AXES, None, None)
    return jax.shard_map(local_layer, mesh=mesh, in_specs=(tok_spec, tok_spec, tok_spec, w_spec, w_spec, w_spec), out_specs=tok_spec, check_vma=False)
```
